32 devices in a mesh: dp: 16 (over z, x, core), tensor: 2 (over y).
Axes of the slice: x: 2, y: 2, z: 4, core: 2. Of those that a mesh axis runs over, the one named last changes fastest.
Arguments:
- inputs: bfloat16 [4096, 2048], P(('dp', 'tensor')), may hold values from -6 to 6
- input_gain: bfloat16 [2048], P(('dp', 'tensor')), may hold values from 0.5 to 1.5
- post_gain: bfloat16 [2048], P(('dp', 'tensor')), may hold values from 0.5 to 1.5
- query_gain: bfloat16 [128], P(('dp', 'tensor')), may hold values from 0.25 to 1.75
- key_gain: bfloat16 [128], P(('dp', 'tensor')), may hold values from 0.25 to 1.75
- query_weight: bfloat16 [4096, 2048], P('tensor', 'dp'), may hold values from -0.125 to 0.125
- key_projection_matrix: bfloat16 [512, 2048], P('tensor', 'dp'), may hold values from -0.125 to 0.125
- value_projection_matrix: bfloat16 [512, 2048], P('tensor', 'dp'), may hold values from -0.125 to 0.125
- output_weight: bfloat16 [2048, 4096], P('dp', 'tensor'), may hold values from -0.375 to 0.375
- router_weight: bfloat16 [2048, 32], P(('dp', 'tensor')), may hold values from -0.125 to 0.125
- gate_weight: bfloat16 [32, 2048, 768], P('dp', None, 'tensor'), may hold values from -0.125 to 0.125
- up_weight: bfloat16 [32, 2048, 768], P('dp', None, 'tensor'), may hold values from -0.125 to 0.125
- down_weight: bfloat16 [32, 768, 2048], P('dp', 'tensor'), may hold values from -0.625 to 0.625
- routes: int32 [4096, 8], P(('dp', 'tensor')), may hold values from 0 to 31, all different within a row; in each aligned block of 128 rows (0 to 127, 128 to 255, ...) at most 64 rows name the same one
- cotangent: bfloat16 [4096, 2048], P(('dp', 'tensor')), may hold values from -6 to 6
Outputs:
- output: bfloat16 [4096, 2048], P(('dp', 'tensor'))
- grad_inputs: bfloat16 [4096, 2048], P(('dp', 'tensor'))
- grad_input_gain: float32 [2048], P(('dp', 'tensor'))
- grad_post_gain: float32 [2048], P(('dp', 'tensor'))
- grad_query_gain: float32 [128], P(('dp', 'tensor'))
- grad_key_gain: float32 [128], P(('dp', 'tensor'))
- grad_query_weight: float32 [4096, 2048], P('tensor', 'dp')
- grad_key_weight: float32 [512, 2048], P('tensor', 'dp')
- grad_value_weight: float32 [512, 2048], P('tensor', 'dp')
- grad_output_weight: float32 [2048, 4096], P('dp', 'tensor')
- grad_router_weight: float32 [2048, 32], P(('dp', 'tensor'))
- grad_gate_weight: float32 [32, 2048, 768], P('dp', None, 'tensor')
- grad_up_weight: float32 [32, 2048, 768], P('dp', None, 'tensor')
- grad_down_weight: float32 [32, 768, 2048], P('dp', 'tensor')
The draws below stay inside these ranges and needn't reach their ends.
Inputs may be any that keep to these rules, and one draw needn't show every extreme that they name: `routes`: each row names 8 different experts. In each aligned block of 128 rows (the rows of one device) no expert is named by more than 64 rows, a bound that some block reaches.
All inputs are finite; a program needn't handle non-finite values.
Results may differ from the reference program's by a relative error of at most 0.025.
Values may be sent and summed in bfloat16 or wider, within the bound.
No kernel may reach another device: no remote copies, remote signals or barrier semaphores. Data moves between devices by JAX's collectives and lax.ppermute only.
A program may use at most 384 MiB of HBM per device.

```python
import math
import jax
import jax.numpy as jnp
import numpy as np
from jax import lax

MODEL_WIDTH = 2048
QUERY_HEADS = 32
KEY_VALUE_HEADS = 4
HEAD_SIZE = 128
FFE = 768
TOP = 8
TOK_DEV = 128
EXPERTS = 32
SEQUENCE_TOKENS = 256
TOKENS = 4096
CAP = 64


def strengthened(array, stream_key, source, target, blocks, factor):
    def block_of(axis_at):
        return (jnp.arange(array.shape[axis_at]) // (array.shape[axis_at] // blocks)).reshape((-1,) + (1,) * (array.ndim - 1 - axis_at))

    one_side = jax.random.permutation(stream_key, blocks)[block_of(target)]
    other_side = (block_of(target) + blocks // 2) % blocks
    return jnp.where((block_of(source) == one_side) | (block_of(source) == other_side), factor * array, array)


def block_scale(rng, shape, shards, smallest, top_value):
    loudness, own = 1.0, jax.random.fold_in(rng, 6)
    for dim, blocks in shards:
        draws = jnp.exp(jax.random.uniform(jax.random.fold_in(own, dim), (blocks,), jnp.float32, smallest / len(shards), top_value / len(shards)))
        loudness = loudness * jnp.repeat(draws, shape[dim] // blocks).reshape([-1 if axis == dim else 1 for axis in range(len(shape))])
    return loudness


def shared_out(rng, own, number, rows, number_of, top, reach, skew):
    order = jax.random.permutation(rng, number_of)
    heavy_load, ordinary = portions_of(number_of, rows * top, reach, skew, True), portions_of(number_of, rows * top, reach, skew, False)
    places = jnp.arange(number_of)

    def named(lengths, turn):
        used = int((lengths > 0).sum())
        fixed = max(1, used // 4)
        moved = fixed + (places - fixed + turn * (used - fixed)) % max(1, number_of - fixed)
        return jnp.zeros((number_of,), jnp.int32).at[order[jnp.where(places < fixed, places, moved)]].set(jnp.asarray(lengths, jnp.int32))

    lengths = jnp.where(number % 4 == 0, named(heavy_load, number // 4), named(ordinary, number - number // 4 - 1))
    mixed = jax.random.permutation(jax.random.fold_in(own, 3), number_of)
    donor, sink = mixed[0:number_of // 2 * 2:2], mixed[1:number_of // 2 * 2:2]
    slack = jnp.minimum(lengths[donor] - 1, reach - lengths[sink]) // 2
    slack = jnp.where((donor == order[0]) | (sink == order[0]) | (lengths[sink] == 0), 0, jnp.maximum(slack, 0))
    moved = jax.random.randint(jax.random.fold_in(own, 4), (number_of // 2,), 0, 1 << 20) % (slack + 1)
    lengths = lengths.at[donor].add(-moved).at[sink].add(moved)
    members = jnp.searchsorted(jnp.cumsum(lengths), jnp.arange(rows * top), side="right").astype(jnp.int32)
    table = members.reshape(top, rows).T
    table = table[jax.random.permutation(jax.random.fold_in(own, 1), rows)]
    turn = jax.random.randint(jax.random.fold_in(own, 2), (rows, 1), 0, top)
    return jnp.take_along_axis(table, (jnp.arange(top)[None, :] + turn) % top, axis=1)


def portions_of(count, total, reach, slope, full):
    weights = [(1 << 20) // math.isqrt(grade ** slope) + 1 for grade in range(1, count + 1)]
    largest = reach if full else min(reach, max(-(-total // count), total * weights[0] // sum(weights)))
    least = 1 if total - largest >= count - 1 else 0
    given, surplus = [largest] + [least] * (count - 1), total - largest - least * (count - 1)
    while surplus > 0:
        movable = [i for i in range(1, count) if given[i] < largest] or [i for i in range(1, count) if given[i] < reach]
        mass, budget = sum([weights[i] for i in movable]), surplus
        for i in movable:
            extra = min(reach - given[i], max(1, budget * weights[i] // mass), surplus)
            given[i] = given[i] + extra
            surplus = surplus - extra
    return np.array(given)


def centred(own_key, extent, width, reach, shards=(), kind=jnp.bfloat16):
    array = width * jax.random.normal(own_key, extent, jnp.float32)
    if shards:
        array = array * block_scale(own_key, extent, shards, -0.22, 0.18)
    return jnp.clip(array, -reach, reach).astype(kind)


def gaussian_with(key, extent, spread, most, pieces, heavy, kind=jnp.bfloat16):
    entries = spread * jax.random.normal(key, extent, jnp.float32)
    if pieces:
        entries = entries * block_scale(key, extent, pieces, -0.22, 0.18)
    return jnp.clip(strengthened(entries, jax.random.fold_in(key, 3), *heavy), -most, most).astype(kind)


def setup_inputs(seed: int = 0) -> dict:
    splits = jax.random.split(jax.random.key(seed), 16)
    inputs = centred(splits[0], (TOKENS, MODEL_WIDTH), 1.0, 6.0, ((0, 32),))
    input_gain = jnp.clip(1.0 + 0.1 * jax.random.normal(splits[1], (MODEL_WIDTH,), jnp.float32), 0.5, 1.5).astype(jnp.bfloat16)
    post_gain = jnp.clip(1.0 + 0.1 * jax.random.normal(splits[2], (MODEL_WIDTH,), jnp.float32), 0.5, 1.5).astype(jnp.bfloat16)
    query_gain = jnp.clip(1.0 + 0.15 * jax.random.normal(splits[3], (HEAD_SIZE,), jnp.float32), 0.25, 1.75).astype(jnp.bfloat16)
    key_gain = jnp.clip(1.0 + 0.15 * jax.random.normal(splits[4], (HEAD_SIZE,), jnp.float32), 0.25, 1.75).astype(jnp.bfloat16)
    query_weight = centred(splits[5], (QUERY_HEADS * HEAD_SIZE, MODEL_WIDTH), MODEL_WIDTH ** -0.5, 0.125, ((0, 2), (1, 16)))
    key_projection_matrix = centred(splits[6], (KEY_VALUE_HEADS * HEAD_SIZE, MODEL_WIDTH), MODEL_WIDTH ** -0.5, 0.125, ((0, 2), (1, 16)))
    value_projection_matrix = centred(splits[7], (KEY_VALUE_HEADS * HEAD_SIZE, MODEL_WIDTH), MODEL_WIDTH ** -0.5, 0.125, ((0, 2), (1, 16)))
    output_weight = centred(splits[8], (MODEL_WIDTH, QUERY_HEADS * HEAD_SIZE), (QUERY_HEADS * HEAD_SIZE // 16) ** -0.5, 0.375, ((0, 16), (1, 2)))
    router_weight = centred(splits[9], (MODEL_WIDTH, EXPERTS), MODEL_WIDTH ** -0.5, 0.125, ((0, 32),))
    gate_weight = centred(splits[10], (EXPERTS, MODEL_WIDTH, FFE), MODEL_WIDTH ** -0.5, 0.125, ((0, 16), (2, 2)))
    up_weight = centred(splits[11], (EXPERTS, MODEL_WIDTH, FFE), MODEL_WIDTH ** -0.5, 0.125, ((0, 16), (2, 2)))
    down_weight = centred(splits[12], (EXPERTS, FFE, MODEL_WIDTH), (FFE // 8) ** -0.5, 0.625, ((0, 16), (1, 2)))
    routes_keys = jax.random.split(jax.random.fold_in(splits[13], 1), TOKENS // TOK_DEV)
    routes_turns = jax.random.permutation(jax.random.fold_in(splits[13], 3), TOKENS // TOK_DEV)
    routes = jax.vmap(lambda own, number: shared_out(jax.random.fold_in(splits[13], 2), own, number, TOK_DEV, EXPERTS, TOP, CAP, 1))(routes_keys, routes_turns).reshape((TOKENS, TOP))
    cotangent = gaussian_with(splits[14], (TOKENS, MODEL_WIDTH), 1.0, 6.0, ((0, 32),), (0, 1, 32, 2.75))
    return dict(inputs=inputs, input_gain=input_gain, post_gain=post_gain, query_gain=query_gain, key_gain=key_gain, query_weight=query_weight, key_projection_matrix=key_projection_matrix, value_projection_matrix=value_projection_matrix, output_weight=output_weight, router_weight=router_weight, gate_weight=gate_weight, up_weight=up_weight, down_weight=down_weight, routes=routes, cotangent=cotangent)


EPSILON = 1e-06
ROPE_BASE = 1000000.0
HIGHEST = lax.Precision.HIGHEST

@jax.custom_vjp
def reduced_precision(v):
    return lax.optimization_barrier(v.astype(jnp.bfloat16)).astype(jnp.float32)

@jax.custom_vjp
def reduced_back_cast(v):
    return v

def low_keep(v):
    return (reduced_precision(v), None)

def low_pass(kept, grad):
    return (grad,)

def back_keep(v):
    return (v, None)

def back_low(kept, grad):
    return (reduced_precision(grad),)
reduced_precision.defvjp(low_keep, low_pass)
reduced_back_cast.defvjp(back_keep, back_low)

def matrix_product(left, right):
    return jnp.matmul(left, right, precision=HIGHEST)

def norm_rows(values, weights):
    inverse = lax.rsqrt(lax.optimization_barrier(jnp.mean(values * values, axis=-1, keepdims=True)) + EPSILON)
    return values * inverse * weights

def rope_tables(length, head_width):
    half_width = head_width // 2
    frequency = jnp.exp(jnp.arange(half_width, dtype=jnp.float32) * (-2.0 * math.log(ROPE_BASE) / head_width))
    angles = jnp.arange(length, dtype=jnp.float32)[:, None] * frequency[None, :]
    angles = jnp.concatenate([angles, angles], axis=-1)
    return (jnp.cos(angles), jnp.sin(angles))

def rotate_half(values):
    half_width = values.shape[-1] // 2
    return jnp.concatenate([-values[..., half_width:], values[..., :half_width]], axis=-1)

def attend_group(sequence_block, input_gain, query_gain, key_gain, query_weight, key_projection_matrix, value_projection_matrix, output_weight):
    heads_per_group = sequence_block.shape[0]
    normalized_rows = reduced_precision(norm_rows(sequence_block, input_gain))
    query_raw = reduced_back_cast(matrix_product(normalized_rows, query_weight.T)).reshape(heads_per_group, SEQUENCE_TOKENS, QUERY_HEADS, HEAD_SIZE)
    key_unrotated = reduced_back_cast(matrix_product(normalized_rows, key_projection_matrix.T)).reshape(heads_per_group, SEQUENCE_TOKENS, KEY_VALUE_HEADS, HEAD_SIZE)
    value_reduced = reduced_back_cast(reduced_precision(matrix_product(normalized_rows, value_projection_matrix.T))).reshape(heads_per_group, SEQUENCE_TOKENS, KEY_VALUE_HEADS, HEAD_SIZE)
    cosine_table, sine_table = rope_tables(SEQUENCE_TOKENS, HEAD_SIZE)
    query_norm = norm_rows(query_raw, query_gain)
    query_reduced = reduced_precision(query_norm * cosine_table[:, None, :] + rotate_half(query_norm) * sine_table[:, None, :])
    key_norm = norm_rows(key_unrotated, key_gain)
    key_low = reduced_precision(key_norm * cosine_table[:, None, :] + rotate_half(key_norm) * sine_table[:, None, :])
    query_reduced = query_reduced.reshape(heads_per_group, SEQUENCE_TOKENS, KEY_VALUE_HEADS, QUERY_HEADS // KEY_VALUE_HEADS, HEAD_SIZE)
    score_scale = 1.0 / math.sqrt(HEAD_SIZE)
    scores = jnp.einsum('bqhgd,bkhd->bhgqk', query_reduced, key_low, precision=HIGHEST) * score_scale
    row_index = jnp.arange(SEQUENCE_TOKENS, dtype=jnp.int32)
    causal = row_index[None, :] <= row_index[:, None]
    scores = reduced_back_cast(jnp.where(causal, scores, -1e+30))
    attend = reduced_precision(jax.nn.softmax(scores, axis=-1))
    mixed_heads = jnp.einsum('bhgqk,bkhd->bqhgd', attend, value_reduced, precision=HIGHEST)
    mixed_heads = reduced_back_cast(reduced_precision(mixed_heads)).reshape(heads_per_group, SEQUENCE_TOKENS, QUERY_HEADS * HEAD_SIZE)
    return sequence_block + reduced_back_cast(matrix_product(mixed_heads, output_weight.T))

def forward(inputs, input_gain, post_gain, query_gain, key_gain, query_weight, key_projection_matrix, value_projection_matrix, output_weight, router_weight, gate_weight, up_weight, down_weight, routes):
    token_count = inputs.shape[0]
    sequences = token_count // SEQUENCE_TOKENS
    heads_per_group = math.gcd(sequences, max(1, 4096 // SEQUENCE_TOKENS))

    def attend_one(sequence_block):
        return attend_group(sequence_block, input_gain, query_gain, key_gain, query_weight, key_projection_matrix, value_projection_matrix, output_weight)
    middle = lax.map(jax.checkpoint(attend_one), inputs.reshape(sequences // heads_per_group, heads_per_group, SEQUENCE_TOKENS, MODEL_WIDTH)).reshape(token_count, MODEL_WIDTH)
    post_low = reduced_precision(norm_rows(middle, post_gain))
    logits = reduced_back_cast(matrix_product(post_low, router_weight))
    picked = jnp.take_along_axis(logits, routes, axis=1)
    route_gate = jax.nn.softmax(picked, axis=-1)
    flat_routes = routes.reshape(-1)
    route_total = flat_routes.shape[0]
    blocks = route_total // (TOK_DEV * TOP)
    expert_ids = jnp.arange(EXPERTS, dtype=jnp.int32)
    route_hits = (flat_routes.reshape(blocks, TOK_DEV * TOP)[:, :, None] == expert_ids[None, None, :]).astype(jnp.int32)
    position = lax.optimization_barrier(jnp.sum((jnp.cumsum(route_hits, axis=1) - route_hits) * route_hits, axis=2)).reshape(-1)
    block_of = jnp.arange(route_total, dtype=jnp.int32) // (TOK_DEV * TOP)
    slot_count = blocks * CAP
    slot_index = flat_routes * slot_count + block_of * CAP + position
    filler = jnp.full((EXPERTS * slot_count,), route_total, dtype=jnp.int32)
    filler = filler.at[slot_index].set(jnp.arange(route_total, dtype=jnp.int32)).reshape(EXPERTS, slot_count)
    post_padded = jnp.concatenate([post_low, jnp.zeros((1, MODEL_WIDTH), dtype=jnp.float32)], axis=0)
    gate_padded = jnp.concatenate([route_gate.reshape(-1), jnp.zeros((1,), dtype=jnp.float32)], axis=0)

    def expert_apply(operands):
        slot_fill, gate_matrix, up_matrix, down_matrix = operands
        slot_rows = reduced_back_cast(post_padded[slot_fill // TOP])
        gate_pre = reduced_back_cast(matrix_product(slot_rows, gate_matrix))
        up_pre = reduced_back_cast(matrix_product(slot_rows, up_matrix))
        hidden = reduced_precision(jax.nn.silu(gate_pre) * up_pre)
        expert_out = reduced_back_cast(reduced_precision(matrix_product(hidden, down_matrix)))
        return expert_out * gate_padded[slot_fill][:, None]
    weighted = lax.map(jax.checkpoint(expert_apply), (filler, gate_weight, up_weight, down_weight))
    expert_sum = jnp.zeros((token_count + 1, MODEL_WIDTH), dtype=jnp.float32)
    expert_sum = expert_sum.at[(filler // TOP).reshape(-1)].add(weighted.reshape(-1, MODEL_WIDTH))[:token_count]
    return middle + expert_sum

def reference(inputs, input_gain, post_gain, query_gain, key_gain, query_weight, key_projection_matrix, value_projection_matrix, output_weight, router_weight, gate_weight, up_weight, down_weight, routes, cotangent):
    float_args = tuple((item.astype(jnp.float32) for item in (inputs, input_gain, post_gain, query_gain, key_gain, query_weight, key_projection_matrix, value_projection_matrix, output_weight, router_weight, gate_weight, up_weight, down_weight)))

    def layer(*operands):
        return forward(*operands, routes)
    result, pullback = jax.vjp(layer, *float_args)
    gradients = pullback(cotangent.astype(jnp.float32))
    return (result.astype(jnp.bfloat16), gradients[0].astype(jnp.bfloat16), gradients[1], gradients[2], gradients[3], gradients[4], gradients[5], gradients[6], gradients[7], gradients[8], gradients[9], gradients[10], gradients[11], gradients[12])
```

```python
import functools
import math

import jax
import jax.numpy as jnp
import numpy as np
from jax import lax
from jax.experimental import pallas as pl
from jax.experimental.pallas import tpu as pltpu
from jax.sharding import PartitionSpec as P

HEAD_SIZE = 128
LANES = 128
EPSILON = 1e-06
ROPE_BASE = 1000000.0
BOTH = ("dp", "tensor")
BF16 = jnp.bfloat16
F32 = jnp.float32
STEP_BLOCKS = 4
VMEM_BYTES = 60 * 1024 * 1024


def norm_rows(values, weights):
    inverse = lax.rsqrt(jnp.mean(values * values, axis=-1, keepdims=True) + EPSILON)
    normalized_rows = values * inverse
    return (normalized_rows * weights, normalized_rows, inverse)


def norm_back(upstream, weights, normalized_rows, inverse):
    scaled = upstream * weights
    inner_term = jnp.mean(scaled * normalized_rows, axis=-1, keepdims=True)
    return (inverse * (scaled - normalized_rows * inner_term), upstream * normalized_rows)


def rope_tables(length, head_width):
    half_width = head_width // 2
    frequency = jnp.exp(
        jnp.arange(half_width, dtype=F32) * (-2.0 * math.log(ROPE_BASE) / head_width)
    )
    angles = jnp.arange(length, dtype=F32)[:, None] * frequency[None, :]
    angles = jnp.concatenate([angles, angles], axis=-1)
    return (jnp.cos(angles), jnp.sin(angles))


def rotate_half(values):
    half_width = values.shape[-1] // 2
    return jnp.concatenate([-values[..., half_width:], values[..., :half_width]], axis=-1)


def rotate_back(values):
    half_width = values.shape[-1] // 2
    return jnp.concatenate([values[..., half_width:], -values[..., :half_width]], axis=-1)


def dot(left, right, left_dim=1, right_dim=0):
    return lax.dot_general(
        left, right, (((left_dim,), (right_dim,)), ((), ())), preferred_element_type=F32
    )


LATTICE = {"z": 4, "x": 2, "core": 2, "y": 2}


def is_lattice(dp_count, tensor_count):
    return dp_count == 16 and tensor_count == 2


def hop(values, axis, step=1):
    sizes = tuple(LATTICE.values())
    place = list(LATTICE).index(axis)
    pairs = []
    for source in range(math.prod(sizes)):
        spot = list(np.unravel_index(source, sizes))
        spot[place] = (spot[place] + step) % sizes[place]
        pairs.append((source, int(np.ravel_multi_index(spot, sizes))))
    return lax.ppermute(values, BOTH, pairs)


def my_spot():
    chip_core = lax.axis_index("dp")
    return {
        "z": chip_core // 4,
        "x": (chip_core // 2) % 2,
        "core": chip_core % 2,
        "y": lax.axis_index("tensor"),
    }


def add_low(first, second):
    return (first.astype(F32) + second.astype(F32)).astype(BF16)


class Pending:
    def __init__(self, first, second):
        self.parts = (first, second)

    def piece(self, place, dim):
        first, second = (lax.index_in_dim(part, place, dim, keepdims=False) for part in self.parts)
        return add_low(first, second)


def reduce_home(partner, own, dims, order):
    dims = list(dims)
    pending = Pending(own, hop(partner, "core"))
    for axis in order:
        dim = dims.index(axis)
        dims.remove(axis)
        if axis == "z":
            moving = pending.piece(3, dim)
            for place in (2, 1):
                moving = add_low(hop(moving, "z", -1), pending.piece(place, dim))
            pending = Pending(pending.piece(0, dim), hop(moving, "z", -1))
        else:
            pending = Pending(pending.piece(0, dim), hop(pending.piece(1, dim), axis))
    first, second = pending.parts
    return first.astype(F32) + second.astype(F32)


def reduce_small(values):
    device_count = values.shape[0]
    number = lax.axis_index("dp") * lax.axis_size("tensor") + lax.axis_index("tensor")
    bit = device_count // 2
    while bit:
        halves = values.reshape((2, bit) + values.shape[1:])
        mine = (number // bit) % 2
        pairs = [(source, source ^ bit) for source in range(device_count)]
        sent = lax.dynamic_index_in_dim(halves, 1 - mine, 0, keepdims=False)
        kept = lax.dynamic_index_in_dim(halves, mine, 0, keepdims=False)
        values = kept + lax.ppermute(sent, BOTH, pairs)
        bit //= 2
    return values[0]


def swap_tensor(values):
    return lax.ppermute(values, "tensor", [(0, 1), (1, 0)])


def in_order(mine, other):
    first = lax.axis_index("tensor") == 0
    return jnp.where(
        first, jnp.concatenate([mine, other], axis=0), jnp.concatenate([other, mine], axis=0)
    )


def sum_tokens(terms):
    low = terms.astype(BF16).reshape((2, terms.shape[0] // 2) + terms.shape[1:])
    half = lax.axis_index("tensor")
    sent = lax.dynamic_index_in_dim(low, 1 - half, 0, keepdims=False)
    kept = lax.dynamic_index_in_dim(low, half, 0, keepdims=False)
    return kept.astype(F32) + swap_tensor(sent).astype(F32)


def choose(position_row, capacity):
    slot = lax.broadcasted_iota(jnp.int32, (capacity, position_row.shape[1]), 0).astype(F32)
    picks = [
        (slot == position_row[e : e + 1, :]).astype(F32) for e in range(position_row.shape[0])
    ]
    return picks


def expert_kernel(capacity, widths, perm, first, *refs):
    blocks = STEP_BLOCKS
    token_refs, grad_refs = refs[:blocks], refs[blocks : 2 * blocks]
    position_ref, mask_ref, router_ref, up_ref, up_t_ref, down_t_ref = refs[
        2 * blocks : 2 * blocks + 6
    ]
    rows_ref, grad_rows_ref, gated_ref, grad_gate_ref, grad_up_ref = refs[
        2 * blocks + 6 : 2 * blocks + 11
    ]
    out_refs = refs[2 * blocks + 11 : 2 * blocks + 14]
    packed_ref = refs[2 * blocks + 14]
    experts_here = up_ref.shape[0]
    hidden_units = down_t_ref.shape[2]
    width = token_refs[0].shape[2]
    first_expert = first[0]
    gates = [[] for _ in range(experts_here)]
    choices = []
    for j in range(blocks):
        tokens = token_refs[j][0]
        grads = grad_refs[j][0]
        picks = choose(position_ref[j], capacity)
        choice = jnp.concatenate(picks, axis=0).astype(BF16)
        choices.append(choice)
        rows = dot(choice, tokens).astype(BF16)
        grad_rows = dot(choice, grads).astype(BF16)
        logits = dot(router_ref[...], tokens, 1, 1)
        chosen = mask_ref[j].astype(F32) > 0.5
        top = jnp.max(jnp.where(chosen, logits, -3e38), axis=0, keepdims=True)
        powers = jnp.where(chosen, jnp.exp(jnp.minimum(logits - top, 0.0)), 0.0)
        gate_all = powers / jnp.sum(powers, axis=0, keepdims=True)
        expert_number = lax.broadcasted_iota(jnp.int32, gate_all.shape, 0)
        for e in range(experts_here):
            here = slice(j * capacity, (j + 1) * capacity)
            rows_ref[e, here, :] = rows[e * capacity : (e + 1) * capacity]
            grad_rows_ref[e, here, :] = grad_rows[e * capacity : (e + 1) * capacity]
            gate_row = jnp.sum(
                jnp.where(expert_number == first_expert + e, gate_all, 0.0), axis=0, keepdims=True
            )
            gates[e].append(jnp.sum(picks[e] * gate_row, axis=1, keepdims=True))
    for e in range(experts_here):
        both = dot(rows_ref[e], up_ref[e])
        gate_pre = both[:, :hidden_units]
        up_pre = both[:, hidden_units:]
        raw = dot(grad_rows_ref[e], down_t_ref[e])
        sigmoid = 1.0 / (1.0 + jnp.exp(-gate_pre))
        silu = gate_pre * sigmoid
        hidden = silu * up_pre
        gate = jnp.concatenate(gates[e], axis=0)
        grad_gate = jnp.sum(hidden * raw, axis=1, keepdims=True)
        grad_hidden = gate * raw
        grad_gate_pre = (
            grad_hidden * up_pre * sigmoid * (1.0 + gate_pre * (1.0 - sigmoid))
        ).astype(BF16)
        grad_up_pre = (grad_hidden * silu).astype(BF16)
        gated_ref[e] = (gate * hidden).astype(BF16)
        grad_gate_ref[e] = grad_gate_pre
        grad_up_ref[e] = grad_up_pre
        back = dot(grad_gate_pre, up_t_ref[e, :hidden_units, :]) + dot(
            grad_up_pre, up_t_ref[e, hidden_units:, :]
        )
        lane = lax.broadcasted_iota(jnp.int32, (blocks * capacity, LANES), 1)
        extra = jnp.where(lane == first_expert + e, grad_gate, 0.0).astype(BF16)
        back = back.astype(BF16)
        for j in range(blocks):
            packed_ref[j, e * capacity : (e + 1) * capacity, :width] = back[
                j * capacity : (j + 1) * capacity
            ]
            packed_ref[j, e * capacity : (e + 1) * capacity, width:] = extra[
                j * capacity : (j + 1) * capacity
            ]
    for j in range(blocks):
        home = dot(choices[j], packed_ref[j], 0, 0).astype(BF16)
        start = 0
        for out_ref, size in zip(out_refs, widths):
            out_ref[j] = home[:, start : start + size]
            start += size


def block_spec(width, place):
    return pl.BlockSpec(
        (1, LANES, width), lambda i, perm, first: (perm[i * STEP_BLOCKS + place], 0, 0)
    )


def whole(shape):
    return pl.BlockSpec(
        shape, lambda i, *scalars: (0,) * len(shape), pipeline_mode=pl.Buffered(1)
    )


def stepped(shape, dim):
    return pl.BlockSpec(
        shape, lambda i, *scalars: tuple(i if d == dim else 0 for d in range(len(shape)))
    )


def expert_grads(
    perm, first, tokens, grads, position, mask, router_t, up_both, up_both_t, down_t, capacity, widths
):
    count = perm.shape[0]
    width = tokens.shape[2]
    experts_here, hidden_units = down_t.shape[0], down_t.shape[2]
    slots = STEP_BLOCKS * capacity
    expert_count = router_t.shape[0]
    slot_shape = lambda size: jax.ShapeDtypeStruct((experts_here, count * capacity, size), BF16)
    flops = 2 * count * capacity * experts_here * (7 * hidden_units * width + 3 * LANES * width)
    call = pl.pallas_call(
        functools.partial(expert_kernel, capacity, widths),
        grid_spec=pltpu.PrefetchScalarGridSpec(
            num_scalar_prefetch=2,
            grid=(count // STEP_BLOCKS,),
            in_specs=[block_spec(width, j) for j in range(STEP_BLOCKS)] * 2
            + [
                stepped((STEP_BLOCKS, experts_here, LANES), 0),
                stepped((STEP_BLOCKS, expert_count, LANES), 0),
                whole(router_t.shape),
                whole(up_both.shape),
                whole(up_both_t.shape),
                whole(down_t.shape),
            ],
            out_specs=[stepped((experts_here, slots, width), 1)] * 2
            + [stepped((experts_here, slots, hidden_units), 1)] * 3
            + [stepped((STEP_BLOCKS, LANES, size), 0) for size in widths],
            scratch_shapes=[
                pltpu.VMEM((STEP_BLOCKS, experts_here * capacity, sum(widths)), BF16)
            ],
        ),
        out_shape=[slot_shape(width)] * 2
        + [slot_shape(hidden_units)] * 3
        + [jax.ShapeDtypeStruct((count, LANES, size), BF16) for size in widths],
        compiler_params=pltpu.CompilerParams(vmem_limit_bytes=VMEM_BYTES),
        cost_estimate=pl.CostEstimate(
            flops=flops, transcendentals=0, bytes_accessed=6 * count * LANES * width * 2
        ),
        name="expert_grads",
    )
    return call(
        perm, first, *([tokens] * STEP_BLOCKS), *([grads] * STEP_BLOCKS),
        position, mask, router_t, up_both, up_both_t, down_t,
    )


def output_kernel(capacity, widths, gated_ref, position_ref, down_ref, *refs):
    out_refs = refs[: len(widths)]
    packed_ref = refs[len(widths)]
    for e in range(down_ref.shape[0]):
        rows = dot(gated_ref[e], down_ref[e]).astype(BF16)
        for j in range(STEP_BLOCKS):
            packed_ref[j, e * capacity : (e + 1) * capacity, :] = rows[
                j * capacity : (j + 1) * capacity
            ]
    for j in range(STEP_BLOCKS):
        choice = jnp.concatenate(choose(position_ref[j], capacity), axis=0).astype(BF16)
        home = dot(choice, packed_ref[j], 0, 0).astype(BF16)
        start = 0
        for out_ref, size in zip(out_refs, widths):
            out_ref[j] = home[:, start : start + size]
            start += size


def expert_outputs(gated, position, down, capacity, widths):
    count = position.shape[0]
    experts_here, hidden_units, width = down.shape
    slots = STEP_BLOCKS * capacity
    call = pl.pallas_call(
        functools.partial(output_kernel, capacity, widths),
        grid=(count // STEP_BLOCKS,),
        in_specs=[
            stepped((experts_here, slots, hidden_units), 1),
            stepped((STEP_BLOCKS, experts_here, LANES), 0),
            whole(down.shape),
        ],
        out_specs=[stepped((STEP_BLOCKS, LANES, size), 0) for size in widths],
        out_shape=[jax.ShapeDtypeStruct((count, LANES, size), BF16) for size in widths],
        scratch_shapes=[pltpu.VMEM((STEP_BLOCKS, experts_here * capacity, width), BF16)],
        compiler_params=pltpu.CompilerParams(vmem_limit_bytes=VMEM_BYTES),
        cost_estimate=pl.CostEstimate(
            flops=2 * count * capacity * experts_here * (hidden_units * width + LANES * width),
            transcendentals=0,
            bytes_accessed=2 * count * LANES * width * 2,
        ),
        name="expert_outputs",
    )
    return call(gated, position, down)


def chunk_kernel(widths, perm, *refs):
    left = jnp.concatenate([ref[...] for ref in refs[:STEP_BLOCKS]], axis=1)
    product = dot(left, refs[STEP_BLOCKS][...], 0, 0).astype(BF16)
    start = 0
    for out_ref, size in zip(refs[STEP_BLOCKS + 1 :], widths):
        for j in range(STEP_BLOCKS):
            out_ref[j] = product[j * LANES : (j + 1) * LANES, start : start + size]
        start += size


def chunk_products(perm, left, right, widths):
    count = perm.shape[0]
    tokens = left.shape[0]

    def column_block(place):
        return pl.BlockSpec((tokens, LANES), lambda i, perm: (0, perm[i * STEP_BLOCKS + place]))

    call = pl.pallas_call(
        functools.partial(chunk_kernel, widths),
        grid_spec=pltpu.PrefetchScalarGridSpec(
            num_scalar_prefetch=1,
            grid=(count // STEP_BLOCKS,),
            in_specs=[column_block(j) for j in range(STEP_BLOCKS)] + [whole(right.shape)],
            out_specs=[stepped((STEP_BLOCKS, LANES, size), 0) for size in widths],
        ),
        out_shape=[jax.ShapeDtypeStruct((count, LANES, size), BF16) for size in widths],
        compiler_params=pltpu.CompilerParams(vmem_limit_bytes=VMEM_BYTES),
        cost_estimate=pl.CostEstimate(
            flops=2 * count * LANES * tokens * right.shape[1],
            transcendentals=0,
            bytes_accessed=count * LANES * right.shape[1] * 2,
        ),
        name="chunk_products",
    )
    return call(perm, *([left] * STEP_BLOCKS), right)


def block_orders(lattice, device_count):
    if not lattice:
        numbers = jnp.arange(device_count, dtype=jnp.int32)
        return numbers[: device_count // 2], numbers[device_count // 2 :]
    spot = my_spot()
    dz, dx, dy = (grid.reshape(-1) for grid in np.indices((4, 2, 2)).astype(np.int32))
    chip = (spot["z"] - dz + 4) % 4 * 2 + (spot["x"] + dx) % 2
    orders = []
    for dc in (1, 0):
        core = (spot["core"] + dc) % 2
        orders.append(((chip * 2 + core) * 2 + (spot["y"] + dy) % 2).astype(jnp.int32))
    return orders


def chunk_orders():
    spot = my_spot()
    dz, dx = (grid.reshape(-1) for grid in np.indices((4, 2)).astype(np.int32))
    chip = (spot["z"] - dz + 4) % 4 * 2 + (spot["x"] + dx) % 2
    return [(chip * 2 + (spot["core"] + dc) % 2).astype(jnp.int32) for dc in (1, 0)]


TOKEN_ORDERS = (("x", "y", "z"), ("y", "z", "x"), ("z", "x", "y"))
CHUNK_ORDERS = (("x", "z"), ("z", "x"))


def tokens_home(lattice, partner, own):
    groups = []
    for first, second, order in zip(partner, own, TOKEN_ORDERS):
        if lattice:
            shape = (4, 2, 2) + first.shape[1:]
            groups.append(
                reduce_home(first.reshape(shape), second.reshape(shape), ("z", "x", "y"), order)
            )
        else:
            everything = jnp.concatenate([first, second], axis=0)
            total = lax.psum_scatter(everything, BOTH, scatter_dimension=0, tiled=True)
            groups.append(total[0].astype(F32))
    return groups


def weight_grads_home(lattice, left, right, widths):
    if not lattice:
        product = dot(left, right, 0, 0).astype(BF16)
        return lax.psum_scatter(product, "dp", scatter_dimension=0, tiled=True).astype(F32)
    partner, own = (chunk_products(order, left, right, widths) for order in chunk_orders())
    groups = []
    for first, second, order in zip(partner, own, CHUNK_ORDERS):
        shape = (4, 2) + first.shape[1:]
        groups.append(reduce_home(first.reshape(shape), second.reshape(shape), ("z", "x"), order))
    return jnp.concatenate(groups, axis=1)


def on_device(
    inputs,
    input_gain,
    post_gain,
    query_gain,
    key_gain,
    query_weight,
    key_projection_matrix,
    value_projection_matrix,
    output_weight,
    router_weight,
    gate_weight,
    up_weight,
    down_weight,
    routes,
    cotangent,
):
    dp_count, tensor_count = lax.axis_size("dp"), lax.axis_size("tensor")
    device_count = dp_count * tensor_count
    lattice = is_lattice(dp_count, tensor_count)
    row_count, width = inputs.shape
    experts = router_weight.shape[1]
    experts_here = gate_weight.shape[0]
    capacity = 2 * row_count * routes.shape[1] // experts

    projections = jnp.concatenate(
        [query_weight, key_projection_matrix, value_projection_matrix], axis=0
    )
    query_rows, key_rows = query_weight.shape[0], key_projection_matrix.shape[0]
    projections_full = lax.all_gather(projections, "dp", axis=1, tiled=True)
    output_held, _ = lax.optimization_barrier((output_weight, projections_full[:8, :128]))
    output_full = lax.all_gather(output_held, "dp", axis=0, tiled=True)
    cotangent_held, _ = lax.optimization_barrier((cotangent, output_full[:8, :128]))
    all_grads = lax.all_gather(cotangent_held[None], BOTH, axis=0, tiled=True)
    other_inputs = swap_tensor(inputs)

    expert_ids = jnp.arange(experts, dtype=jnp.int32)
    chosen_mask = jnp.any(routes[:, :, None] == expert_ids[None, None, :], axis=1)
    small = [input_gain, post_gain, query_gain, key_gain]
    sizes = [item.shape[0] for item in small]
    flat = jnp.concatenate(small)
    padded = -(-flat.shape[0] // LANES) * LANES
    flat = jnp.pad(flat, (0, padded - flat.shape[0]))
    router_lines = router_weight.size // LANES
    payload = jnp.concatenate(
        [
            router_weight.reshape(router_lines, LANES),
            flat.reshape(-1, LANES),
            chosen_mask.T.astype(BF16),
        ],
        axis=0,
    )
    gathered = lax.all_gather(payload[None], BOTH, axis=0, tiled=True)
    router_full = gathered[:, :router_lines].reshape(width, experts)
    flat_all = gathered[:, router_lines : router_lines + padded // LANES].reshape(
        device_count, padded
    )
    starts = np.cumsum([0] + sizes)
    input_scale, post_scale, query_scale, key_scale = (
        flat_all[:, starts[n] : starts[n + 1]].reshape(-1).astype(F32) for n in range(4)
    )
    mask_all = gathered[:, router_lines + padded // LANES :]
    first_expert = lax.axis_index("dp") * experts_here
    mask_here = lax.dynamic_slice_in_dim(mask_all, first_expert, experts_here, axis=1)
    earlier = jnp.asarray(np.triu(np.ones((row_count, row_count), np.float32), 1), BF16)
    rank = jnp.einsum("bet,tu->beu", mask_here, earlier, preferred_element_type=F32)
    position = jnp.where(mask_here > 0.5, rank, -1.0)
    orders = block_orders(lattice, device_count)
    positions = [position[order] for order in orders]
    masks = [mask_all[order] for order in orders]
    router_t = router_full.T
    up_both = jnp.concatenate([gate_weight, up_weight], axis=2)
    up_both_t = jnp.swapaxes(up_both, 1, 2)
    down_t = jnp.swapaxes(down_weight, 1, 2)

    both_inputs = in_order(inputs, other_inputs).astype(F32)
    residual_in = inputs.astype(F32)
    sequence = norm_rows(both_inputs, input_scale)[0].astype(BF16)
    _, input_hat, input_inv = norm_rows(residual_in, input_scale)
    seq_len = sequence.shape[0]
    local_heads = query_rows // HEAD_SIZE
    local_groups = key_rows // HEAD_SIZE
    per_group = local_heads // local_groups
    projected = dot(sequence, projections_full, 1, 1)
    query_raw = projected[:, :query_rows].reshape(seq_len, local_heads, HEAD_SIZE)
    key_raw = projected[:, query_rows : query_rows + key_rows].reshape(
        seq_len, local_groups, HEAD_SIZE
    )
    value_low = (
        projected[:, query_rows + key_rows :]
        .astype(BF16)
        .reshape(seq_len, local_groups, HEAD_SIZE)
    )
    cosine_table, sine_table = rope_tables(seq_len, HEAD_SIZE)
    cosine, sine = cosine_table[:, None, :], sine_table[:, None, :]
    query_norm, query_hat, query_inv = norm_rows(query_raw, query_scale)
    query_low = (query_norm * cosine + rotate_half(query_norm) * sine).astype(BF16)
    key_norm, key_hat, key_inv = norm_rows(key_raw, key_scale)
    key_low = (key_norm * cosine + rotate_half(key_norm) * sine).astype(BF16)
    score_scale = 1.0 / math.sqrt(HEAD_SIZE)
    query_groups = query_low.reshape(seq_len, local_groups, per_group, HEAD_SIZE)
    scores = (
        jnp.einsum("qhgd,khd->hgqk", query_groups, key_low, preferred_element_type=F32)
        * score_scale
    )
    row_index = jnp.arange(seq_len, dtype=jnp.int32)
    scores = jnp.where(row_index[None, :] <= row_index[:, None], scores, -1e30)
    attend = jax.nn.softmax(scores, axis=-1)
    attend_low = attend.astype(BF16)
    mixed_low = (
        jnp.einsum("hgqk,khd->qhgd", attend_low, value_low, preferred_element_type=F32)
        .astype(BF16)
        .reshape(seq_len, query_rows)
    )
    residual_mid = residual_in + sum_tokens(dot(mixed_low, output_full, 1, 1))
    post_norm, post_hat, post_inv = norm_rows(residual_mid, post_scale)
    post_low = post_norm.astype(BF16)
    all_tokens = lax.all_gather(post_low[None], BOTH, axis=0, tiled=True)

    logits = dot(post_low, router_full)
    top = jnp.max(jnp.where(chosen_mask, logits, -3e38), axis=-1, keepdims=True)
    powers = jnp.where(chosen_mask, jnp.exp(jnp.minimum(logits - top, 0.0)), 0.0)
    gates = powers / jnp.sum(powers, axis=-1, keepdims=True)

    wide = width // 8 * 3
    widths = (wide, wide, width - 2 * wide + LANES)
    first_scalar = first_expert.astype(jnp.int32).reshape(1)
    results = [
        expert_grads(
            order, first_scalar, all_tokens, all_grads, positions[n], masks[n],
            router_t, up_both, up_both_t, down_t, capacity, widths,
        )
        for n, order in enumerate(orders)
    ]
    home = tokens_home(lattice, results[0][5:], results[1][5:])
    out_widths = (wide, wide, width - 2 * wide)
    outputs = [
        expert_outputs(results[n][2], positions[n], down_weight, capacity, out_widths)
        for n in range(2)
    ]
    rows, grad_rows, gated, grad_gate_pre, grad_up_pre = (
        [results[n][place] for n in range(2)] for place in range(5)
    )

    def slot_product(left, right):
        return sum(
            jnp.einsum("esd,esf->edf", left[n], right[n], preferred_element_type=F32)
            for n in range(2)
        )

    grad_down = slot_product(gated, grad_rows)
    grad_gate_w = slot_product(rows, grad_gate_pre)
    grad_up_w = slot_product(rows, grad_up_pre)
    out_home = jnp.concatenate(tokens_home(lattice, outputs[0], outputs[1]), axis=1)
    result = (residual_mid + out_home).astype(BF16)

    grad_out = cotangent.astype(F32)
    grad_post = jnp.concatenate([home[0], home[1], home[2][:, : width - 2 * wide]], axis=1)
    start = width - 2 * wide
    grad_gates = home[2][:, start : start + experts]
    grad_logits = (
        gates * (grad_gates - jnp.sum(gates * grad_gates, axis=-1, keepdims=True))
    ).astype(BF16)
    grad_post = grad_post + dot(grad_logits, router_full, 1, 1)
    grad_router = dot(post_low, grad_logits, 0, 0)
    grad_mid_norm, post_terms = norm_back(grad_post, post_scale, post_hat, post_inv)
    grad_post_gain = jnp.sum(post_terms, axis=0)
    grad_mid = grad_out + grad_mid_norm
    grad_mid_low = grad_mid.astype(BF16)
    grad_attention = in_order(grad_mid_low, swap_tensor(grad_mid_low))
    early = reduce_small(
        jnp.concatenate(
            [
                grad_router.reshape(device_count, -1),
                grad_post_gain.reshape(device_count, -1),
                jnp.zeros((device_count, LANES - sizes[1]), F32),
            ],
            axis=1,
        ).reshape(device_count, -1, LANES)
    ).reshape(-1)
    grad_router = early[: router_weight.size].reshape(router_weight.shape)
    grad_post_gain = early[router_weight.size : router_weight.size + sizes[1]]

    grad_mixed = dot(grad_attention, output_full).astype(BF16)
    out_split = (query_rows // 8 * 5, query_rows - query_rows // 8 * 5)
    grad_output_w = weight_grads_home(lattice, grad_attention, mixed_low, out_split)
    grad_groups = grad_mixed.reshape(seq_len, local_groups, per_group, HEAD_SIZE)
    grad_attend = jnp.einsum(
        "qhgd,khd->hgqk", grad_groups, value_low, preferred_element_type=F32
    )
    grad_value = jnp.einsum(
        "hgqk,qhgd->khd", attend_low, grad_groups, preferred_element_type=F32
    )
    row_inner = jnp.sum(attend * grad_attend, axis=-1, keepdims=True)
    grad_scores = (attend * (grad_attend - row_inner)).astype(BF16)
    grad_query_rot = (
        jnp.einsum("hgqk,khd->qhgd", grad_scores, key_low, preferred_element_type=F32)
        * score_scale
    ).reshape(seq_len, local_heads, HEAD_SIZE)
    grad_key_rot = (
        jnp.einsum("hgqk,qhgd->khd", grad_scores, query_groups, preferred_element_type=F32)
        * score_scale
    )
    grad_query_norm = grad_query_rot * cosine + rotate_back(grad_query_rot * sine)
    grad_query_raw, query_terms = norm_back(grad_query_norm, query_scale, query_hat, query_inv)
    grad_query_gain = jnp.sum(query_terms, axis=(0, 1))
    grad_key_norm = grad_key_rot * cosine + rotate_back(grad_key_rot * sine)
    grad_key_raw, key_terms = norm_back(grad_key_norm, key_scale, key_hat, key_inv)
    grad_key_gain = jnp.sum(key_terms, axis=(0, 1))
    grad_projected = jnp.concatenate(
        [
            grad_query_raw.reshape(seq_len, query_rows).astype(BF16),
            grad_key_raw.reshape(seq_len, key_rows).astype(BF16),
            grad_value.reshape(seq_len, key_rows).astype(BF16),
        ],
        axis=1,
    )
    total_rows = query_rows + 2 * key_rows
    split = total_rows // LANES * 3 // 5 * LANES
    grad_projections = weight_grads_home(
        lattice, sequence, grad_projected, (split, total_rows - split)
    ).T
    grad_query_w = grad_projections[:query_rows]
    grad_key_w = grad_projections[query_rows : query_rows + key_rows]
    grad_value_w = grad_projections[query_rows + key_rows :]
    grad_normed = sum_tokens(dot(grad_projected, projections_full))
    grad_in_norm, input_terms = norm_back(grad_normed, input_scale, input_hat, input_inv)
    grad_input_gain = jnp.sum(input_terms, axis=0)
    grad_inputs = (grad_mid + grad_in_norm).astype(BF16)
    late_parts = [grad_input_gain, grad_query_gain, grad_key_gain]
    late_sizes = [sizes[0], sizes[2], sizes[3]]
    late = reduce_small(
        jnp.concatenate(
            [part.reshape(device_count, -1) for part in late_parts]
            + [jnp.zeros((device_count, LANES - sum(late_sizes)), F32)],
            axis=1,
        ).reshape(device_count, 1, LANES)
    ).reshape(-1)
    bounds = np.cumsum([0] + late_sizes)
    grad_input_gain, grad_query_gain, grad_key_gain = (
        late[bounds[n] : bounds[n + 1]] for n in range(3)
    )
    return (
        result,
        grad_inputs,
        grad_input_gain,
        grad_post_gain,
        grad_query_gain,
        grad_key_gain,
        grad_query_w,
        grad_key_w,
        grad_value_w,
        grad_output_w,
        grad_router,
        grad_gate_w,
        grad_up_w,
        grad_down,
    )


def solution(mesh):
    return jax.shard_map(
        on_device,
        mesh=mesh,
        in_specs=(
            P(("dp", "tensor"), None),
            P(("dp", "tensor")),
            P(("dp", "tensor")),
            P(("dp", "tensor")),
            P(("dp", "tensor")),
            P("tensor", "dp"),
            P("tensor", "dp"),
            P("tensor", "dp"),
            P("dp", "tensor"),
            P(("dp", "tensor"), None),
            P("dp", None, "tensor"),
            P("dp", None, "tensor"),
            P("dp", "tensor", None),
            P(("dp", "tensor"), None),
            P(("dp", "tensor"), None),
        ),
        out_specs=(
            P(("dp", "tensor"), None),
            P(("dp", "tensor"), None),
            P(("dp", "tensor")),
            P(("dp", "tensor")),
            P(("dp", "tensor")),
            P(("dp", "tensor")),
            P("tensor", "dp"),
            P("tensor", "dp"),
            P("tensor", "dp"),
            P("dp", "tensor"),
            P(("dp", "tensor"), None),
            P("dp", None, "tensor"),
            P("dp", None, "tensor"),
            P("dp", "tensor", None),
        ),
        check_vma=False,
    )
```

```python
import functools
import math

import jax
import jax.numpy as jnp
import numpy as np
from jax import lax
from jax.experimental import pallas as pl
from jax.experimental.pallas import tpu as pltpu
from jax.sharding import PartitionSpec as P

HEAD_SIZE = 128
LANES = 128
EPSILON = 1e-06
ROPE_BASE = 1000000.0
DP = ("chip", "core")
BOTH = ("chip", "core", "tensor")
BF16 = jnp.bfloat16
F32 = jnp.float32
STEP_BLOCKS = 4
VMEM_BYTES = 60 * 1024 * 1024


def norm_rows(values, weights):
    inverse = lax.rsqrt(jnp.mean(values * values, axis=-1, keepdims=True) + EPSILON)
    normalized_rows = values * inverse
    return (normalized_rows * weights, normalized_rows, inverse)


def norm_back(upstream, weights, normalized_rows, inverse):
    scaled = upstream * weights
    inner_term = jnp.mean(scaled * normalized_rows, axis=-1, keepdims=True)
    return (inverse * (scaled - normalized_rows * inner_term), upstream * normalized_rows)


def rope_tables(length, head_width):
    half_width = head_width // 2
    frequency = jnp.exp(
        jnp.arange(half_width, dtype=F32) * (-2.0 * math.log(ROPE_BASE) / head_width)
    )
    angles = jnp.arange(length, dtype=F32)[:, None] * frequency[None, :]
    angles = jnp.concatenate([angles, angles], axis=-1)
    return (jnp.cos(angles), jnp.sin(angles))


def rotate_half(values):
    half_width = values.shape[-1] // 2
    return jnp.concatenate([-values[..., half_width:], values[..., :half_width]], axis=-1)


def rotate_back(values):
    half_width = values.shape[-1] // 2
    return jnp.concatenate([values[..., half_width:], -values[..., :half_width]], axis=-1)


def dot(left, right, left_dim=1, right_dim=0):
    return lax.dot_general(
        left, right, (((left_dim,), (right_dim,)), ((), ())), preferred_element_type=F32
    )


LATTICE = {"z": 4, "x": 2, "core": 2, "y": 2}


def is_lattice(dp_count, tensor_count):
    return dp_count == 16 and tensor_count == 2


def hop(values, axis, step=1):
    sizes = tuple(LATTICE.values())
    place = list(LATTICE).index(axis)
    pairs = []
    for source in range(math.prod(sizes)):
        spot = list(np.unravel_index(source, sizes))
        spot[place] = (spot[place] + step) % sizes[place]
        pairs.append((source, int(np.ravel_multi_index(spot, sizes))))
    return lax.ppermute(values, BOTH, pairs)


def my_spot():
    chip_core = lax.axis_index(DP)
    return {
        "z": chip_core // 4,
        "x": (chip_core // 2) % 2,
        "core": chip_core % 2,
        "y": lax.axis_index("tensor"),
    }


def add_low(first, second):
    return (first.astype(F32) + second.astype(F32)).astype(BF16)


class Pending:
    def __init__(self, *parts):
        self.parts = parts

    def total(self):
        return sum(part.astype(F32) for part in self.parts)

    def piece(self, place, dim):
        picked = [lax.index_in_dim(part, place, dim, keepdims=False) for part in self.parts]
        return Pending(*picked).total().astype(BF16)


def after(values, others):
    return lax.optimization_barrier((values, others))[0]


class Links:
    def __init__(self):
        self.active = []

    def add(self, *jobs):
        places = [[None] for _ in jobs]
        for job, place in zip(jobs, places):
            self.advance(job, place, None)
        return places

    def advance(self, job, place, arrived):
        try:
            self.active.append((job, place, job.send(arrived)))
        except StopIteration as stop:
            place[0] = stop.value

    def round(self, work=None, *operands):
        sending, self.active = self.active, []
        sent = [array for _, _, sends in sending for array, _ in sends]
        result = None
        if sent:
            sent = list(lax.optimization_barrier(tuple(sent)))
        moves = [move for _, _, sends in sending for _, move in sends]
        arrived = [move(array) for move, array in zip(moves, sent)]
        if work is not None:
            result = work(*(after(operands, sent) if sent else operands))
            arrived, result = lax.optimization_barrier((arrived, result))
        for job, place, sends in sending:
            self.advance(job, place, arrived[: len(sends)])
            arrived = arrived[len(sends) :]
        return result

    def finish(self):
        while self.active:
            self.round()


def mover(axis, step=1):
    return lambda values: hop(values, axis, step)


def home_job(partner, own, axes, order, turn):
    axes = list(axes)
    if partner is None:
        pending = own
    else:
        (received,) = yield [(partner, mover("core"))]
        pending = Pending(own, received)
    for axis in order:
        dim = axes.index(axis)
        axes.remove(axis)
        if axis == "z":
            (received,) = yield [(pending.piece(2, dim), mover("z", turn))]
            near = {-1: pending.piece(1, dim), 1: pending.piece(3, dim)}
            near[turn] = add_low(near[turn], received)
            arrived = yield [(near[step], mover("z", step)) for step in (-1, 1)]
        else:
            arrived = yield [(pending.piece(1, dim), mover(axis))]
        pending = Pending(pending.piece(0, dim), *arrived)
    return pending.total()


def spread_job(own, order, turn):
    pieces = own[None, None, None]
    for axis in order:
        dim = ("z", "x", "y").index(axis)
        if axis == "z":
            near = yield [(pieces, mover("z", 1)), (pieces, mover("z", -1))]
            (far,) = yield [(near[0 if turn == 1 else 1], mover("z", turn))]
            pieces = jnp.concatenate([pieces, near[0], far, near[1]], axis=dim)
        else:
            (other,) = yield [(pieces, mover(axis))]
            pieces = jnp.concatenate([pieces, other], axis=dim)
    flat = pieces.reshape((-1,) + own.shape)
    (partner,) = yield [(flat, mover("core"))]
    return partner, flat


def flip(bits):
    count = lax.axis_size(BOTH)
    return lambda values: lax.ppermute(
        values, BOTH, [(source, source ^ bits) for source in range(count)]
    )


def gather_small_job(values):
    device_count = lax.axis_size(BOTH)
    number = lax.axis_index(BOTH)
    everything = jnp.zeros((device_count,) + values.shape, values.dtype)
    everything = lax.dynamic_update_index_in_dim(everything, values, number, 0)
    bit = 1
    while bit < device_count:
        fan = min(4, device_count // bit)
        start = number // bit * bit
        sent = lax.dynamic_slice_in_dim(everything, start, bit, 0)
        arrived = yield [(sent, flip(k * bit)) for k in range(1, fan)]
        for k, received in enumerate(arrived, 1):
            everything = lax.dynamic_update_slice_in_dim(
                everything, received, start ^ (k * bit), 0
            )
        bit *= fan
    return everything


def reduce_small_job(values):
    number = lax.axis_index(BOTH)
    count = values.shape[0]
    while count > 1:
        fan = min(4, count)
        bit = count // fan
        parts = values.reshape((fan, bit) + values.shape[1:])
        mine = (number // bit) % fan
        pick = lambda place: lax.dynamic_index_in_dim(parts, place, 0, keepdims=False)
        arrived = yield [(pick(mine ^ k), flip(k * bit)) for k in range(1, fan)]
        values = sum(arrived, pick(mine))
        count = bit
    return values[0]


def swap_tensor(values):
    return lax.ppermute(values, "tensor", [(0, 1), (1, 0)])


def swap_job(values):
    (received,) = yield [(values, swap_tensor)]
    return received


def in_order(mine, other):
    first = lax.axis_index("tensor") == 0
    return jnp.where(
        first, jnp.concatenate([mine, other], axis=0), jnp.concatenate([other, mine], axis=0)
    )


def sum_tokens_job(terms):
    low = terms.astype(BF16).reshape((2, terms.shape[0] // 2) + terms.shape[1:])
    half = lax.axis_index("tensor")
    sent = lax.dynamic_index_in_dim(low, 1 - half, 0, keepdims=False)
    kept = lax.dynamic_index_in_dim(low, half, 0, keepdims=False)
    (received,) = yield [(sent, swap_tensor)]
    return kept.astype(F32) + received.astype(F32)


def choose(position_row, capacity):
    slot = lax.broadcasted_iota(jnp.int32, (capacity, position_row.shape[1]), 0).astype(F32)
    picks = [
        (slot == position_row[e : e + 1, :]).astype(F32) for e in range(position_row.shape[0])
    ]
    return picks


def expert_kernel(capacity, widths, grad_groups, carried, perm, first, *refs):
    blocks = STEP_BLOCKS
    token_refs, grad_refs, refs = (
        refs[:blocks],
        refs[blocks : blocks + grad_groups],
        refs[blocks + grad_groups :],
    )
    position_ref, mask_ref, router_ref, up_ref, up_t_ref, down_t_ref = refs[:6]
    refs = refs[6 + carried :]
    rows_ref, grad_rows_ref, gated_ref, grad_gate_ref, grad_up_ref = refs[:5]
    out_refs, packed_ref = refs[5:-1], refs[-1]
    experts_here = up_ref.shape[0]
    hidden_units = down_t_ref.shape[2]
    width = token_refs[0].shape[2]
    first_expert = first[0]
    gates = [[] for _ in range(experts_here)]
    choices = []
    for j in range(blocks):
        tokens = token_refs[j][0]
        picks = choose(position_ref[j], capacity)
        choice = jnp.concatenate(picks, axis=0).astype(BF16)
        choices.append(choice)
        rows = dot(choice, tokens).astype(BF16)
        grad_rows = [dot(choice, grad_ref[j]).astype(BF16) for grad_ref in grad_refs]
        logits = dot(router_ref[...], tokens, 1, 1)
        chosen = mask_ref[j].astype(F32) > 0.5
        top = jnp.max(jnp.where(chosen, logits, -3e38), axis=0, keepdims=True)
        powers = jnp.where(chosen, jnp.exp(jnp.minimum(logits - top, 0.0)), 0.0)
        gate_all = powers / jnp.sum(powers, axis=0, keepdims=True)
        expert_number = lax.broadcasted_iota(jnp.int32, gate_all.shape, 0)
        for e in range(experts_here):
            here = slice(j * capacity, (j + 1) * capacity)
            rows_ref[e, here, :] = rows[e * capacity : (e + 1) * capacity]
            start = 0
            for group in grad_rows:
                grad_rows_ref[e, here, start : start + group.shape[1]] = group[
                    e * capacity : (e + 1) * capacity
                ]
                start += group.shape[1]
            gate_row = jnp.sum(
                jnp.where(expert_number == first_expert + e, gate_all, 0.0), axis=0, keepdims=True
            )
            gates[e].append(jnp.sum(picks[e] * gate_row, axis=1, keepdims=True))
    for e in range(experts_here):
        both = dot(rows_ref[e], up_ref[e])
        gate_pre = both[:, :hidden_units]
        up_pre = both[:, hidden_units:]
        raw = dot(grad_rows_ref[e], down_t_ref[e])
        sigmoid = 1.0 / (1.0 + jnp.exp(-gate_pre))
        silu = gate_pre * sigmoid
        hidden = silu * up_pre
        gate = jnp.concatenate(gates[e], axis=0)
        grad_gate = jnp.sum(hidden * raw, axis=1, keepdims=True)
        grad_hidden = gate * raw
        grad_gate_pre = (
            grad_hidden * up_pre * sigmoid * (1.0 + gate_pre * (1.0 - sigmoid))
        ).astype(BF16)
        grad_up_pre = (grad_hidden * silu).astype(BF16)
        gated_ref[e] = (gate * hidden).astype(BF16)
        grad_gate_ref[e] = grad_gate_pre
        grad_up_ref[e] = grad_up_pre
        back = dot(grad_gate_pre, up_t_ref[e, :hidden_units, :]) + dot(
            grad_up_pre, up_t_ref[e, hidden_units:, :]
        )
        lane = lax.broadcasted_iota(jnp.int32, (blocks * capacity, LANES), 1)
        extra = jnp.where(lane == first_expert + e, grad_gate, 0.0).astype(BF16)
        back = back.astype(BF16)
        for j in range(blocks):
            packed_ref[j, e * capacity : (e + 1) * capacity, :width] = back[
                j * capacity : (j + 1) * capacity
            ]
            packed_ref[j, e * capacity : (e + 1) * capacity, width:] = extra[
                j * capacity : (j + 1) * capacity
            ]
    for j in range(blocks):
        home = dot(choices[j], packed_ref[j], 0, 0).astype(BF16)
        start = 0
        for out_ref, size in zip(out_refs, widths):
            out_ref[j] = home[:, start : start + size]
            start += size


def block_spec(width, place):
    return pl.BlockSpec(
        (1, LANES, width), lambda i, perm, first: (perm[i * STEP_BLOCKS + place], 0, 0)
    )


def whole(shape):
    return pl.BlockSpec(
        shape, lambda i, *scalars: (0,) * len(shape), pipeline_mode=pl.Buffered(1)
    )


def stepped(shape, dim):
    return pl.BlockSpec(
        shape, lambda i, *scalars: tuple(i if d == dim else 0 for d in range(len(shape)))
    )


def expert_grads(
    half, carry, perm, first, tokens, grads, grad_start, position, mask,
    router_t, up_both, up_both_t, down_t, capacity, widths,
):
    count = perm.shape[0]
    width = tokens.shape[2]
    experts_here, hidden_units = down_t.shape[0], down_t.shape[2]
    slots = STEP_BLOCKS * capacity
    expert_count = router_t.shape[0]
    slot_shape = lambda size: jax.ShapeDtypeStruct((experts_here, 2 * count * capacity, size), BF16)
    steps = count // STEP_BLOCKS
    slot_spec = lambda size: pl.BlockSpec(
        (experts_here, slots, size), lambda i, *scalars: (0, i + half * steps, 0)
    )
    before = 2 + STEP_BLOCKS + len(grads) + 6
    flops = 2 * count * capacity * experts_here * (7 * hidden_units * width + 3 * LANES * width)
    call = pl.pallas_call(
        functools.partial(expert_kernel, capacity, widths, len(grads), len(carry)),
        grid_spec=pltpu.PrefetchScalarGridSpec(
            num_scalar_prefetch=2,
            grid=(count // STEP_BLOCKS,),
            in_specs=[block_spec(width, j) for j in range(STEP_BLOCKS)]
            + [
                pl.BlockSpec(
                    (STEP_BLOCKS, LANES, group.shape[2]),
                    lambda i, *scalars: (i + grad_start // STEP_BLOCKS, 0, 0),
                )
                for group in grads
            ]
            + [
                stepped((STEP_BLOCKS, experts_here, LANES), 0),
                stepped((STEP_BLOCKS, expert_count, LANES), 0),
                whole(router_t.shape),
                whole(up_both.shape),
                whole(up_both_t.shape),
                whole(down_t.shape),
            ]
            + [pl.BlockSpec(memory_space=pl.ANY)] * len(carry),
            out_specs=[slot_spec(width)] * 2
            + [slot_spec(hidden_units)] * 3
            + [stepped((STEP_BLOCKS, LANES, size), 0) for size in widths],
            scratch_shapes=[
                pltpu.VMEM((STEP_BLOCKS, experts_here * capacity, sum(widths)), BF16)
            ],
        ),
        out_shape=[slot_shape(width)] * 2
        + [slot_shape(hidden_units)] * 3
        + [jax.ShapeDtypeStruct((count, LANES, size), BF16) for size in widths],
        compiler_params=pltpu.CompilerParams(vmem_limit_bytes=VMEM_BYTES),
        cost_estimate=pl.CostEstimate(
            flops=flops, transcendentals=0, bytes_accessed=6 * count * LANES * width * 2
        ),
        input_output_aliases={before + n: n for n in range(len(carry))},
        name="expert_grads",
    )
    return call(
        perm, first, *([tokens] * STEP_BLOCKS), *grads,
        position, mask, router_t, up_both, up_both_t, down_t, *carry,
    )


def output_kernel(capacity, widths, gated_ref, position_ref, down_ref, *refs):
    out_refs, packed_ref = refs[:-1], refs[-1]
    for e in range(down_ref.shape[0]):
        rows = dot(gated_ref[e], down_ref[e]).astype(BF16)
        for j in range(STEP_BLOCKS):
            packed_ref[j, e * capacity : (e + 1) * capacity, :] = rows[
                j * capacity : (j + 1) * capacity
            ]
    for j in range(STEP_BLOCKS):
        choice = jnp.concatenate(choose(position_ref[j], capacity), axis=0).astype(BF16)
        home = dot(choice, packed_ref[j], 0, 0).astype(BF16)
        start = 0
        for out_ref, size in zip(out_refs, widths):
            out_ref[j] = home[:, start : start + size]
            start += size


def expert_outputs(half, gated, position, down, capacity, widths):
    count = position.shape[0]
    experts_here, hidden_units, width = down.shape
    slots = STEP_BLOCKS * capacity
    steps = count // STEP_BLOCKS
    call = pl.pallas_call(
        functools.partial(output_kernel, capacity, widths),
        grid=(steps,),
        in_specs=[
            pl.BlockSpec(
                (experts_here, slots, hidden_units), lambda i: (0, i + half * steps, 0)
            ),
            stepped((STEP_BLOCKS, experts_here, LANES), 0),
            whole(down.shape),
        ],
        out_specs=[stepped((STEP_BLOCKS, LANES, size), 0) for size in widths],
        out_shape=[jax.ShapeDtypeStruct((count, LANES, size), BF16) for size in widths],
        scratch_shapes=[pltpu.VMEM((STEP_BLOCKS, experts_here * capacity, width), BF16)],
        compiler_params=pltpu.CompilerParams(vmem_limit_bytes=VMEM_BYTES),
        cost_estimate=pl.CostEstimate(
            flops=2 * count * capacity * experts_here * (hidden_units * width + LANES * width),
            transcendentals=0,
            bytes_accessed=2 * count * LANES * width * 2,
        ),
        name="expert_outputs",
    )
    return call(gated, position, down)


def chunk_kernel(widths, perm, *refs):
    left = jnp.concatenate([ref[...] for ref in refs[:STEP_BLOCKS]], axis=1)
    product = dot(left, refs[STEP_BLOCKS][...], 0, 0).astype(BF16)
    start = 0
    for out_ref, size in zip(refs[STEP_BLOCKS + 1 :], widths):
        for j in range(STEP_BLOCKS):
            out_ref[j] = product[j * LANES : (j + 1) * LANES, start : start + size]
        start += size


def chunk_products(perm, left, right, widths):
    count = perm.shape[0]
    tokens = left.shape[0]

    def column_block(place):
        return pl.BlockSpec((tokens, LANES), lambda i, perm: (0, perm[i * STEP_BLOCKS + place]))

    call = pl.pallas_call(
        functools.partial(chunk_kernel, widths),
        grid_spec=pltpu.PrefetchScalarGridSpec(
            num_scalar_prefetch=1,
            grid=(count // STEP_BLOCKS,),
            in_specs=[column_block(j) for j in range(STEP_BLOCKS)] + [whole(right.shape)],
            out_specs=[stepped((STEP_BLOCKS, LANES, size), 0) for size in widths],
        ),
        out_shape=[jax.ShapeDtypeStruct((count, LANES, size), BF16) for size in widths],
        compiler_params=pltpu.CompilerParams(vmem_limit_bytes=VMEM_BYTES),
        cost_estimate=pl.CostEstimate(
            flops=2 * count * LANES * tokens * right.shape[1],
            transcendentals=0,
            bytes_accessed=count * LANES * right.shape[1] * 2,
        ),
        name="chunk_products",
    )
    return call(perm, *([left] * STEP_BLOCKS), right)


def block_orders(lattice, device_count):
    if not lattice:
        numbers = jnp.arange(device_count, dtype=jnp.int32)
        return numbers[: device_count // 2], numbers[device_count // 2 :]
    spot = my_spot()
    dz, dx, dy = (grid.reshape(-1) for grid in np.indices((4, 2, 2)).astype(np.int32))
    chip = (spot["z"] - dz + 4) % 4 * 2 + (spot["x"] + dx) % 2
    orders = []
    for dc in (1, 0):
        core = (spot["core"] + dc) % 2
        orders.append(((chip * 2 + core) * 2 + (spot["y"] + dy) % 2).astype(jnp.int32))
    return orders


def chunk_orders():
    spot = my_spot()
    dz, dx = (grid.reshape(-1) for grid in np.indices((4, 2)).astype(np.int32))
    chip = (spot["z"] - dz + 4) % 4 * 2 + (spot["x"] + dx) % 2
    return [(chip * 2 + (spot["core"] + dc) % 2).astype(jnp.int32) for dc in (1, 0)]


TOKEN_ORDERS = (("x", "y", "z"), ("y", "z", "x"), ("z", "x", "y"))
GATHER_ORDERS = (("z", "y", "x"), ("x", "z", "y"), ("y", "x", "z"))
CHUNK_ORDERS = (("x", "z"), ("z", "x"))
TURNS = (1, -1, 1)


def scatter_job(partner, own):
    everything = jnp.concatenate([partner, own], axis=0)
    total = lax.psum_scatter(everything, BOTH, scatter_dimension=0, tiled=True)
    return total[0].astype(F32)
    yield


def tokens_home_jobs(lattice, partner, own, received=None):
    jobs = []
    for n, order in enumerate(TOKEN_ORDERS):
        if not lattice:
            jobs.append(scatter_job(partner[n], own[n]))
            continue
        shape = (4, 2, 2) + own[n].shape[1:]
        mine = own[n].reshape(shape)
        if received is None:
            jobs.append(home_job(partner[n].reshape(shape), mine, "zxy", order, TURNS[n]))
        else:
            both = Pending(mine, received[n].reshape(shape))
            jobs.append(home_job(None, both, "zxy", order, TURNS[n]))
    return jobs


def product_job(left, right):
    product = dot(left, right, 0, 0).astype(BF16)
    return lax.psum_scatter(product, DP, scatter_dimension=0, tiled=True).astype(F32)
    yield


def weight_grads_chunks(lattice, left, right, widths):
    if not lattice:
        return left, right
    return tuple(chunk_products(order, left, right, widths) for order in chunk_orders())


def weight_grads_jobs(lattice, first, second):
    if not lattice:
        return [product_job(first, second)]
    jobs = []
    for n, order in enumerate(CHUNK_ORDERS):
        shape = (4, 2) + first[n].shape[1:]
        jobs.append(
            home_job(first[n].reshape(shape), second[n].reshape(shape), "zx", order, TURNS[n])
        )
    return jobs


def on_device(
    inputs,
    input_gain,
    post_gain,
    query_gain,
    key_gain,
    query_weight,
    key_projection_matrix,
    value_projection_matrix,
    output_weight,
    router_weight,
    gate_weight,
    up_weight,
    down_weight,
    routes,
    cotangent,
):
    dp_count, tensor_count = lax.axis_size(DP), lax.axis_size("tensor")
    device_count = dp_count * tensor_count
    lattice = is_lattice(dp_count, tensor_count)
    row_count, width = inputs.shape
    experts = router_weight.shape[1]
    experts_here = gate_weight.shape[0]
    capacity = 2 * row_count * routes.shape[1] // experts

    links = Links()
    projections = jnp.concatenate(
        [query_weight, key_projection_matrix, value_projection_matrix], axis=0
    )
    query_rows, key_rows = query_weight.shape[0], key_projection_matrix.shape[0]
    projections_full = lax.all_gather(projections, DP, axis=1, tiled=True)

    expert_ids = jnp.arange(experts, dtype=jnp.int32)
    chosen_mask = jnp.any(routes[:, :, None] == expert_ids[None, None, :], axis=1)
    small = [input_gain, post_gain, query_gain, key_gain]
    sizes = [item.shape[0] for item in small]
    flat = jnp.concatenate(small)
    padded = -(-flat.shape[0] // LANES) * LANES
    flat = jnp.pad(flat, (0, padded - flat.shape[0]))
    router_lines = router_weight.size // LANES
    payload = jnp.concatenate(
        [
            router_weight.reshape(router_lines, LANES),
            flat.reshape(-1, LANES),
            chosen_mask.T.astype(BF16),
        ],
        axis=0,
    )
    gathered_at, other_inputs_at = links.add(gather_small_job(payload), swap_job(inputs))
    if lattice:
        cuts = (width // 8 * 3, width // 16 * 11)
        grad_at = links.add(
            *(
                spread_job(group, order, turn)
                for group, order, turn in zip(
                    jnp.split(cotangent, cuts, axis=1), GATHER_ORDERS, TURNS
                )
            )
        )

    def join_up(gate, up):
        return jnp.concatenate([gate, up], axis=2)

    def turn_last(values):
        return jnp.swapaxes(values, 1, 2)

    up_both = links.round(join_up, gate_weight, up_weight)
    output_held = after(output_weight, up_both[0, :8, :LANES])
    output_full = lax.all_gather(output_held, DP, axis=0, tiled=True)
    up_both_t = links.round(turn_last, up_both)
    down_t = links.round(turn_last, down_weight)
    other_inputs, gathered = other_inputs_at[0], None
    while gathered_at[0] is None:
        links.round()
    gathered = gathered_at[0]

    router_full = gathered[:, :router_lines].reshape(width, experts)
    flat_all = gathered[:, router_lines : router_lines + padded // LANES].reshape(
        device_count, padded
    )
    starts = np.cumsum([0] + sizes)
    input_scale, post_scale, query_scale, key_scale = (
        flat_all[:, starts[n] : starts[n + 1]].reshape(-1).astype(F32) for n in range(4)
    )
    mask_all = gathered[:, router_lines + padded // LANES :]
    first_expert = lax.axis_index(DP) * experts_here
    mask_here = lax.dynamic_slice_in_dim(mask_all, first_expert, experts_here, axis=1)
    earlier = jnp.asarray(np.triu(np.ones((row_count, row_count), np.float32), 1), BF16)
    rank = jnp.einsum("bet,tu->beu", mask_here, earlier, preferred_element_type=F32)
    position = jnp.where(mask_here > 0.5, rank, -1.0)
    orders = block_orders(lattice, device_count)
    positions = [position[order] for order in orders]
    masks = [mask_all[order] for order in orders]
    router_t = router_full.T

    both_inputs = in_order(inputs, other_inputs).astype(F32)
    residual_in = inputs.astype(F32)
    sequence = norm_rows(both_inputs, input_scale)[0].astype(BF16)
    _, input_hat, input_inv = norm_rows(residual_in, input_scale)
    seq_len = sequence.shape[0]
    local_heads = query_rows // HEAD_SIZE
    local_groups = key_rows // HEAD_SIZE
    per_group = local_heads // local_groups
    cosine_table, sine_table = rope_tables(seq_len, HEAD_SIZE)
    cosine, sine = cosine_table[:, None, :], sine_table[:, None, :]
    score_scale = 1.0 / math.sqrt(HEAD_SIZE)

    def attention(projections_full):
        projected = dot(sequence, projections_full, 1, 1)
        query_raw = projected[:, :query_rows].reshape(seq_len, local_heads, HEAD_SIZE)
        key_raw = projected[:, query_rows : query_rows + key_rows].reshape(
            seq_len, local_groups, HEAD_SIZE
        )
        value_low = (
            projected[:, query_rows + key_rows :]
            .astype(BF16)
            .reshape(seq_len, local_groups, HEAD_SIZE)
        )
        query_norm, query_hat, query_inv = norm_rows(query_raw, query_scale)
        query_low = (query_norm * cosine + rotate_half(query_norm) * sine).astype(BF16)
        key_norm, key_hat, key_inv = norm_rows(key_raw, key_scale)
        key_low = (key_norm * cosine + rotate_half(key_norm) * sine).astype(BF16)
        query_groups = query_low.reshape(seq_len, local_groups, per_group, HEAD_SIZE)
        scores = (
            jnp.einsum("qhgd,khd->hgqk", query_groups, key_low, preferred_element_type=F32)
            * score_scale
        )
        row_index = jnp.arange(seq_len, dtype=jnp.int32)
        scores = jnp.where(row_index[None, :] <= row_index[:, None], scores, -1e30)
        attend = jax.nn.softmax(scores, axis=-1)
        attend_low = attend.astype(BF16)
        mixed_low = (
            jnp.einsum("hgqk,khd->qhgd", attend_low, value_low, preferred_element_type=F32)
            .astype(BF16)
            .reshape(seq_len, query_rows)
        )
        return (
            query_hat, query_inv, query_groups, key_hat, key_inv, key_low, value_low,
            attend, attend_low, mixed_low, projections_full,
        )

    (
        query_hat, query_inv, query_groups, key_hat, key_inv, key_low, value_low,
        attend, attend_low, mixed_low, projections_full,
    ) = links.round(attention, projections_full)
    mixed_out = links.round(lambda mixed: dot(mixed, output_full, 1, 1), mixed_low)
    links.finish()
    if lattice:
        all_grads = [[place[0][n] for place in grad_at] for n in range(2)]
        grad_starts = (0, 0)
    else:
        all_grads = ([lax.all_gather(cotangent[None], BOTH, axis=0, tiled=True)],) * 2
        grad_starts = (0, device_count // 2)
    (mixed_home,) = links.add(sum_tokens_job(mixed_out))
    links.finish()
    residual_mid = residual_in + mixed_home[0]
    post_norm, post_hat, post_inv = norm_rows(residual_mid, post_scale)
    post_low = post_norm.astype(BF16)
    all_tokens = lax.all_gather(post_low[None], BOTH, axis=0, tiled=True)

    logits = dot(post_low, router_full)
    top = jnp.max(jnp.where(chosen_mask, logits, -3e38), axis=-1, keepdims=True)
    powers = jnp.where(chosen_mask, jnp.exp(jnp.minimum(logits - top, 0.0)), 0.0)
    gates = powers / jnp.sum(powers, axis=-1, keepdims=True)

    wide = width // 8 * 3
    widths = (wide, wide, width - 2 * wide + LANES)
    first_scalar = first_expert.astype(jnp.int32).reshape(1)

    def half_grads(half, carry):
        return expert_grads(
            half, carry, orders[half], first_scalar, all_tokens, all_grads[half],
            grad_starts[half], positions[half], masks[half],
            router_t, up_both, up_both_t, down_t, capacity, widths,
        )

    results = half_grads(0, ())
    partner = results[5:]
    received = [hop(group, "core") for group in partner] if lattice else None
    results = half_grads(1, results[:5])
    rows, grad_rows, gated, grad_gate_pre, grad_up_pre = results[:5]
    own = results[5:]

    def slot_product(left, right):
        return jnp.einsum("esd,esf->edf", left, right, preferred_element_type=F32)

    out_widths = (wide, wide, width - 2 * wide)

    def outputs(gated):
        return [
            expert_outputs(n, gated, positions[n], down_weight, capacity, out_widths)
            for n in range(2)
        ]

    home = links.add(*tokens_home_jobs(lattice, partner, own, received))
    out_parts = links.round(outputs, gated)
    grad_gate_w = links.round(slot_product, rows, grad_gate_pre)
    grad_down = links.round(slot_product, gated, grad_rows)
    links.finish()
    home = [place[0] for place in home]

    grad_out = cotangent.astype(F32)
    grad_post = jnp.concatenate([home[0], home[1], home[2][:, : width - 2 * wide]], axis=1)
    start = width - 2 * wide
    grad_gates = home[2][:, start : start + experts]
    grad_logits = (
        gates * (grad_gates - jnp.sum(gates * grad_gates, axis=-1, keepdims=True))
    ).astype(BF16)
    grad_post = grad_post + dot(grad_logits, router_full, 1, 1)
    grad_mid_norm, post_terms = norm_back(grad_post, post_scale, post_hat, post_inv)
    grad_mid = grad_out + grad_mid_norm
    grad_mid_low = grad_mid.astype(BF16)
    out_home = links.add(*tokens_home_jobs(lattice, *out_parts))
    (other_grads,) = links.add(swap_job(grad_mid_low))
    grad_up_w = links.round(slot_product, rows, grad_up_pre)
    grad_attention = in_order(grad_mid_low, other_grads[0])

    out_split = (query_rows // 8 * 3, query_rows - query_rows // 8 * 3)

    def back_scores(grad_attention):
        grad_mixed = dot(grad_attention, output_full).astype(BF16)
        chunks = weight_grads_chunks(lattice, grad_attention, mixed_low, out_split)
        grad_groups = grad_mixed.reshape(seq_len, local_groups, per_group, HEAD_SIZE)
        grad_attend = jnp.einsum(
            "qhgd,khd->hgqk", grad_groups, value_low, preferred_element_type=F32
        )
        row_inner = jnp.sum(attend * grad_attend, axis=-1, keepdims=True)
        grad_scores = (attend * (grad_attend - row_inner)).astype(BF16)
        return grad_groups, grad_scores, chunks

    grad_groups, grad_scores, chunks = links.round(back_scores, grad_attention)
    grad_output_at = links.add(*weight_grads_jobs(lattice, *chunks))
    grad_router = dot(post_low, grad_logits, 0, 0)
    grad_post_gain = jnp.sum(post_terms, axis=0)
    (early,) = links.add(
        reduce_small_job(
            jnp.concatenate(
                [
                    grad_router.reshape(device_count, -1),
                    grad_post_gain.reshape(device_count, -1),
                    jnp.zeros((device_count, LANES - sizes[1]), F32),
                ],
                axis=1,
            ).reshape(device_count, -1, LANES)
        )
    )

    def back_heads(grad_groups, grad_scores):
        grad_value = jnp.einsum(
            "hgqk,qhgd->khd", attend_low, grad_groups, preferred_element_type=F32
        )
        grad_key_rot = (
            jnp.einsum("hgqk,qhgd->khd", grad_scores, query_groups, preferred_element_type=F32)
            * score_scale
        )
        grad_query_rot = (
            jnp.einsum("hgqk,khd->qhgd", grad_scores, key_low, preferred_element_type=F32)
            * score_scale
        ).reshape(seq_len, local_heads, HEAD_SIZE)
        return grad_value, grad_key_rot, grad_query_rot

    grad_value, grad_key_rot, grad_query_rot = links.round(back_heads, grad_groups, grad_scores)

    def back_norms(grad_value, grad_key_rot, grad_query_rot):
        grad_query_norm = grad_query_rot * cosine + rotate_back(grad_query_rot * sine)
        grad_query_raw, query_terms = norm_back(grad_query_norm, query_scale, query_hat, query_inv)
        grad_query_gain = jnp.sum(query_terms, axis=(0, 1))
        grad_key_norm = grad_key_rot * cosine + rotate_back(grad_key_rot * sine)
        grad_key_raw, key_terms = norm_back(grad_key_norm, key_scale, key_hat, key_inv)
        grad_key_gain = jnp.sum(key_terms, axis=(0, 1))
        grad_projected = jnp.concatenate(
            [
                grad_query_raw.reshape(seq_len, query_rows).astype(BF16),
                grad_key_raw.reshape(seq_len, key_rows).astype(BF16),
                grad_value.reshape(seq_len, key_rows).astype(BF16),
            ],
            axis=1,
        )
        return grad_projected, grad_query_gain, grad_key_gain

    grad_projected, grad_query_gain, grad_key_gain = links.round(
        back_norms, grad_value, grad_key_rot, grad_query_rot
    )
    total_rows = query_rows + 2 * key_rows
    split = total_rows // LANES * 2 // 5 * LANES
    chunks = weight_grads_chunks(
        lattice, sequence, grad_projected, (split, total_rows - split)
    )
    grad_projections_at = links.add(*weight_grads_jobs(lattice, *chunks))
    normed_parts = links.round(
        lambda grad: dot(grad, projections_full), grad_projected
    )
    (grad_normed,) = links.add(sum_tokens_job(normed_parts))
    links.round()
    grad_in_norm, input_terms = norm_back(grad_normed[0], input_scale, input_hat, input_inv)
    grad_input_gain = jnp.sum(input_terms, axis=0)
    grad_inputs = (grad_mid + grad_in_norm).astype(BF16)
    late_parts = [grad_input_gain, grad_query_gain, grad_key_gain]
    late_sizes = [sizes[0], sizes[2], sizes[3]]
    (late,) = links.add(
        reduce_small_job(
            jnp.concatenate(
                [part.reshape(device_count, -1) for part in late_parts]
                + [jnp.zeros((device_count, LANES - sum(late_sizes)), F32)],
                axis=1,
            ).reshape(device_count, 1, LANES)
        )
    )
    links.finish()
    result = (residual_mid + jnp.concatenate([p[0] for p in out_home], axis=1)).astype(BF16)
    early, late = early[0].reshape(-1), late[0].reshape(-1)
    grad_router = early[: router_weight.size].reshape(router_weight.shape)
    grad_post_gain = early[router_weight.size : router_weight.size + sizes[1]]
    grad_output_w = jnp.concatenate([place[0] for place in grad_output_at], axis=1)
    grad_projections = jnp.concatenate([place[0] for place in grad_projections_at], axis=1).T
    grad_query_w = grad_projections[:query_rows]
    grad_key_w = grad_projections[query_rows : query_rows + key_rows]
    grad_value_w = grad_projections[query_rows + key_rows :]
    bounds = np.cumsum([0] + late_sizes)
    grad_input_gain, grad_query_gain, grad_key_gain = (
        late[bounds[n] : bounds[n + 1]] for n in range(3)
    )
    return (
        result,
        grad_inputs,
        grad_input_gain,
        grad_post_gain,
        grad_query_gain,
        grad_key_gain,
        grad_query_w,
        grad_key_w,
        grad_value_w,
        grad_output_w,
        grad_router,
        grad_gate_w,
        grad_up_w,
        grad_down,
    )


def solution(mesh):
    dp_count, tensor_count = mesh.devices.shape
    split = jax.sharding.Mesh(
        mesh.devices.reshape(dp_count // 2, 2, tensor_count), ("chip", "core", "tensor")
    )
    tokens, line = P(BOTH, None), P(BOTH)
    gated = P(DP, None, "tensor")
    weights = (P("tensor", DP),) * 3 + (P(DP, "tensor"), tokens, gated, gated, P(DP, "tensor", None))
    return jax.shard_map(
        on_device,
        mesh=split,
        in_specs=(tokens,) + (line,) * 4 + weights + (tokens, tokens),
        out_specs=(tokens, tokens) + (line,) * 4 + weights,
        check_vma=False,
    )
```

```python
import functools
import math

import jax
import jax.numpy as jnp
import numpy as np
from jax import lax
from jax.experimental import pallas as pl
from jax.experimental.pallas import tpu as pltpu
from jax.sharding import PartitionSpec as P

HEAD_SIZE = 128
LANES = 128
EPSILON = 1e-06
ROPE_BASE = 1000000.0
DP = ("chip", "core")
BOTH = ("chip", "core", "tensor")
BF16 = jnp.bfloat16
F32 = jnp.float32
STEP_BLOCKS = 4
VMEM_BYTES = 60 * 1024 * 1024


def norm_rows(values, weights):
    inverse = lax.rsqrt(jnp.mean(values * values, axis=-1, keepdims=True) + EPSILON)
    normalized_rows = values * inverse
    return (normalized_rows * weights, normalized_rows, inverse)


def norm_back(upstream, weights, normalized_rows, inverse):
    scaled = upstream * weights
    inner_term = jnp.mean(scaled * normalized_rows, axis=-1, keepdims=True)
    return (inverse * (scaled - normalized_rows * inner_term), upstream * normalized_rows)


def rope_tables(length, head_width):
    half_width = head_width // 2
    frequency = jnp.exp(
        jnp.arange(half_width, dtype=F32) * (-2.0 * math.log(ROPE_BASE) / head_width)
    )
    angles = jnp.arange(length, dtype=F32)[:, None] * frequency[None, :]
    angles = jnp.concatenate([angles, angles], axis=-1)
    return (jnp.cos(angles), jnp.sin(angles))


def rotate_half(values):
    half_width = values.shape[-1] // 2
    return jnp.concatenate([-values[..., half_width:], values[..., :half_width]], axis=-1)


def rotate_back(values):
    half_width = values.shape[-1] // 2
    return jnp.concatenate([values[..., half_width:], -values[..., :half_width]], axis=-1)


def dot(left, right, left_dim=1, right_dim=0):
    return lax.dot_general(
        left, right, (((left_dim,), (right_dim,)), ((), ())), preferred_element_type=F32
    )


LATTICE = {"z": 4, "x": 2, "core": 2, "y": 2}


def is_lattice(dp_count, tensor_count):
    return dp_count == 16 and tensor_count == 2


def hop(values, axis, step=1):
    sizes = tuple(LATTICE.values())
    place = list(LATTICE).index(axis)
    pairs = []
    for source in range(math.prod(sizes)):
        spot = list(np.unravel_index(source, sizes))
        spot[place] = (spot[place] + step) % sizes[place]
        pairs.append((source, int(np.ravel_multi_index(spot, sizes))))
    return lax.ppermute(values, BOTH, pairs)


def my_spot():
    chip_core = lax.axis_index(DP)
    return {
        "z": chip_core // 4,
        "x": (chip_core // 2) % 2,
        "core": chip_core % 2,
        "y": lax.axis_index("tensor"),
    }


def add_low(first, second):
    return (first.astype(F32) + second.astype(F32)).astype(BF16)


class Pending:
    def __init__(self, *parts):
        self.parts = parts

    def total(self):
        return sum(part.astype(F32) for part in self.parts)

    def piece(self, place, dim):
        picked = [lax.index_in_dim(part, place, dim, keepdims=False) for part in self.parts]
        return Pending(*picked).total().astype(BF16)


def after(values, others):
    return lax.optimization_barrier((values, others))[0]


class Links:
    def __init__(self):
        self.active = []
        self.marks = []

    def add(self, *jobs):
        places = [[None] for _ in jobs]
        for job, place in zip(jobs, places):
            self.advance(job, place, None)
        return places

    def advance(self, job, place, arrived):
        try:
            sends = job.send(arrived)
        except StopIteration as stop:
            place[0] = stop.value
            return
        sent = lax.optimization_barrier(tuple(array for array, _ in sends))
        self.marks += sent
        moved = [move(array) for (_, move), array in zip(sends, sent)]
        self.active.append((job, place, moved))

    def round(self, work=None, *operands):
        moving, self.active = self.active, []
        result = None
        if work is not None:
            result = work(*(after(operands, self.marks) if self.marks else operands))
            self.marks = jax.tree.leaves(result)[:1]
        for job, place, moved in moving:
            if self.marks:
                moved = after(moved, self.marks)
            self.marks = []
            self.advance(job, place, moved)
        return result

    def finish(self):
        while self.active:
            self.round()


def mover(axis, step=1):
    return lambda values: hop(values, axis, step)


def home_job(partner, own, axes, order, turn):
    axes = list(axes)
    if partner is None:
        pending = own
    else:
        (received,) = yield [(partner, mover("core"))]
        pending = Pending(own, received)
    for axis in order:
        dim = axes.index(axis)
        axes.remove(axis)
        if axis == "z":
            (received,) = yield [(pending.piece(2, dim), mover("z", turn))]
            near = {-1: pending.piece(1, dim), 1: pending.piece(3, dim)}
            near[turn] = add_low(near[turn], received)
            arrived = yield [(near[step], mover("z", step)) for step in (-1, 1)]
        else:
            arrived = yield [(pending.piece(1, dim), mover(axis))]
        pending = Pending(pending.piece(0, dim), *arrived)
    return pending.total()


def spread_job(own, order, turn):
    pieces = own[None, None, None]
    for axis in order:
        dim = ("z", "x", "y").index(axis)
        if axis == "z":
            near = yield [(pieces, mover("z", 1)), (pieces, mover("z", -1))]
            (far,) = yield [(near[0 if turn == 1 else 1], mover("z", turn))]
            pieces = jnp.concatenate([pieces, near[0], far, near[1]], axis=dim)
        else:
            (other,) = yield [(pieces, mover(axis))]
            pieces = jnp.concatenate([pieces, other], axis=dim)
    flat = pieces.reshape((-1,) + own.shape)
    (partner,) = yield [(flat, mover("core"))]
    return partner, flat


def flip(bits):
    count = lax.axis_size(BOTH)
    return lambda values: lax.ppermute(
        values, BOTH, [(source, source ^ bits) for source in range(count)]
    )


def gather_small_job(values):
    device_count = lax.axis_size(BOTH)
    number = lax.axis_index(BOTH)
    everything = jnp.zeros((device_count,) + values.shape, values.dtype)
    everything = lax.dynamic_update_index_in_dim(everything, values, number, 0)
    bit = 1
    while bit < device_count:
        fan = min(4, device_count // bit)
        start = number // bit * bit
        sent = lax.dynamic_slice_in_dim(everything, start, bit, 0)
        arrived = yield [(sent, flip(k * bit)) for k in range(1, fan)]
        for k, received in enumerate(arrived, 1):
            everything = lax.dynamic_update_slice_in_dim(
                everything, received, start ^ (k * bit), 0
            )
        bit *= fan
    return everything


def reduce_small_job(values):
    number = lax.axis_index(BOTH)
    count = values.shape[0]
    while count > 1:
        fan = min(4, count)
        bit = count // fan
        parts = values.reshape((fan, bit) + values.shape[1:])
        mine = (number // bit) % fan
        pick = lambda place: lax.dynamic_index_in_dim(parts, place, 0, keepdims=False)
        arrived = yield [(pick(mine ^ k), flip(k * bit)) for k in range(1, fan)]
        values = sum(arrived, pick(mine))
        count = bit
    return values[0]


def swap_tensor(values):
    return lax.ppermute(values, "tensor", [(0, 1), (1, 0)])


def swap_job(values):
    (received,) = yield [(values, swap_tensor)]
    return received


def in_order(mine, other):
    first = lax.axis_index("tensor") == 0
    return jnp.where(
        first, jnp.concatenate([mine, other], axis=0), jnp.concatenate([other, mine], axis=0)
    )


def sum_tokens_job(terms):
    low = terms.astype(BF16).reshape((2, terms.shape[0] // 2) + terms.shape[1:])
    half = lax.axis_index("tensor")
    sent = lax.dynamic_index_in_dim(low, 1 - half, 0, keepdims=False)
    kept = lax.dynamic_index_in_dim(low, half, 0, keepdims=False)
    (received,) = yield [(sent, swap_tensor)]
    return kept.astype(F32) + received.astype(F32)


def choose(position_row, capacity):
    slot = lax.broadcasted_iota(jnp.int32, (capacity, position_row.shape[1]), 0).astype(F32)
    picks = [
        (slot == position_row[e : e + 1, :]).astype(F32) for e in range(position_row.shape[0])
    ]
    return picks


def expert_kernel(capacity, widths, grad_groups, carried, perm, first, *refs):
    blocks = STEP_BLOCKS
    token_refs, grad_refs, refs = (
        refs[:blocks],
        refs[blocks : blocks + grad_groups],
        refs[blocks + grad_groups :],
    )
    position_ref, mask_ref, router_ref, up_ref, up_t_ref, down_t_ref = refs[:6]
    refs = refs[6 + carried :]
    rows_ref, grad_rows_ref, gated_ref, grad_gate_ref, grad_up_ref = refs[:5]
    out_refs, packed_ref = refs[5:-1], refs[-1]
    experts_here = up_ref.shape[0]
    hidden_units = down_t_ref.shape[2]
    width = token_refs[0].shape[2]
    first_expert = first[0]
    gates = [[] for _ in range(experts_here)]
    choices = []
    for j in range(blocks):
        tokens = token_refs[j][0]
        picks = choose(position_ref[j], capacity)
        choice = jnp.concatenate(picks, axis=0).astype(BF16)
        choices.append(choice)
        rows = dot(choice, tokens).astype(BF16)
        grad_rows = [dot(choice, grad_ref[j]).astype(BF16) for grad_ref in grad_refs]
        logits = dot(router_ref[...], tokens, 1, 1)
        chosen = mask_ref[j].astype(F32) > 0.5
        top = jnp.max(jnp.where(chosen, logits, -3e38), axis=0, keepdims=True)
        powers = jnp.where(chosen, jnp.exp(jnp.minimum(logits - top, 0.0)), 0.0)
        gate_all = powers / jnp.sum(powers, axis=0, keepdims=True)
        expert_number = lax.broadcasted_iota(jnp.int32, gate_all.shape, 0)
        for e in range(experts_here):
            here = slice(j * capacity, (j + 1) * capacity)
            rows_ref[e, here, :] = rows[e * capacity : (e + 1) * capacity]
            start = 0
            for group in grad_rows:
                grad_rows_ref[e, here, start : start + group.shape[1]] = group[
                    e * capacity : (e + 1) * capacity
                ]
                start += group.shape[1]
            gate_row = jnp.sum(
                jnp.where(expert_number == first_expert + e, gate_all, 0.0), axis=0, keepdims=True
            )
            gates[e].append(jnp.sum(picks[e] * gate_row, axis=1, keepdims=True))
    for e in range(experts_here):
        both = dot(rows_ref[e], up_ref[e])
        gate_pre = both[:, :hidden_units]
        up_pre = both[:, hidden_units:]
        raw = dot(grad_rows_ref[e], down_t_ref[e])
        sigmoid = 1.0 / (1.0 + jnp.exp(-gate_pre))
        silu = gate_pre * sigmoid
        hidden = silu * up_pre
        gate = jnp.concatenate(gates[e], axis=0)
        grad_gate = jnp.sum(hidden * raw, axis=1, keepdims=True)
        grad_hidden = gate * raw
        grad_gate_pre = (
            grad_hidden * up_pre * sigmoid * (1.0 + gate_pre * (1.0 - sigmoid))
        ).astype(BF16)
        grad_up_pre = (grad_hidden * silu).astype(BF16)
        gated_ref[e] = (gate * hidden).astype(BF16)
        grad_gate_ref[e] = grad_gate_pre
        grad_up_ref[e] = grad_up_pre
        back = dot(grad_gate_pre, up_t_ref[e, :hidden_units, :]) + dot(
            grad_up_pre, up_t_ref[e, hidden_units:, :]
        )
        lane = lax.broadcasted_iota(jnp.int32, (blocks * capacity, LANES), 1)
        extra = jnp.where(lane == first_expert + e, grad_gate, 0.0).astype(BF16)
        back = back.astype(BF16)
        for j in range(blocks):
            packed_ref[j, e * capacity : (e + 1) * capacity, :width] = back[
                j * capacity : (j + 1) * capacity
            ]
            packed_ref[j, e * capacity : (e + 1) * capacity, width:] = extra[
                j * capacity : (j + 1) * capacity
            ]
    for j in range(blocks):
        home = dot(choices[j], packed_ref[j], 0, 0).astype(BF16)
        start = 0
        for out_ref, size in zip(out_refs, widths):
            out_ref[j] = home[:, start : start + size]
            start += size


def block_spec(width, place):
    return pl.BlockSpec(
        (1, LANES, width), lambda i, perm, first: (perm[i * STEP_BLOCKS + place], 0, 0)
    )


def whole(shape):
    return pl.BlockSpec(
        shape, lambda i, *scalars: (0,) * len(shape), pipeline_mode=pl.Buffered(1)
    )


def stepped(shape, dim):
    return pl.BlockSpec(
        shape, lambda i, *scalars: tuple(i if d == dim else 0 for d in range(len(shape)))
    )


def expert_grads(
    half, carry, perm, first, tokens, grads, grad_start, position, mask,
    router_t, up_both, up_both_t, down_t, capacity, widths,
):
    count = perm.shape[0]
    width = tokens.shape[2]
    experts_here, hidden_units = down_t.shape[0], down_t.shape[2]
    slots = STEP_BLOCKS * capacity
    expert_count = router_t.shape[0]
    slot_shape = lambda size: jax.ShapeDtypeStruct((experts_here, 2 * count * capacity, size), BF16)
    steps = count // STEP_BLOCKS
    slot_spec = lambda size: pl.BlockSpec(
        (experts_here, slots, size), lambda i, *scalars: (0, i + half * steps, 0)
    )
    before = 2 + STEP_BLOCKS + len(grads) + 6
    flops = 2 * count * capacity * experts_here * (7 * hidden_units * width + 3 * LANES * width)
    call = pl.pallas_call(
        functools.partial(expert_kernel, capacity, widths, len(grads), len(carry)),
        grid_spec=pltpu.PrefetchScalarGridSpec(
            num_scalar_prefetch=2,
            grid=(count // STEP_BLOCKS,),
            in_specs=[block_spec(width, j) for j in range(STEP_BLOCKS)]
            + [
                pl.BlockSpec(
                    (STEP_BLOCKS, LANES, group.shape[2]),
                    lambda i, *scalars: (i + grad_start // STEP_BLOCKS, 0, 0),
                )
                for group in grads
            ]
            + [
                stepped((STEP_BLOCKS, experts_here, LANES), 0),
                stepped((STEP_BLOCKS, expert_count, LANES), 0),
                whole(router_t.shape),
                whole(up_both.shape),
                whole(up_both_t.shape),
                whole(down_t.shape),
            ]
            + [pl.BlockSpec(memory_space=pl.ANY)] * len(carry),
            out_specs=[slot_spec(width)] * 2
            + [slot_spec(hidden_units)] * 3
            + [stepped((STEP_BLOCKS, LANES, size), 0) for size in widths],
            scratch_shapes=[
                pltpu.VMEM((STEP_BLOCKS, experts_here * capacity, sum(widths)), BF16)
            ],
        ),
        out_shape=[slot_shape(width)] * 2
        + [slot_shape(hidden_units)] * 3
        + [jax.ShapeDtypeStruct((count, LANES, size), BF16) for size in widths],
        compiler_params=pltpu.CompilerParams(vmem_limit_bytes=VMEM_BYTES),
        cost_estimate=pl.CostEstimate(
            flops=flops, transcendentals=0, bytes_accessed=6 * count * LANES * width * 2
        ),
        input_output_aliases={before + n: n for n in range(len(carry))},
        name="expert_grads",
    )
    return call(
        perm, first, *([tokens] * STEP_BLOCKS), *grads,
        position, mask, router_t, up_both, up_both_t, down_t, *carry,
    )


def output_kernel(capacity, widths, gated_ref, position_ref, down_ref, *refs):
    out_refs, packed_ref = refs[:-1], refs[-1]
    for e in range(down_ref.shape[0]):
        rows = dot(gated_ref[e], down_ref[e]).astype(BF16)
        for j in range(STEP_BLOCKS):
            packed_ref[j, e * capacity : (e + 1) * capacity, :] = rows[
                j * capacity : (j + 1) * capacity
            ]
    for j in range(STEP_BLOCKS):
        choice = jnp.concatenate(choose(position_ref[j], capacity), axis=0).astype(BF16)
        home = dot(choice, packed_ref[j], 0, 0).astype(BF16)
        start = 0
        for out_ref, size in zip(out_refs, widths):
            out_ref[j] = home[:, start : start + size]
            start += size


def expert_outputs(half, gated, position, down, capacity, widths):
    count = position.shape[0]
    experts_here, hidden_units, width = down.shape
    slots = STEP_BLOCKS * capacity
    steps = count // STEP_BLOCKS
    call = pl.pallas_call(
        functools.partial(output_kernel, capacity, widths),
        grid=(steps,),
        in_specs=[
            pl.BlockSpec(
                (experts_here, slots, hidden_units), lambda i: (0, i + half * steps, 0)
            ),
            stepped((STEP_BLOCKS, experts_here, LANES), 0),
            whole(down.shape),
        ],
        out_specs=[stepped((STEP_BLOCKS, LANES, size), 0) for size in widths],
        out_shape=[jax.ShapeDtypeStruct((count, LANES, size), BF16) for size in widths],
        scratch_shapes=[pltpu.VMEM((STEP_BLOCKS, experts_here * capacity, width), BF16)],
        compiler_params=pltpu.CompilerParams(vmem_limit_bytes=VMEM_BYTES),
        cost_estimate=pl.CostEstimate(
            flops=2 * count * capacity * experts_here * (hidden_units * width + LANES * width),
            transcendentals=0,
            bytes_accessed=2 * count * LANES * width * 2,
        ),
        name="expert_outputs",
    )
    return call(gated, position, down)


def chunk_kernel(widths, perm, *refs):
    left = jnp.concatenate([ref[...] for ref in refs[:STEP_BLOCKS]], axis=1)
    product = dot(left, refs[STEP_BLOCKS][...], 0, 0).astype(BF16)
    start = 0
    for out_ref, size in zip(refs[STEP_BLOCKS + 1 :], widths):
        for j in range(STEP_BLOCKS):
            out_ref[j] = product[j * LANES : (j + 1) * LANES, start : start + size]
        start += size


def chunk_products(perm, left, right, widths):
    count = perm.shape[0]
    tokens = left.shape[0]

    def column_block(place):
        return pl.BlockSpec((tokens, LANES), lambda i, perm: (0, perm[i * STEP_BLOCKS + place]))

    call = pl.pallas_call(
        functools.partial(chunk_kernel, widths),
        grid_spec=pltpu.PrefetchScalarGridSpec(
            num_scalar_prefetch=1,
            grid=(count // STEP_BLOCKS,),
            in_specs=[column_block(j) for j in range(STEP_BLOCKS)] + [whole(right.shape)],
            out_specs=[stepped((STEP_BLOCKS, LANES, size), 0) for size in widths],
        ),
        out_shape=[jax.ShapeDtypeStruct((count, LANES, size), BF16) for size in widths],
        compiler_params=pltpu.CompilerParams(vmem_limit_bytes=VMEM_BYTES),
        cost_estimate=pl.CostEstimate(
            flops=2 * count * LANES * tokens * right.shape[1],
            transcendentals=0,
            bytes_accessed=count * LANES * right.shape[1] * 2,
        ),
        name="chunk_products",
    )
    return call(perm, *([left] * STEP_BLOCKS), right)


def block_orders(lattice, device_count):
    if not lattice:
        numbers = jnp.arange(device_count, dtype=jnp.int32)
        return numbers[: device_count // 2], numbers[device_count // 2 :]
    spot = my_spot()
    dz, dx, dy = (grid.reshape(-1) for grid in np.indices((4, 2, 2)).astype(np.int32))
    chip = (spot["z"] - dz + 4) % 4 * 2 + (spot["x"] + dx) % 2
    orders = []
    for dc in (1, 0):
        core = (spot["core"] + dc) % 2
        orders.append(((chip * 2 + core) * 2 + (spot["y"] + dy) % 2).astype(jnp.int32))
    return orders


def chunk_orders():
    spot = my_spot()
    dz, dx = (grid.reshape(-1) for grid in np.indices((4, 2)).astype(np.int32))
    chip = (spot["z"] - dz + 4) % 4 * 2 + (spot["x"] + dx) % 2
    return [(chip * 2 + (spot["core"] + dc) % 2).astype(jnp.int32) for dc in (1, 0)]


TOKEN_ORDERS = (("x", "y", "z"), ("y", "z", "x"), ("z", "x", "y"))
GATHER_ORDERS = (("z", "y", "x"), ("x", "z", "y"), ("y", "x", "z"))
CHUNK_ORDERS = (("x", "z"), ("z", "x"))
TURNS = (1, -1, 1)


def scatter_job(partner, own):
    everything = jnp.concatenate([partner, own], axis=0)
    total = lax.psum_scatter(everything, BOTH, scatter_dimension=0, tiled=True)
    return total[0].astype(F32)
    yield


def tokens_home_jobs(lattice, partner, own, received=None):
    jobs = []
    for n, order in enumerate(TOKEN_ORDERS):
        if not lattice:
            jobs.append(scatter_job(partner[n], own[n]))
            continue
        shape = (4, 2, 2) + own[n].shape[1:]
        mine = own[n].reshape(shape)
        if received is None:
            jobs.append(home_job(partner[n].reshape(shape), mine, "zxy", order, TURNS[n]))
        else:
            both = Pending(mine, received[n].reshape(shape))
            jobs.append(home_job(None, both, "zxy", order, TURNS[n]))
    return jobs


def product_job(left, right):
    product = dot(left, right, 0, 0).astype(BF16)
    return lax.psum_scatter(product, DP, scatter_dimension=0, tiled=True).astype(F32)
    yield


def weight_grads_chunks(lattice, left, right, widths):
    if not lattice:
        return left, right
    return tuple(chunk_products(order, left, right, widths) for order in chunk_orders())


def weight_grads_jobs(lattice, first, second):
    if not lattice:
        return [product_job(first, second)]
    jobs = []
    for n, order in enumerate(CHUNK_ORDERS):
        shape = (4, 2) + first[n].shape[1:]
        jobs.append(
            home_job(first[n].reshape(shape), second[n].reshape(shape), "zx", order, TURNS[n])
        )
    return jobs


def on_device(
    inputs,
    input_gain,
    post_gain,
    query_gain,
    key_gain,
    query_weight,
    key_projection_matrix,
    value_projection_matrix,
    output_weight,
    router_weight,
    gate_weight,
    up_weight,
    down_weight,
    routes,
    cotangent,
):
    dp_count, tensor_count = lax.axis_size(DP), lax.axis_size("tensor")
    device_count = dp_count * tensor_count
    lattice = is_lattice(dp_count, tensor_count)
    row_count, width = inputs.shape
    experts = router_weight.shape[1]
    experts_here = gate_weight.shape[0]
    capacity = 2 * row_count * routes.shape[1] // experts

    links = Links()
    projections = jnp.concatenate(
        [query_weight, key_projection_matrix, value_projection_matrix], axis=0
    )
    query_rows, key_rows = query_weight.shape[0], key_projection_matrix.shape[0]
    projections_full = lax.all_gather(projections, DP, axis=1, tiled=True)

    expert_ids = jnp.arange(experts, dtype=jnp.int32)
    chosen_mask = jnp.any(routes[:, :, None] == expert_ids[None, None, :], axis=1)
    small = [input_gain, post_gain, query_gain, key_gain]
    sizes = [item.shape[0] for item in small]
    flat = jnp.concatenate(small)
    padded = -(-flat.shape[0] // LANES) * LANES
    flat = jnp.pad(flat, (0, padded - flat.shape[0]))
    router_lines = router_weight.size // LANES
    payload = jnp.concatenate(
        [
            router_weight.reshape(router_lines, LANES),
            flat.reshape(-1, LANES),
            chosen_mask.T.astype(BF16),
        ],
        axis=0,
    )
    gathered_at, other_inputs_at = links.add(gather_small_job(payload), swap_job(inputs))
    if lattice:
        cuts = (width // 8 * 3, width // 16 * 11)
        grad_at = links.add(
            *(
                spread_job(group, order, turn)
                for group, order, turn in zip(
                    jnp.split(cotangent, cuts, axis=1), GATHER_ORDERS, TURNS
                )
            )
        )

    def join_up(gate, up):
        return jnp.concatenate([gate, up], axis=2)

    def turn_last(values):
        return jnp.swapaxes(values, 1, 2)

    up_both = links.round(join_up, gate_weight, up_weight)
    output_held = after(output_weight, up_both[0, :8, :LANES])
    output_full = lax.all_gather(output_held, DP, axis=0, tiled=True)
    up_both_t = links.round(turn_last, up_both)
    down_t = links.round(turn_last, down_weight)
    other_inputs, gathered = other_inputs_at[0], None
    while gathered_at[0] is None:
        links.round()
    gathered = gathered_at[0]

    router_full = gathered[:, :router_lines].reshape(width, experts)
    flat_all = gathered[:, router_lines : router_lines + padded // LANES].reshape(
        device_count, padded
    )
    starts = np.cumsum([0] + sizes)
    input_scale, post_scale, query_scale, key_scale = (
        flat_all[:, starts[n] : starts[n + 1]].reshape(-1).astype(F32) for n in range(4)
    )
    mask_all = gathered[:, router_lines + padded // LANES :]
    first_expert = lax.axis_index(DP) * experts_here
    mask_here = lax.dynamic_slice_in_dim(mask_all, first_expert, experts_here, axis=1)
    earlier = jnp.asarray(np.triu(np.ones((row_count, row_count), np.float32), 1), BF16)
    rank = jnp.einsum("bet,tu->beu", mask_here, earlier, preferred_element_type=F32)
    position = jnp.where(mask_here > 0.5, rank, -1.0)
    orders = block_orders(lattice, device_count)
    positions = [position[order] for order in orders]
    masks = [mask_all[order] for order in orders]
    router_t = router_full.T

    both_inputs = in_order(inputs, other_inputs).astype(F32)
    residual_in = inputs.astype(F32)
    sequence = norm_rows(both_inputs, input_scale)[0].astype(BF16)
    _, input_hat, input_inv = norm_rows(residual_in, input_scale)
    seq_len = sequence.shape[0]
    local_heads = query_rows // HEAD_SIZE
    local_groups = key_rows // HEAD_SIZE
    per_group = local_heads // local_groups
    cosine_table, sine_table = rope_tables(seq_len, HEAD_SIZE)
    cosine, sine = cosine_table[:, None, :], sine_table[:, None, :]
    score_scale = 1.0 / math.sqrt(HEAD_SIZE)

    def attention(projections_full):
        projected = dot(sequence, projections_full, 1, 1)
        query_raw = projected[:, :query_rows].reshape(seq_len, local_heads, HEAD_SIZE)
        key_raw = projected[:, query_rows : query_rows + key_rows].reshape(
            seq_len, local_groups, HEAD_SIZE
        )
        value_low = (
            projected[:, query_rows + key_rows :]
            .astype(BF16)
            .reshape(seq_len, local_groups, HEAD_SIZE)
        )
        query_norm, query_hat, query_inv = norm_rows(query_raw, query_scale)
        query_low = (query_norm * cosine + rotate_half(query_norm) * sine).astype(BF16)
        key_norm, key_hat, key_inv = norm_rows(key_raw, key_scale)
        key_low = (key_norm * cosine + rotate_half(key_norm) * sine).astype(BF16)
        query_groups = query_low.reshape(seq_len, local_groups, per_group, HEAD_SIZE)
        scores = (
            jnp.einsum("qhgd,khd->hgqk", query_groups, key_low, preferred_element_type=F32)
            * score_scale
        )
        row_index = jnp.arange(seq_len, dtype=jnp.int32)
        scores = jnp.where(row_index[None, :] <= row_index[:, None], scores, -1e30)
        attend = jax.nn.softmax(scores, axis=-1)
        attend_low = attend.astype(BF16)
        mixed_low = (
            jnp.einsum("hgqk,khd->qhgd", attend_low, value_low, preferred_element_type=F32)
            .astype(BF16)
            .reshape(seq_len, query_rows)
        )
        return (
            query_hat, query_inv, query_groups, key_hat, key_inv, key_low, value_low,
            attend, attend_low, mixed_low, projections_full,
        )

    (
        query_hat, query_inv, query_groups, key_hat, key_inv, key_low, value_low,
        attend, attend_low, mixed_low, projections_full,
    ) = links.round(attention, projections_full)
    mixed_out = links.round(lambda mixed: dot(mixed, output_full, 1, 1), mixed_low)
    links.finish()
    if lattice:
        all_grads = [[place[0][n] for place in grad_at] for n in range(2)]
        grad_starts = (0, 0)
    else:
        all_grads = ([lax.all_gather(cotangent[None], BOTH, axis=0, tiled=True)],) * 2
        grad_starts = (0, device_count // 2)
    (mixed_home,) = links.add(sum_tokens_job(mixed_out))
    links.finish()
    residual_mid = residual_in + mixed_home[0]
    post_norm, post_hat, post_inv = norm_rows(residual_mid, post_scale)
    post_low = post_norm.astype(BF16)
    all_tokens = lax.all_gather(post_low[None], BOTH, axis=0, tiled=True)

    logits = dot(post_low, router_full)
    top = jnp.max(jnp.where(chosen_mask, logits, -3e38), axis=-1, keepdims=True)
    powers = jnp.where(chosen_mask, jnp.exp(jnp.minimum(logits - top, 0.0)), 0.0)
    gates = powers / jnp.sum(powers, axis=-1, keepdims=True)

    wide = width // 8 * 3
    widths = (wide, wide, width - 2 * wide + LANES)
    first_scalar = first_expert.astype(jnp.int32).reshape(1)

    def half_grads(half, carry):
        return expert_grads(
            half, carry, orders[half], first_scalar, all_tokens, all_grads[half],
            grad_starts[half], positions[half], masks[half],
            router_t, up_both, up_both_t, down_t, capacity, widths,
        )

    results = half_grads(0, ())
    partner = results[5:]
    received = [hop(group, "core") for group in partner] if lattice else None
    results = half_grads(1, results[:5])
    rows, grad_rows, gated, grad_gate_pre, grad_up_pre = results[:5]
    own = results[5:]

    def slot_product(left, right):
        return jnp.einsum("esd,esf->edf", left, right, preferred_element_type=F32)

    out_widths = (wide, wide, width - 2 * wide)

    def outputs(gated):
        return [
            expert_outputs(n, gated, positions[n], down_weight, capacity, out_widths)
            for n in range(2)
        ]

    home = links.add(*tokens_home_jobs(lattice, partner, own, received))
    out_parts = links.round(outputs, gated)
    grad_gate_w = links.round(slot_product, rows, grad_gate_pre)
    grad_down = links.round(slot_product, gated, grad_rows)
    links.finish()
    home = [place[0] for place in home]

    grad_out = cotangent.astype(F32)
    grad_post = jnp.concatenate([home[0], home[1], home[2][:, : width - 2 * wide]], axis=1)
    start = width - 2 * wide
    grad_gates = home[2][:, start : start + experts]
    grad_logits = (
        gates * (grad_gates - jnp.sum(gates * grad_gates, axis=-1, keepdims=True))
    ).astype(BF16)
    grad_post = grad_post + dot(grad_logits, router_full, 1, 1)
    grad_mid_norm, post_terms = norm_back(grad_post, post_scale, post_hat, post_inv)
    grad_mid = grad_out + grad_mid_norm
    grad_mid_low = grad_mid.astype(BF16)
    out_home = links.add(*tokens_home_jobs(lattice, *out_parts))
    (other_grads,) = links.add(swap_job(grad_mid_low))
    grad_up_w = links.round(slot_product, rows, grad_up_pre)
    grad_attention = in_order(grad_mid_low, other_grads[0])

    out_split = (query_rows // 8 * 3, query_rows - query_rows // 8 * 3)

    def back_scores(grad_attention):
        grad_mixed = dot(grad_attention, output_full).astype(BF16)
        chunks = weight_grads_chunks(lattice, grad_attention, mixed_low, out_split)
        grad_groups = grad_mixed.reshape(seq_len, local_groups, per_group, HEAD_SIZE)
        grad_attend = jnp.einsum(
            "qhgd,khd->hgqk", grad_groups, value_low, preferred_element_type=F32
        )
        row_inner = jnp.sum(attend * grad_attend, axis=-1, keepdims=True)
        grad_scores = (attend * (grad_attend - row_inner)).astype(BF16)
        return grad_groups, grad_scores, chunks

    grad_groups, grad_scores, chunks = links.round(back_scores, grad_attention)
    grad_output_at = links.add(*weight_grads_jobs(lattice, *chunks))
    grad_router = dot(post_low, grad_logits, 0, 0)
    grad_post_gain = jnp.sum(post_terms, axis=0)
    def back_heads(grad_groups, grad_scores):
        grad_value = jnp.einsum(
            "hgqk,qhgd->khd", attend_low, grad_groups, preferred_element_type=F32
        )
        grad_key_rot = (
            jnp.einsum("hgqk,qhgd->khd", grad_scores, query_groups, preferred_element_type=F32)
            * score_scale
        )
        grad_query_rot = (
            jnp.einsum("hgqk,khd->qhgd", grad_scores, key_low, preferred_element_type=F32)
            * score_scale
        ).reshape(seq_len, local_heads, HEAD_SIZE)
        return grad_value, grad_key_rot, grad_query_rot

    grad_value, grad_key_rot, grad_query_rot = links.round(back_heads, grad_groups, grad_scores)

    def back_norms(grad_value, grad_key_rot, grad_query_rot):
        grad_query_norm = grad_query_rot * cosine + rotate_back(grad_query_rot * sine)
        grad_query_raw, query_terms = norm_back(grad_query_norm, query_scale, query_hat, query_inv)
        grad_query_gain = jnp.sum(query_terms, axis=(0, 1))
        grad_key_norm = grad_key_rot * cosine + rotate_back(grad_key_rot * sine)
        grad_key_raw, key_terms = norm_back(grad_key_norm, key_scale, key_hat, key_inv)
        grad_key_gain = jnp.sum(key_terms, axis=(0, 1))
        grad_projected = jnp.concatenate(
            [
                grad_query_raw.reshape(seq_len, query_rows).astype(BF16),
                grad_key_raw.reshape(seq_len, key_rows).astype(BF16),
                grad_value.reshape(seq_len, key_rows).astype(BF16),
            ],
            axis=1,
        )
        return grad_projected, grad_query_gain, grad_key_gain

    grad_projected, grad_query_gain, grad_key_gain = links.round(
        back_norms, grad_value, grad_key_rot, grad_query_rot
    )
    total_rows = query_rows + 2 * key_rows
    split = total_rows // LANES * 2 // 5 * LANES
    chunks = weight_grads_chunks(
        lattice, sequence, grad_projected, (split, total_rows - split)
    )
    grad_projections_at = links.add(*weight_grads_jobs(lattice, *chunks))
    normed_parts = links.round(
        lambda grad: dot(grad, projections_full), grad_projected
    )
    (grad_normed,) = links.add(sum_tokens_job(normed_parts))
    links.round()
    grad_in_norm, input_terms = norm_back(grad_normed[0], input_scale, input_hat, input_inv)
    grad_input_gain = jnp.sum(input_terms, axis=0)
    grad_inputs = (grad_mid + grad_in_norm).astype(BF16)
    late_parts = [grad_router, grad_post_gain, grad_input_gain, grad_query_gain, grad_key_gain]
    flat = jnp.concatenate([part.reshape(device_count, -1) for part in late_parts], axis=1)
    flat = jnp.pad(flat, ((0, 0), (0, -flat.shape[1] % LANES)))
    (late,) = links.add(reduce_small_job(flat.reshape(device_count, -1, LANES)))
    links.finish()
    result = (residual_mid + jnp.concatenate([p[0] for p in out_home], axis=1)).astype(BF16)
    grad_output_w = jnp.concatenate([place[0] for place in grad_output_at], axis=1)
    grad_projections = jnp.concatenate([place[0] for place in grad_projections_at], axis=1).T
    grad_query_w = grad_projections[:query_rows]
    grad_key_w = grad_projections[query_rows : query_rows + key_rows]
    grad_value_w = grad_projections[query_rows + key_rows :]
    bounds = np.cumsum([0, router_weight.size, sizes[1], sizes[0], sizes[2], sizes[3]])
    late = late[0].reshape(-1)
    grad_router, grad_post_gain, grad_input_gain, grad_query_gain, grad_key_gain = (
        late[bounds[n] : bounds[n + 1]] for n in range(5)
    )
    grad_router = grad_router.reshape(router_weight.shape)
    return (
        result,
        grad_inputs,
        grad_input_gain,
        grad_post_gain,
        grad_query_gain,
        grad_key_gain,
        grad_query_w,
        grad_key_w,
        grad_value_w,
        grad_output_w,
        grad_router,
        grad_gate_w,
        grad_up_w,
        grad_down,
    )


def solution(mesh):
    dp_count, tensor_count = mesh.devices.shape
    split = jax.sharding.Mesh(
        mesh.devices.reshape(dp_count // 2, 2, tensor_count), ("chip", "core", "tensor")
    )
    tokens, line = P(BOTH, None), P(BOTH)
    gated = P(DP, None, "tensor")
    weights = (P("tensor", DP),) * 3 + (P(DP, "tensor"), tokens, gated, gated, P(DP, "tensor", None))
    return jax.shard_map(
        on_device,
        mesh=split,
        in_specs=(tokens,) + (line,) * 4 + weights + (tokens, tokens),
        out_specs=(tokens, tokens) + (line,) * 4 + weights,
        check_vma=False,
    )
```

```python
import functools
import math

import jax
import jax.numpy as jnp
import numpy as np
from jax import lax
from jax.experimental import pallas as pl
from jax.experimental.layout import Layout, with_layout_constraint
from jax.experimental.pallas import tpu as pltpu
from jax.sharding import PartitionSpec as P

HEAD_SIZE = 128
LANES = 128
EPSILON = 1e-06
ROPE_BASE = 1000000.0
DP = ("chip", "core")
BOTH = ("chip", "core", "tensor")
BF16 = jnp.bfloat16
F32 = jnp.float32
STEP_BLOCKS = 4
VMEM_BYTES = 60 * 1024 * 1024


def norm_rows(values, weights):
    inverse = lax.rsqrt(jnp.mean(values * values, axis=-1, keepdims=True) + EPSILON)
    normalized_rows = values * inverse
    return (normalized_rows * weights, normalized_rows, inverse)


def norm_back(upstream, weights, normalized_rows, inverse):
    scaled = upstream * weights
    inner_term = jnp.mean(scaled * normalized_rows, axis=-1, keepdims=True)
    return (inverse * (scaled - normalized_rows * inner_term), upstream * normalized_rows)


def rope_tables(length, head_width):
    half_width = head_width // 2
    frequency = jnp.exp(
        jnp.arange(half_width, dtype=F32) * (-2.0 * math.log(ROPE_BASE) / head_width)
    )
    angles = jnp.arange(length, dtype=F32)[:, None] * frequency[None, :]
    angles = jnp.concatenate([angles, angles], axis=-1)
    return (jnp.cos(angles), jnp.sin(angles))


def rotate_half(values):
    half_width = values.shape[-1] // 2
    return jnp.concatenate([-values[..., half_width:], values[..., :half_width]], axis=-1)


def rotate_back(values):
    half_width = values.shape[-1] // 2
    return jnp.concatenate([values[..., half_width:], -values[..., :half_width]], axis=-1)


def dot(left, right, left_dim=1, right_dim=0):
    return lax.dot_general(
        left, right, (((left_dim,), (right_dim,)), ((), ())), preferred_element_type=F32
    )


LATTICE = {"z": 4, "x": 2, "core": 2, "y": 2}


def is_lattice(dp_count, tensor_count):
    return dp_count == 16 and tensor_count == 2


def hop(values, axis, step=1):
    sizes = tuple(LATTICE.values())
    place = list(LATTICE).index(axis)
    pairs = []
    for source in range(math.prod(sizes)):
        spot = list(np.unravel_index(source, sizes))
        spot[place] = (spot[place] + step) % sizes[place]
        pairs.append((source, int(np.ravel_multi_index(spot, sizes))))
    return lax.ppermute(values, BOTH, pairs)


def my_spot():
    chip_core = lax.axis_index(DP)
    return {
        "z": chip_core // 4,
        "x": (chip_core // 2) % 2,
        "core": chip_core % 2,
        "y": lax.axis_index("tensor"),
    }


def add_low(first, second):
    return (first.astype(F32) + second.astype(F32)).astype(BF16)


class Pending:
    def __init__(self, *parts):
        self.parts = parts

    def total(self):
        return sum(part.astype(F32) for part in self.parts)

    def piece(self, place, dim):
        picked = [lax.index_in_dim(part, place, dim, keepdims=False) for part in self.parts]
        return Pending(*picked).total().astype(BF16)


def after(values, others):
    return lax.optimization_barrier((values, others))[0]


class Links:
    def __init__(self):
        self.active = []
        self.marks = []

    def add(self, *jobs, rank=0):
        places = [[None] for _ in jobs]
        for job, place in zip(jobs, places):
            self.advance(rank, job, place, None)
        return places

    def advance(self, rank, job, place, arrived):
        try:
            sends = job.send(arrived)
        except StopIteration as stop:
            place[0] = stop.value
            return
        sent = lax.optimization_barrier(tuple(array for array, _ in sends))
        self.marks += sent
        moved = [move(array) for (_, move), array in zip(sends, sent)]
        self.active.append((rank, job, place, moved))

    def round(self, work=None, *operands):
        moving, self.active = sorted(self.active, key=lambda entry: entry[0]), []
        result = None
        if work is not None:
            result = work(*(after(operands, self.marks) if self.marks else operands))
            self.marks = jax.tree.leaves(result)[:1]
        for rank, job, place, moved in moving:
            if self.marks:
                moved = after(moved, self.marks)
            self.marks = []
            self.advance(rank, job, place, moved)
        return result

    def finish(self):
        while self.active:
            self.round()

    def aside(self, main):
        self.marks = main.marks
        self.round()
        main.marks = self.marks


def mover(axis, step=1):
    return lambda values: hop(values, axis, step)


def home_job(partner, own, axes, order, turn):
    axes = list(axes)
    if partner is None:
        pending = own
    else:
        (received,) = yield [(partner, mover("core"))]
        pending = Pending(own, received)
    for axis in order:
        dim = axes.index(axis)
        axes.remove(axis)
        if axis == "z":
            (received,) = yield [(pending.piece(2, dim), mover("z", turn))]
            near = {-1: pending.piece(1, dim), 1: pending.piece(3, dim)}
            near[turn] = add_low(near[turn], received)
            arrived = yield [(near[step], mover("z", step)) for step in (-1, 1)]
        else:
            arrived = yield [(pending.piece(1, dim), mover(axis))]
        pending = Pending(pending.piece(0, dim), *arrived)
    return pending.total()


def spread_job(own, axes, order, turn):
    pieces = own.reshape((1,) * len(axes) + own.shape)
    for axis in order:
        dim = axes.index(axis)
        if axis == "z":
            near = yield [(pieces, mover("z", 1)), (pieces, mover("z", -1))]
            (far,) = yield [(near[0 if turn == 1 else 1], mover("z", turn))]
            pieces = jnp.concatenate([pieces, near[0], far, near[1]], axis=dim)
        else:
            (other,) = yield [(pieces, mover(axis))]
            pieces = jnp.concatenate([pieces, other], axis=dim)
    flat = pieces.reshape((-1,) + own.shape)
    (partner,) = yield [(flat, mover("core"))]
    return partner, flat


def spread_jobs(own, cuts, axes, orders):
    groups = jnp.split(own, cuts, axis=1)
    return [spread_job(*job) for job in zip(groups, [axes] * len(groups), orders, TURNS)]


def gathered_groups(places):
    return [[place[0][half] for place in places] for half in range(2)]


def flip(bits):
    count = lax.axis_size(BOTH)
    return lambda values: lax.ppermute(
        values, BOTH, [(source, source ^ bits) for source in range(count)]
    )


def gather_small_job(values):
    device_count = lax.axis_size(BOTH)
    number = lax.axis_index(BOTH)
    everything = jnp.zeros((device_count,) + values.shape, values.dtype)
    everything = lax.dynamic_update_index_in_dim(everything, values, number, 0)
    bit = 1
    while bit < device_count:
        fan = min(4, device_count // bit)
        start = number // bit * bit
        sent = lax.dynamic_slice_in_dim(everything, start, bit, 0)
        arrived = yield [(sent, flip(k * bit)) for k in range(1, fan)]
        for k, received in enumerate(arrived, 1):
            everything = lax.dynamic_update_slice_in_dim(
                everything, received, start ^ (k * bit), 0
            )
        bit *= fan
    return everything


def reduce_small_job(values):
    number = lax.axis_index(BOTH)
    count = values.shape[0]
    while count > 1:
        fan = min(4, count)
        bit = count // fan
        parts = values.reshape((fan, bit) + values.shape[1:])
        mine = (number // bit) % fan
        pick = lambda place: lax.dynamic_index_in_dim(parts, place, 0, keepdims=False)
        arrived = yield [(pick(mine ^ k), flip(k * bit)) for k in range(1, fan)]
        values = sum(arrived, pick(mine))
        count = bit
    return values[0]


def swap_tensor(values):
    return lax.ppermute(values, "tensor", [(0, 1), (1, 0)])


def swap_job(values):
    (received,) = yield [(values, swap_tensor)]
    return received


def in_order(mine, other):
    first = lax.axis_index("tensor") == 0
    return jnp.where(
        first, jnp.concatenate([mine, other], axis=0), jnp.concatenate([other, mine], axis=0)
    )


def sum_tokens_job(terms):
    low = terms.astype(BF16).reshape((2, terms.shape[0] // 2) + terms.shape[1:])
    half = lax.axis_index("tensor")
    sent = lax.dynamic_index_in_dim(low, 1 - half, 0, keepdims=False)
    kept = lax.dynamic_index_in_dim(low, half, 0, keepdims=False)
    (received,) = yield [(sent, swap_tensor)]
    return kept.astype(F32) + received.astype(F32)


def choose(position_row, capacity):
    slot = lax.broadcasted_iota(jnp.int32, (capacity, position_row.shape[1]), 0).astype(F32)
    picks = [
        (slot == position_row[e : e + 1, :]).astype(F32) for e in range(position_row.shape[0])
    ]
    return picks


def expert_kernel(capacity, widths, token_groups, grad_groups, carried, first, *refs):
    blocks = STEP_BLOCKS
    groups = token_groups + grad_groups
    token_refs, grad_refs, refs = refs[:token_groups], refs[token_groups:groups], refs[groups:]
    position_ref, mask_ref, router_ref, up_ref, up_t_ref, down_t_ref = refs[:6]
    refs = refs[6 + carried :]
    rows_ref, grad_rows_ref, gated_ref, grad_gate_ref, grad_up_ref = refs[:5]
    out_refs, packed_ref = refs[5:-1], refs[-1]
    experts_here = up_ref.shape[0]
    hidden_units = down_t_ref.shape[2]
    width = sum(ref.shape[2] for ref in token_refs)
    first_expert = first[0]
    gates = [[] for _ in range(experts_here)]
    choices = []
    for j in range(blocks):
        picks = choose(position_ref[j], capacity)
        choice = jnp.concatenate(picks, axis=0).astype(BF16)
        choices.append(choice)
        here = slice(j * capacity, (j + 1) * capacity)
        for group_refs, kept_ref in ((token_refs, rows_ref), (grad_refs, grad_rows_ref)):
            start = 0
            for ref in group_refs:
                size = ref.shape[2]
                picked = dot(choice, ref[j]).astype(BF16)
                for e in range(experts_here):
                    kept_ref[e, here, start : start + size] = picked[
                        e * capacity : (e + 1) * capacity
                    ]
                start += size
        logits, start = 0.0, 0
        for ref in token_refs:
            size = ref.shape[2]
            logits = logits + dot(router_ref[:, start : start + size], ref[j], 1, 1)
            start += size
        chosen = mask_ref[j].astype(F32) > 0.5
        top = jnp.max(jnp.where(chosen, logits, -3e38), axis=0, keepdims=True)
        powers = jnp.where(chosen, jnp.exp(jnp.minimum(logits - top, 0.0)), 0.0)
        gate_all = powers / jnp.sum(powers, axis=0, keepdims=True)
        expert_number = lax.broadcasted_iota(jnp.int32, gate_all.shape, 0)
        for e in range(experts_here):
            gate_row = jnp.sum(
                jnp.where(expert_number == first_expert + e, gate_all, 0.0), axis=0, keepdims=True
            )
            gates[e].append(jnp.sum(picks[e] * gate_row, axis=1, keepdims=True))
    for e in range(experts_here):
        both = dot(rows_ref[e], up_ref[e])
        gate_pre = both[:, :hidden_units]
        up_pre = both[:, hidden_units:]
        raw = dot(grad_rows_ref[e], down_t_ref[e])
        sigmoid = 1.0 / (1.0 + jnp.exp(-gate_pre))
        silu = gate_pre * sigmoid
        hidden = silu * up_pre
        gate = jnp.concatenate(gates[e], axis=0)
        grad_gate = jnp.sum(hidden * raw, axis=1, keepdims=True)
        grad_hidden = gate * raw
        grad_gate_pre = (
            grad_hidden * up_pre * sigmoid * (1.0 + gate_pre * (1.0 - sigmoid))
        ).astype(BF16)
        grad_up_pre = (grad_hidden * silu).astype(BF16)
        gated_ref[e] = (gate * hidden).astype(BF16)
        grad_gate_ref[e] = grad_gate_pre
        grad_up_ref[e] = grad_up_pre
        back = dot(grad_gate_pre, up_t_ref[e, :hidden_units, :]) + dot(
            grad_up_pre, up_t_ref[e, hidden_units:, :]
        )
        lane = lax.broadcasted_iota(jnp.int32, (blocks * capacity, LANES), 1)
        extra = jnp.where(lane == first_expert + e, grad_gate, 0.0).astype(BF16)
        back = back.astype(BF16)
        for j in range(blocks):
            packed_ref[j, e * capacity : (e + 1) * capacity, :width] = back[
                j * capacity : (j + 1) * capacity
            ]
            packed_ref[j, e * capacity : (e + 1) * capacity, width:] = extra[
                j * capacity : (j + 1) * capacity
            ]
    for j in range(blocks):
        home = dot(choices[j], packed_ref[j], 0, 0).astype(BF16)
        start = 0
        for out_ref, size in zip(out_refs, widths):
            out_ref[j] = home[:, start : start + size]
            start += size


def whole(shape):
    return pl.BlockSpec(
        shape, lambda i, *scalars: (0,) * len(shape), pipeline_mode=pl.Buffered(1)
    )


def stepped(shape, dim):
    return pl.BlockSpec(
        shape, lambda i, *scalars: tuple(i if d == dim else 0 for d in range(len(shape)))
    )


def expert_grads(
    half, carry, first, tokens, grads, block_start, position, mask,
    router_t, up_both, up_both_t, down_t, capacity, widths,
):
    count = position.shape[0]
    width = sum(group.shape[2] for group in tokens)
    experts_here, hidden_units = down_t.shape[0], down_t.shape[2]
    slots = STEP_BLOCKS * capacity
    expert_count = router_t.shape[0]
    slot_shape = lambda size: jax.ShapeDtypeStruct((experts_here, 2 * count * capacity, size), BF16)
    steps = count // STEP_BLOCKS
    slot_spec = lambda size: pl.BlockSpec(
        (experts_here, slots, size), lambda i, *scalars: (0, i + half * steps, 0)
    )
    before = 1 + len(tokens) + len(grads) + 6
    flops = 2 * count * capacity * experts_here * (7 * hidden_units * width + 3 * LANES * width)
    call = pl.pallas_call(
        functools.partial(
            expert_kernel, capacity, widths, len(tokens), len(grads), len(carry)
        ),
        grid_spec=pltpu.PrefetchScalarGridSpec(
            num_scalar_prefetch=1,
            grid=(steps,),
            in_specs=[
                pl.BlockSpec(
                    (STEP_BLOCKS, LANES, group.shape[2]),
                    lambda i, *scalars: (i + block_start // STEP_BLOCKS, 0, 0),
                )
                for group in (*tokens, *grads)
            ]
            + [
                stepped((STEP_BLOCKS, experts_here, LANES), 0),
                stepped((STEP_BLOCKS, expert_count, LANES), 0),
                whole(router_t.shape),
                whole(up_both.shape),
                whole(up_both_t.shape),
                whole(down_t.shape),
            ]
            + [pl.BlockSpec(memory_space=pl.ANY)] * len(carry),
            out_specs=[slot_spec(width)] * 2
            + [slot_spec(hidden_units)] * 3
            + [stepped((STEP_BLOCKS, LANES, size), 0) for size in widths],
            scratch_shapes=[
                pltpu.VMEM((STEP_BLOCKS, experts_here * capacity, sum(widths)), BF16)
            ],
        ),
        out_shape=[slot_shape(width)] * 2
        + [slot_shape(hidden_units)] * 3
        + [jax.ShapeDtypeStruct((count, LANES, size), BF16) for size in widths],
        compiler_params=pltpu.CompilerParams(vmem_limit_bytes=VMEM_BYTES),
        cost_estimate=pl.CostEstimate(
            flops=flops, transcendentals=0, bytes_accessed=6 * count * LANES * width * 2
        ),
        input_output_aliases={before + n: n for n in range(len(carry))},
        name="expert_grads",
    )
    return call(
        first, *tokens, *grads,
        position, mask, router_t, up_both, up_both_t, down_t, *carry,
    )


def output_kernel(capacity, widths, gated_ref, position_ref, down_ref, *refs):
    out_refs, packed_ref = refs[:-1], refs[-1]
    for e in range(down_ref.shape[0]):
        rows = dot(gated_ref[e], down_ref[e]).astype(BF16)
        for j in range(STEP_BLOCKS):
            packed_ref[j, e * capacity : (e + 1) * capacity, :] = rows[
                j * capacity : (j + 1) * capacity
            ]
    for j in range(STEP_BLOCKS):
        choice = jnp.concatenate(choose(position_ref[j], capacity), axis=0).astype(BF16)
        home = dot(choice, packed_ref[j], 0, 0).astype(BF16)
        start = 0
        for out_ref, size in zip(out_refs, widths):
            out_ref[j] = home[:, start : start + size]
            start += size


def expert_outputs(half, gated, position, down, capacity, widths):
    count = position.shape[0]
    experts_here, hidden_units, width = down.shape
    slots = STEP_BLOCKS * capacity
    steps = count // STEP_BLOCKS
    call = pl.pallas_call(
        functools.partial(output_kernel, capacity, widths),
        grid=(steps,),
        in_specs=[
            pl.BlockSpec(
                (experts_here, slots, hidden_units), lambda i: (0, i + half * steps, 0)
            ),
            stepped((STEP_BLOCKS, experts_here, LANES), 0),
            whole(down.shape),
        ],
        out_specs=[stepped((STEP_BLOCKS, LANES, size), 0) for size in widths],
        out_shape=[jax.ShapeDtypeStruct((count, LANES, size), BF16) for size in widths],
        scratch_shapes=[pltpu.VMEM((STEP_BLOCKS, experts_here * capacity, width), BF16)],
        compiler_params=pltpu.CompilerParams(vmem_limit_bytes=VMEM_BYTES),
        cost_estimate=pl.CostEstimate(
            flops=2 * count * capacity * experts_here * (hidden_units * width + LANES * width),
            transcendentals=0,
            bytes_accessed=2 * count * LANES * width * 2,
        ),
        name="expert_outputs",
    )
    return call(gated, position, down)


def chunk_kernel(widths, perm, *refs):
    left = jnp.concatenate([ref[...] for ref in refs[:STEP_BLOCKS]], axis=1)
    product = dot(left, refs[STEP_BLOCKS][...], 0, 0).astype(BF16)
    start = 0
    for out_ref, size in zip(refs[STEP_BLOCKS + 1 :], widths):
        for j in range(STEP_BLOCKS):
            out_ref[j] = product[j * LANES : (j + 1) * LANES, start : start + size]
        start += size


def chunk_products(perm, left, right, widths):
    count = perm.shape[0]
    tokens = left.shape[0]

    def column_block(place):
        return pl.BlockSpec((tokens, LANES), lambda i, perm: (0, perm[i * STEP_BLOCKS + place]))

    call = pl.pallas_call(
        functools.partial(chunk_kernel, widths),
        grid_spec=pltpu.PrefetchScalarGridSpec(
            num_scalar_prefetch=1,
            grid=(count // STEP_BLOCKS,),
            in_specs=[column_block(j) for j in range(STEP_BLOCKS)] + [whole(right.shape)],
            out_specs=[stepped((STEP_BLOCKS, LANES, size), 0) for size in widths],
        ),
        out_shape=[jax.ShapeDtypeStruct((count, LANES, size), BF16) for size in widths],
        compiler_params=pltpu.CompilerParams(vmem_limit_bytes=VMEM_BYTES),
        cost_estimate=pl.CostEstimate(
            flops=2 * count * LANES * tokens * right.shape[1],
            transcendentals=0,
            bytes_accessed=count * LANES * right.shape[1] * 2,
        ),
        name="chunk_products",
    )
    return call(perm, *([left] * STEP_BLOCKS), right)


def block_orders(lattice, device_count):
    if not lattice:
        numbers = jnp.arange(device_count, dtype=jnp.int32)
        return numbers[: device_count // 2], numbers[device_count // 2 :]
    spot = my_spot()
    dz, dx, dy = (grid.reshape(-1) for grid in np.indices((4, 2, 2)).astype(np.int32))
    chip = (spot["z"] - dz + 4) % 4 * 2 + (spot["x"] + dx) % 2
    orders = []
    for dc in (1, 0):
        core = (spot["core"] + dc) % 2
        orders.append(((chip * 2 + core) * 2 + (spot["y"] + dy) % 2).astype(jnp.int32))
    return orders


def chunk_orders():
    spot = my_spot()
    dz, dx = (grid.reshape(-1) for grid in np.indices((4, 2)).astype(np.int32))
    chip = (spot["z"] - dz + 4) % 4 * 2 + (spot["x"] + dx) % 2
    return [(chip * 2 + (spot["core"] + dc) % 2).astype(jnp.int32) for dc in (1, 0)]


TOKEN_ORDERS = (("x", "y", "z"), ("y", "z", "x"), ("z", "x", "y"))
GATHER_ORDERS = (("z", "y", "x"), ("x", "z", "y"), ("y", "x", "z"))
PROJECTION_ORDERS = (("x", "z"), ("z", "x"))
OUTPUT_ORDERS = (("x", "z"),)
TURNS = (1, -1, 1)


def scatter_job(partner, own):
    everything = jnp.concatenate([partner, own], axis=0)
    total = lax.psum_scatter(everything, BOTH, scatter_dimension=0, tiled=True)
    return total[0].astype(F32)
    yield


def tokens_home_jobs(lattice, partner, own, received=None):
    jobs = []
    for n, order in enumerate(TOKEN_ORDERS):
        if not lattice:
            jobs.append(scatter_job(partner[n], own[n]))
            continue
        shape = (4, 2, 2) + own[n].shape[1:]
        mine = own[n].reshape(shape)
        if received is None:
            jobs.append(home_job(partner[n].reshape(shape), mine, "zxy", order, TURNS[n]))
        else:
            both = Pending(mine, received[n].reshape(shape))
            jobs.append(home_job(None, both, "zxy", order, TURNS[n]))
    return jobs


def product_job(left, right):
    product = dot(left, right, 0, 0).astype(BF16)
    return lax.psum_scatter(product, DP, scatter_dimension=0, tiled=True).astype(F32)
    yield


def weight_grads_chunks(lattice, left, right, widths):
    if not lattice:
        return left, right
    return tuple(chunk_products(order, left, right, widths) for order in chunk_orders())


def weight_grads_jobs(lattice, first, second, orders):
    if not lattice:
        return [product_job(first, second)]
    jobs = []
    for n, order in enumerate(orders):
        shape = (4, 2) + first[n].shape[1:]
        jobs.append(
            home_job(first[n].reshape(shape), second[n].reshape(shape), "zx", order, TURNS[n])
        )
    return jobs


def on_device(
    inputs,
    input_gain,
    post_gain,
    query_gain,
    key_gain,
    query_weight,
    key_projection_matrix,
    value_projection_matrix,
    output_weight,
    router_weight,
    gate_weight,
    up_weight,
    down_weight,
    routes,
    cotangent,
):
    dp_count, tensor_count = lax.axis_size(DP), lax.axis_size("tensor")
    device_count = dp_count * tensor_count
    lattice = is_lattice(dp_count, tensor_count)
    row_count, width = inputs.shape
    experts = router_weight.shape[1]
    experts_here = gate_weight.shape[0]
    capacity = 2 * row_count * routes.shape[1] // experts

    links, slow = Links(), Links()
    projections = jnp.concatenate(
        [query_weight, key_projection_matrix, value_projection_matrix], axis=0
    )
    query_rows, key_rows = query_weight.shape[0], key_projection_matrix.shape[0]

    expert_ids = jnp.arange(experts, dtype=jnp.int32)
    chosen_mask = jnp.any(routes[:, :, None] == expert_ids[None, None, :], axis=1)
    small = [input_gain, post_gain, query_gain, key_gain]
    sizes = [item.shape[0] for item in small]
    flat = jnp.concatenate(small)
    padded = -(-flat.shape[0] // LANES) * LANES
    flat = jnp.pad(flat, (0, padded - flat.shape[0]))
    router_lines = router_weight.size // LANES
    payload = jnp.concatenate(
        [
            router_weight.reshape(router_lines, LANES),
            flat.reshape(-1, LANES),
            chosen_mask.T.astype(BF16),
        ],
        axis=0,
    )
    gathered_at, other_inputs_at = links.add(gather_small_job(payload), swap_job(inputs))
    projections_full = lax.all_gather(projections.T, DP, axis=0, tiled=True)
    if lattice:
        cuts = (width // 8 * 3, width // 16 * 11)
        grads_at = links.add(*spread_jobs(cotangent, cuts, "zxy", GATHER_ORDERS))

    def join_up(gate, up):
        return jnp.concatenate([gate, up], axis=2)

    def turn_last(values):
        return with_layout_constraint(jnp.swapaxes(values, 1, 2), Layout((0, 1, 2)))

    up_both = links.round(join_up, gate_weight, up_weight)
    output_held = after(output_weight, up_both[0, :8, :LANES])
    output_full = lax.all_gather(output_held, DP, axis=0, tiled=True)
    up_both_t = links.round(turn_last, up_both)
    down_t = links.round(turn_last, down_weight)
    while gathered_at[0] is None:
        links.round()
    gathered, other_inputs = gathered_at[0], other_inputs_at[0]

    router_full = gathered[:, :router_lines].reshape(width, experts)
    flat_all = gathered[:, router_lines : router_lines + padded // LANES].reshape(
        device_count, padded
    )
    starts = np.cumsum([0] + sizes)
    input_scale, post_scale, query_scale, key_scale = (
        flat_all[:, starts[n] : starts[n + 1]].reshape(-1).astype(F32) for n in range(4)
    )
    mask_all = gathered[:, router_lines + padded // LANES :]
    first_expert = lax.axis_index(DP) * experts_here
    mask_here = lax.dynamic_slice_in_dim(mask_all, first_expert, experts_here, axis=1)
    earlier = jnp.asarray(np.triu(np.ones((row_count, row_count), np.float32), 1), BF16)
    rank = jnp.einsum("bet,tu->beu", mask_here, earlier, preferred_element_type=F32)
    position = jnp.where(mask_here > 0.5, rank, -1.0)
    orders = block_orders(lattice, device_count)
    positions = [position[order] for order in orders]
    masks = [mask_all[order] for order in orders]
    router_t = router_full.T

    both_inputs = in_order(inputs, other_inputs).astype(F32)
    residual_in = inputs.astype(F32)
    sequence = norm_rows(both_inputs, input_scale)[0].astype(BF16)
    _, input_hat, input_inv = norm_rows(residual_in, input_scale)
    seq_len = sequence.shape[0]
    local_heads = query_rows // HEAD_SIZE
    local_groups = key_rows // HEAD_SIZE
    per_group = local_heads // local_groups
    cosine_table, sine_table = rope_tables(seq_len, HEAD_SIZE)
    cosine, sine = cosine_table[:, None, :], sine_table[:, None, :]
    score_scale = 1.0 / math.sqrt(HEAD_SIZE)

    def project(projections_full):
        projected = dot(sequence, projections_full)
        query_raw = projected[:, :query_rows].reshape(seq_len, local_heads, HEAD_SIZE)
        key_raw = projected[:, query_rows : query_rows + key_rows].reshape(
            seq_len, local_groups, HEAD_SIZE
        )
        value_low = (
            projected[:, query_rows + key_rows :]
            .astype(BF16)
            .reshape(seq_len, local_groups, HEAD_SIZE)
        )
        query_norm, query_hat, query_inv = norm_rows(query_raw, query_scale)
        query_low = (query_norm * cosine + rotate_half(query_norm) * sine).astype(BF16)
        key_norm, key_hat, key_inv = norm_rows(key_raw, key_scale)
        key_low = (key_norm * cosine + rotate_half(key_norm) * sine).astype(BF16)
        query_groups = query_low.reshape(seq_len, local_groups, per_group, HEAD_SIZE)
        return query_groups, query_hat, query_inv, key_hat, key_inv, key_low, value_low

    def attention(query_groups, key_low, value_low):
        scores = (
            jnp.einsum("qhgd,khd->hgqk", query_groups, key_low, preferred_element_type=F32)
            * score_scale
        )
        row_index = jnp.arange(seq_len, dtype=jnp.int32)
        scores = jnp.where(row_index[None, :] <= row_index[:, None], scores, -1e30)
        attend = jax.nn.softmax(scores, axis=-1)
        attend_low = attend.astype(BF16)
        mixed_low = (
            jnp.einsum("hgqk,khd->qhgd", attend_low, value_low, preferred_element_type=F32)
            .astype(BF16)
            .reshape(seq_len, query_rows)
        )
        return mixed_low, attend, attend_low

    query_groups, query_hat, query_inv, key_hat, key_inv, key_low, value_low = links.round(
        project, projections_full
    )
    mixed_low, attend, attend_low = links.round(attention, query_groups, key_low, value_low)
    links.finish()
    ready = (positions, masks, router_t, up_both, up_both_t, down_t)
    mixed_low, (positions, masks, router_t, up_both, up_both_t, down_t) = (
        lax.optimization_barrier((mixed_low, ready))
    )
    mixed_out = dot(after(mixed_low, links.marks), output_full, 1, 1)
    (mixed_home,) = links.add(sum_tokens_job(mixed_out))
    links.finish()
    residual_mid = residual_in + mixed_home[0]
    post_norm, post_hat, post_inv = norm_rows(residual_mid, post_scale)
    post_low = post_norm.astype(BF16)
    block_starts = (0, 0)
    if lattice:
        tokens_at = links.add(*spread_jobs(post_low, cuts, "zxy", GATHER_ORDERS))
        links.finish()
        all_tokens, all_grads = gathered_groups(tokens_at), gathered_groups(grads_at)
    else:
        block_starts = (0, device_count // 2)
        all_tokens, all_grads = (
            ([lax.all_gather(values[None], BOTH, axis=0, tiled=True)],) * 2
            for values in (post_low, cotangent)
        )

    logits = dot(post_low, router_full)
    top = jnp.max(jnp.where(chosen_mask, logits, -3e38), axis=-1, keepdims=True)
    powers = jnp.where(chosen_mask, jnp.exp(jnp.minimum(logits - top, 0.0)), 0.0)
    gates = powers / jnp.sum(powers, axis=-1, keepdims=True)

    wide = width // 8 * 3
    widths = (wide, wide, width - 2 * wide + LANES)
    first_scalar = first_expert.astype(jnp.int32).reshape(1)

    def half_grads(half, carry):
        return expert_grads(
            half, carry, first_scalar, all_tokens[half], all_grads[half],
            block_starts[half], positions[half], masks[half],
            router_t, up_both, up_both_t, down_t, capacity, widths,
        )

    results = half_grads(0, ())
    partner = results[5:]
    received = [hop(group, "core") for group in partner] if lattice else None
    results = half_grads(1, results[:5])
    rows, grad_rows, gated, grad_gate_pre, grad_up_pre = results[:5]
    own = results[5:]

    def slot_product(left, right):
        return jnp.einsum("esd,esf->edf", left, right, preferred_element_type=F32)

    out_widths = (wide, wide, width - 2 * wide)

    def outputs(gated):
        return [
            expert_outputs(n, gated, positions[n], down_weight, capacity, out_widths)
            for n in range(2)
        ]

    home = links.add(*tokens_home_jobs(lattice, partner, own, received))
    out_partner, out_own = links.round(outputs, gated)
    out_received = [hop(group, "core") for group in out_partner] if lattice else None
    grad_gate_w = links.round(slot_product, rows, grad_gate_pre)
    grad_down = links.round(slot_product, gated, grad_rows)
    links.finish()
    home = [place[0] for place in home]

    grad_out = cotangent.astype(F32)
    grad_post = jnp.concatenate([home[0], home[1], home[2][:, : width - 2 * wide]], axis=1)
    start = width - 2 * wide
    grad_gates = home[2][:, start : start + experts]
    grad_logits = (
        gates * (grad_gates - jnp.sum(gates * grad_gates, axis=-1, keepdims=True))
    ).astype(BF16)
    grad_post = grad_post + dot(grad_logits, router_full, 1, 1)
    grad_mid_norm, post_terms = norm_back(grad_post, post_scale, post_hat, post_inv)
    grad_mid = grad_out + grad_mid_norm
    grad_mid_low = grad_mid.astype(BF16)
    (other_grads,) = links.add(swap_job(grad_mid_low))
    out_jobs = tokens_home_jobs(lattice, out_partner, out_own, out_received)
    out_home = links.add(*out_jobs)
    grad_up_w = slot_product(*after((rows, grad_up_pre), links.marks))
    links.marks = [grad_up_w]
    while other_grads[0] is None:
        swapped = links.active.pop(0)
        links.advance(*swapped[:3], after(swapped[3], links.marks))
    grad_attention = in_order(grad_mid_low, other_grads[0])


    def back_scores(grad_attention):
        grad_mixed = dot(grad_attention, output_full).astype(BF16)
        grad_groups = grad_mixed.reshape(seq_len, local_groups, per_group, HEAD_SIZE)
        grad_attend = jnp.einsum(
            "qhgd,khd->hgqk", grad_groups, value_low, preferred_element_type=F32
        )
        row_inner = jnp.sum(attend * grad_attend, axis=-1, keepdims=True)
        grad_scores = (attend * (grad_attend - row_inner)).astype(BF16)
        return grad_groups, grad_scores

    chunks = weight_grads_chunks(lattice, grad_attention, mixed_low, (query_rows,))
    grad_output_at = slow.add(*weight_grads_jobs(lattice, *chunks, OUTPUT_ORDERS))
    links.marks = links.marks + slow.marks
    grad_groups, grad_scores = links.round(back_scores, grad_attention)
    slow.aside(links)
    grad_router = dot(post_low, grad_logits, 0, 0)
    grad_post_gain = jnp.sum(post_terms, axis=0)
    def back_heads(grad_groups, grad_scores):
        grad_value = jnp.einsum(
            "hgqk,qhgd->khd", attend_low, grad_groups, preferred_element_type=F32
        )
        grad_key_rot = (
            jnp.einsum("hgqk,qhgd->khd", grad_scores, query_groups, preferred_element_type=F32)
            * score_scale
        )
        grad_query_rot = (
            jnp.einsum("hgqk,khd->qhgd", grad_scores, key_low, preferred_element_type=F32)
            * score_scale
        ).reshape(seq_len, local_heads, HEAD_SIZE)
        return grad_value, grad_key_rot, grad_query_rot

    grad_value, grad_key_rot, grad_query_rot = links.round(back_heads, grad_groups, grad_scores)

    def back_norms(grad_query_rot):
        grad_query_norm = grad_query_rot * cosine + rotate_back(grad_query_rot * sine)
        grad_query_raw, query_terms = norm_back(grad_query_norm, query_scale, query_hat, query_inv)
        return grad_query_raw.reshape(seq_len, query_rows).astype(BF16), query_terms

    grad_query_low, query_terms = links.round(back_norms, grad_query_rot)
    grad_query_gain = jnp.sum(query_terms, axis=(0, 1))
    grad_key_norm = grad_key_rot * cosine + rotate_back(grad_key_rot * sine)
    grad_key_raw, key_terms = norm_back(grad_key_norm, key_scale, key_hat, key_inv)
    grad_key_gain = jnp.sum(key_terms, axis=(0, 1))
    grad_projected = jnp.concatenate(
        [
            grad_query_low,
            grad_key_raw.reshape(seq_len, key_rows).astype(BF16),
            grad_value.reshape(seq_len, key_rows).astype(BF16),
        ],
        axis=1,
    )
    total_rows = query_rows + 2 * key_rows
    split = total_rows // LANES * 2 // 5 * LANES
    chunks = weight_grads_chunks(
        lattice, sequence, grad_projected, (split, total_rows - split)
    )
    grad_projections_at = links.add(
        *weight_grads_jobs(lattice, *chunks, PROJECTION_ORDERS), rank=-1
    )
    slow.aside(links)
    normed_parts = links.round(
        lambda grad: dot(grad, projections_full, 1, 1), grad_projected
    )
    (grad_normed,) = links.add(sum_tokens_job(normed_parts), rank=-1)
    links.round()
    slow.aside(links)
    grad_in_norm, input_terms = norm_back(grad_normed[0], input_scale, input_hat, input_inv)
    grad_input_gain = jnp.sum(input_terms, axis=0)
    grad_inputs = (grad_mid + grad_in_norm).astype(BF16)
    late_parts = [grad_router, grad_post_gain, grad_input_gain, grad_query_gain, grad_key_gain]
    flat = jnp.concatenate([part.reshape(device_count, -1) for part in late_parts], axis=1)
    flat = jnp.pad(flat, ((0, 0), (0, -flat.shape[1] % LANES)))
    (late,) = links.add(reduce_small_job(flat.reshape(device_count, -1, LANES)))
    while links.active or slow.active:
        links.round()
        slow.aside(links)
    result = (residual_mid + jnp.concatenate([p[0] for p in out_home], axis=1)).astype(BF16)
    grad_output_w = jnp.concatenate([place[0] for place in grad_output_at], axis=1)
    grad_projections = jnp.concatenate([place[0] for place in grad_projections_at], axis=1).T
    grad_query_w = grad_projections[:query_rows]
    grad_key_w = grad_projections[query_rows : query_rows + key_rows]
    grad_value_w = grad_projections[query_rows + key_rows :]
    bounds = np.cumsum([0, router_weight.size, sizes[1], sizes[0], sizes[2], sizes[3]])
    late = late[0].reshape(-1)
    grad_router, grad_post_gain, grad_input_gain, grad_query_gain, grad_key_gain = (
        late[bounds[n] : bounds[n + 1]] for n in range(5)
    )
    grad_router = grad_router.reshape(router_weight.shape)
    return (
        result,
        grad_inputs,
        grad_input_gain,
        grad_post_gain,
        grad_query_gain,
        grad_key_gain,
        grad_query_w,
        grad_key_w,
        grad_value_w,
        grad_output_w,
        grad_router,
        grad_gate_w,
        grad_up_w,
        grad_down,
    )


def solution(mesh):
    dp_count, tensor_count = mesh.devices.shape
    split = jax.sharding.Mesh(
        mesh.devices.reshape(dp_count // 2, 2, tensor_count), ("chip", "core", "tensor")
    )
    tokens, line = P(BOTH, None), P(BOTH)
    gated = P(DP, None, "tensor")
    weights = (P("tensor", DP),) * 3 + (P(DP, "tensor"), tokens, gated, gated, P(DP, "tensor", None))
    return jax.shard_map(
        on_device,
        mesh=split,
        in_specs=(tokens,) + (line,) * 4 + weights + (tokens, tokens),
        out_specs=(tokens, tokens) + (line,) * 4 + weights,
        check_vma=False,
    )
```

```python
import functools
import math

import jax
import jax.numpy as jnp
import numpy as np
from jax import lax
from jax.experimental import pallas as pl
from jax.experimental.layout import Layout, with_layout_constraint
from jax.experimental.pallas import tpu as pltpu
from jax.sharding import PartitionSpec as P

HEAD_SIZE = 128
LANES = 128
EPSILON = 1e-06
ROPE_BASE = 1000000.0
DP = ("chip", "core")
BOTH = ("chip", "core", "tensor")
BF16 = jnp.bfloat16
F32 = jnp.float32
STEP_BLOCKS = 4
VMEM_BYTES = 60 * 1024 * 1024


def norm_rows(values, weights):
    inverse = lax.rsqrt(jnp.mean(values * values, axis=-1, keepdims=True) + EPSILON)
    normalized_rows = values * inverse
    return (normalized_rows * weights, normalized_rows, inverse)


def norm_back(upstream, weights, normalized_rows, inverse):
    scaled = upstream * weights
    inner_term = jnp.mean(scaled * normalized_rows, axis=-1, keepdims=True)
    return (inverse * (scaled - normalized_rows * inner_term), upstream * normalized_rows)


def rope_tables(length, head_width):
    half_width = head_width // 2
    frequency = jnp.exp(
        jnp.arange(half_width, dtype=F32) * (-2.0 * math.log(ROPE_BASE) / head_width)
    )
    angles = jnp.arange(length, dtype=F32)[:, None] * frequency[None, :]
    angles = jnp.concatenate([angles, angles], axis=-1)
    return (jnp.cos(angles), jnp.sin(angles))


def rotate_half(values):
    half_width = values.shape[-1] // 2
    return jnp.concatenate([-values[..., half_width:], values[..., :half_width]], axis=-1)


def rotate_back(values):
    half_width = values.shape[-1] // 2
    return jnp.concatenate([values[..., half_width:], -values[..., :half_width]], axis=-1)


def dot(left, right, left_dim=1, right_dim=0):
    return lax.dot_general(
        left, right, (((left_dim,), (right_dim,)), ((), ())), preferred_element_type=F32
    )


LATTICE = {"z": 4, "x": 2, "core": 2, "y": 2}


def is_lattice(dp_count, tensor_count):
    return dp_count == 16 and tensor_count == 2


def hop(values, axis, step=1):
    sizes = tuple(LATTICE.values())
    place = list(LATTICE).index(axis)
    pairs = []
    for source in range(math.prod(sizes)):
        spot = list(np.unravel_index(source, sizes))
        spot[place] = (spot[place] + step) % sizes[place]
        pairs.append((source, int(np.ravel_multi_index(spot, sizes))))
    return lax.ppermute(values, BOTH, pairs)


def my_spot():
    chip_core = lax.axis_index(DP)
    return {
        "z": chip_core // 4,
        "x": (chip_core // 2) % 2,
        "core": chip_core % 2,
        "y": lax.axis_index("tensor"),
    }


def add_low(first, second):
    return (first.astype(F32) + second.astype(F32)).astype(BF16)


class Pending:
    def __init__(self, *parts):
        self.parts = parts

    def total(self):
        return sum(part.astype(F32) for part in self.parts)

    def piece(self, place, dim):
        picked = [lax.index_in_dim(part, place, dim, keepdims=False) for part in self.parts]
        return Pending(*picked).total().astype(BF16)


def after(values, others):
    return lax.optimization_barrier((values, others))[0]


class Links:
    def __init__(self):
        self.active = []
        self.marks = []

    def add(self, *jobs, rank=0):
        places = [[None] for _ in jobs]
        for job, place in zip(jobs, places):
            self.advance(rank, job, place, None)
        return places

    def advance(self, rank, job, place, arrived):
        try:
            sends = job.send(arrived)
        except StopIteration as stop:
            place[0] = stop.value
            return
        sent = lax.optimization_barrier(tuple(array for array, _ in sends))
        self.marks += sent
        moved = [move(array) for (_, move), array in zip(sends, sent)]
        self.active.append((rank, job, place, moved))

    def round(self, work=None, *operands):
        moving, self.active = sorted(self.active, key=lambda entry: entry[0]), []
        result = None
        if work is not None:
            result = work(*(after(operands, self.marks) if self.marks else operands))
            self.marks = jax.tree.leaves(result)[:1]
        for rank, job, place, moved in moving:
            if self.marks:
                moved = after(moved, self.marks)
            self.marks = []
            self.advance(rank, job, place, moved)
        return result

    def finish(self):
        while self.active:
            self.round()

    def aside(self, main):
        self.marks = main.marks
        self.round()
        main.marks = self.marks


def mover(axis, step=1):
    return lambda values: hop(values, axis, step)


def home_job(partner, own, axes, order, turn):
    axes = list(axes)
    if partner is None:
        pending = own
    else:
        (received,) = yield [(partner, mover("core"))]
        pending = Pending(own, received)
    for axis in order:
        dim = axes.index(axis)
        axes.remove(axis)
        if axis == "z":
            (received,) = yield [(pending.piece(2, dim), mover("z", turn))]
            near = {-1: pending.piece(1, dim), 1: pending.piece(3, dim)}
            near[turn] = add_low(near[turn], received)
            arrived = yield [(near[step], mover("z", step)) for step in (-1, 1)]
        else:
            arrived = yield [(pending.piece(1, dim), mover(axis))]
        pending = Pending(pending.piece(0, dim), *arrived)
    return pending.total()


def spread_job(own, axes, order, turn):
    pieces = own.reshape((1,) * len(axes) + own.shape)
    for axis in order:
        dim = axes.index(axis)
        if axis == "z":
            near = yield [(pieces, mover("z", 1)), (pieces, mover("z", -1))]
            (far,) = yield [(near[0 if turn == 1 else 1], mover("z", turn))]
            pieces = jnp.concatenate([pieces, near[0], far, near[1]], axis=dim)
        else:
            (other,) = yield [(pieces, mover(axis))]
            pieces = jnp.concatenate([pieces, other], axis=dim)
    flat = pieces.reshape((-1,) + own.shape)
    (partner,) = yield [(flat, mover("core"))]
    return partner, flat


def spread_jobs(own, cuts, axes, orders):
    groups = jnp.split(own, cuts, axis=1)
    return [spread_job(*job) for job in zip(groups, [axes] * len(groups), orders, TURNS)]


def gathered_groups(places):
    return [[place[0][half] for place in places] for half in range(2)]


def flip(bits):
    count = lax.axis_size(BOTH)
    return lambda values: lax.ppermute(
        values, BOTH, [(source, source ^ bits) for source in range(count)]
    )


def gather_small_job(values):
    device_count = lax.axis_size(BOTH)
    number = lax.axis_index(BOTH)
    everything = jnp.zeros((device_count,) + values.shape, values.dtype)
    everything = lax.dynamic_update_index_in_dim(everything, values, number, 0)
    bit = 1
    while bit < device_count:
        fan = min(4, device_count // bit)
        start = number // bit * bit
        sent = lax.dynamic_slice_in_dim(everything, start, bit, 0)
        arrived = yield [(sent, flip(k * bit)) for k in range(1, fan)]
        for k, received in enumerate(arrived, 1):
            everything = lax.dynamic_update_slice_in_dim(
                everything, received, start ^ (k * bit), 0
            )
        bit *= fan
    return everything


def reduce_small_job(values):
    number = lax.axis_index(BOTH)
    count = values.shape[0]
    while count > 1:
        fan = min(4, count)
        bit = count // fan
        parts = values.reshape((fan, bit) + values.shape[1:])
        mine = (number // bit) % fan
        pick = lambda place: lax.dynamic_index_in_dim(parts, place, 0, keepdims=False)
        arrived = yield [(pick(mine ^ k), flip(k * bit)) for k in range(1, fan)]
        values = sum(arrived, pick(mine))
        count = bit
    return values[0]


def swap_tensor(values):
    return lax.ppermute(values, "tensor", [(0, 1), (1, 0)])


def swap_job(values):
    (received,) = yield [(values, swap_tensor)]
    return received


def in_order(mine, other):
    first = lax.axis_index("tensor") == 0
    return jnp.where(
        first, jnp.concatenate([mine, other], axis=0), jnp.concatenate([other, mine], axis=0)
    )


def sum_tokens_job(terms):
    low = terms.astype(BF16).reshape((2, terms.shape[0] // 2) + terms.shape[1:])
    half = lax.axis_index("tensor")
    sent = lax.dynamic_index_in_dim(low, 1 - half, 0, keepdims=False)
    kept = lax.dynamic_index_in_dim(low, half, 0, keepdims=False)
    (received,) = yield [(sent, swap_tensor)]
    return kept.astype(F32) + received.astype(F32)


def choose(position_row, capacity):
    slot = lax.broadcasted_iota(jnp.int32, (capacity, position_row.shape[1]), 0).astype(F32)
    picks = [
        (slot == position_row[e : e + 1, :]).astype(F32) for e in range(position_row.shape[0])
    ]
    return picks


def expert_kernel(capacity, widths, token_groups, grad_groups, carried, first, *refs):
    blocks = STEP_BLOCKS
    groups = token_groups + grad_groups
    token_refs, grad_refs, refs = refs[:token_groups], refs[token_groups:groups], refs[groups:]
    position_ref, mask_ref, router_ref, up_ref, up_t_ref, down_t_ref = refs[:6]
    refs = refs[6 + carried :]
    rows_ref, grad_rows_ref, gated_ref, grad_gate_ref, grad_up_ref = refs[:5]
    out_refs, packed_ref = refs[5:-1], refs[-1]
    experts_here = up_ref.shape[0]
    hidden_units = down_t_ref.shape[2]
    width = sum(ref.shape[2] for ref in token_refs)
    first_expert = first[0]
    gates = [[] for _ in range(experts_here)]
    choices = []
    for j in range(blocks):
        picks = choose(position_ref[j], capacity)
        choice = jnp.concatenate(picks, axis=0).astype(BF16)
        choices.append(choice)
        here = slice(j * capacity, (j + 1) * capacity)
        for group_refs, kept_ref in ((token_refs, rows_ref), (grad_refs, grad_rows_ref)):
            start = 0
            for ref in group_refs:
                size = ref.shape[2]
                picked = dot(choice, ref[j]).astype(BF16)
                for e in range(experts_here):
                    kept_ref[e, here, start : start + size] = picked[
                        e * capacity : (e + 1) * capacity
                    ]
                start += size
        logits, start = 0.0, 0
        for ref in token_refs:
            size = ref.shape[2]
            logits = logits + dot(router_ref[:, start : start + size], ref[j], 1, 1)
            start += size
        chosen = mask_ref[j].astype(F32) > 0.5
        top = jnp.max(jnp.where(chosen, logits, -3e38), axis=0, keepdims=True)
        powers = jnp.where(chosen, jnp.exp(jnp.minimum(logits - top, 0.0)), 0.0)
        gate_all = powers / jnp.sum(powers, axis=0, keepdims=True)
        expert_number = lax.broadcasted_iota(jnp.int32, gate_all.shape, 0)
        for e in range(experts_here):
            gate_row = jnp.sum(
                jnp.where(expert_number == first_expert + e, gate_all, 0.0), axis=0, keepdims=True
            )
            gates[e].append(jnp.sum(picks[e] * gate_row, axis=1, keepdims=True))
    for e in range(experts_here):
        both = dot(rows_ref[e], up_ref[e])
        gate_pre = both[:, :hidden_units]
        up_pre = both[:, hidden_units:]
        raw = dot(grad_rows_ref[e], down_t_ref[e])
        sigmoid = 1.0 / (1.0 + jnp.exp(-gate_pre))
        silu = gate_pre * sigmoid
        hidden = silu * up_pre
        gate = jnp.concatenate(gates[e], axis=0)
        grad_gate = jnp.sum(hidden * raw, axis=1, keepdims=True)
        grad_hidden = gate * raw
        grad_gate_pre = (
            grad_hidden * up_pre * sigmoid * (1.0 + gate_pre * (1.0 - sigmoid))
        ).astype(BF16)
        grad_up_pre = (grad_hidden * silu).astype(BF16)
        gated_ref[e] = (gate * hidden).astype(BF16)
        grad_gate_ref[e] = grad_gate_pre
        grad_up_ref[e] = grad_up_pre
        back = dot(grad_gate_pre, up_t_ref[e, :hidden_units, :]) + dot(
            grad_up_pre, up_t_ref[e, hidden_units:, :]
        )
        lane = lax.broadcasted_iota(jnp.int32, (blocks * capacity, LANES), 1)
        extra = jnp.where(lane == first_expert + e, grad_gate, 0.0).astype(BF16)
        back = back.astype(BF16)
        for j in range(blocks):
            packed_ref[j, e * capacity : (e + 1) * capacity, :width] = back[
                j * capacity : (j + 1) * capacity
            ]
            packed_ref[j, e * capacity : (e + 1) * capacity, width:] = extra[
                j * capacity : (j + 1) * capacity
            ]
    for j in range(blocks):
        home = dot(choices[j], packed_ref[j], 0, 0).astype(BF16)
        start = 0
        for out_ref, size in zip(out_refs, widths):
            out_ref[j] = home[:, start : start + size]
            start += size


def whole(shape):
    return pl.BlockSpec(
        shape, lambda i, *scalars: (0,) * len(shape), pipeline_mode=pl.Buffered(1)
    )


def stepped(shape, dim):
    return pl.BlockSpec(
        shape, lambda i, *scalars: tuple(i if d == dim else 0 for d in range(len(shape)))
    )


def expert_grads(
    half, carry, first, tokens, grads, block_start, position, mask,
    router_t, up_both, up_both_t, down_t, capacity, widths,
):
    count = position.shape[0]
    width = sum(group.shape[2] for group in tokens)
    experts_here, hidden_units = down_t.shape[0], down_t.shape[2]
    slots = STEP_BLOCKS * capacity
    expert_count = router_t.shape[0]
    slot_shape = lambda size: jax.ShapeDtypeStruct((experts_here, 2 * count * capacity, size), BF16)
    steps = count // STEP_BLOCKS
    slot_spec = lambda size: pl.BlockSpec(
        (experts_here, slots, size), lambda i, *scalars: (0, i + half * steps, 0)
    )
    before = 1 + len(tokens) + len(grads) + 6
    flops = 2 * count * capacity * experts_here * (7 * hidden_units * width + 3 * LANES * width)
    call = pl.pallas_call(
        functools.partial(
            expert_kernel, capacity, widths, len(tokens), len(grads), len(carry)
        ),
        grid_spec=pltpu.PrefetchScalarGridSpec(
            num_scalar_prefetch=1,
            grid=(steps,),
            in_specs=[
                pl.BlockSpec(
                    (STEP_BLOCKS, LANES, group.shape[2]),
                    lambda i, *scalars: (i + block_start // STEP_BLOCKS, 0, 0),
                )
                for group in (*tokens, *grads)
            ]
            + [
                stepped((STEP_BLOCKS, experts_here, LANES), 0),
                stepped((STEP_BLOCKS, expert_count, LANES), 0),
                whole(router_t.shape),
                whole(up_both.shape),
                whole(up_both_t.shape),
                whole(down_t.shape),
            ]
            + [pl.BlockSpec(memory_space=pl.ANY)] * len(carry),
            out_specs=[slot_spec(width)] * 2
            + [slot_spec(hidden_units)] * 3
            + [stepped((STEP_BLOCKS, LANES, size), 0) for size in widths],
            scratch_shapes=[
                pltpu.VMEM((STEP_BLOCKS, experts_here * capacity, sum(widths)), BF16)
            ],
        ),
        out_shape=[slot_shape(width)] * 2
        + [slot_shape(hidden_units)] * 3
        + [jax.ShapeDtypeStruct((count, LANES, size), BF16) for size in widths],
        compiler_params=pltpu.CompilerParams(vmem_limit_bytes=VMEM_BYTES),
        cost_estimate=pl.CostEstimate(
            flops=flops, transcendentals=0, bytes_accessed=6 * count * LANES * width * 2
        ),
        input_output_aliases={before + n: n for n in range(len(carry))},
        name="expert_grads",
    )
    return call(
        first, *tokens, *grads,
        position, mask, router_t, up_both, up_both_t, down_t, *carry,
    )


def output_kernel(capacity, widths, gated_ref, position_ref, down_ref, *refs):
    out_refs, packed_ref = refs[:-1], refs[-1]
    for e in range(down_ref.shape[0]):
        rows = dot(gated_ref[e], down_ref[e]).astype(BF16)
        for j in range(STEP_BLOCKS):
            packed_ref[j, e * capacity : (e + 1) * capacity, :] = rows[
                j * capacity : (j + 1) * capacity
            ]
    for j in range(STEP_BLOCKS):
        choice = jnp.concatenate(choose(position_ref[j], capacity), axis=0).astype(BF16)
        home = dot(choice, packed_ref[j], 0, 0).astype(BF16)
        start = 0
        for out_ref, size in zip(out_refs, widths):
            out_ref[j] = home[:, start : start + size]
            start += size


def expert_outputs(half, gated, position, down, capacity, widths):
    count = position.shape[0]
    experts_here, hidden_units, width = down.shape
    slots = STEP_BLOCKS * capacity
    steps = count // STEP_BLOCKS
    call = pl.pallas_call(
        functools.partial(output_kernel, capacity, widths),
        grid=(steps,),
        in_specs=[
            pl.BlockSpec(
                (experts_here, slots, hidden_units), lambda i: (0, i + half * steps, 0)
            ),
            stepped((STEP_BLOCKS, experts_here, LANES), 0),
            whole(down.shape),
        ],
        out_specs=[stepped((STEP_BLOCKS, LANES, size), 0) for size in widths],
        out_shape=[jax.ShapeDtypeStruct((count, LANES, size), BF16) for size in widths],
        scratch_shapes=[pltpu.VMEM((STEP_BLOCKS, experts_here * capacity, width), BF16)],
        compiler_params=pltpu.CompilerParams(vmem_limit_bytes=VMEM_BYTES),
        cost_estimate=pl.CostEstimate(
            flops=2 * count * capacity * experts_here * (hidden_units * width + LANES * width),
            transcendentals=0,
            bytes_accessed=2 * count * LANES * width * 2,
        ),
        name="expert_outputs",
    )
    return call(gated, position, down)


def chunk_kernel(widths, perm, *refs):
    left = jnp.concatenate([ref[...] for ref in refs[:STEP_BLOCKS]], axis=1)
    product = dot(left, refs[STEP_BLOCKS][...], 0, 0).astype(BF16)
    start = 0
    for out_ref, size in zip(refs[STEP_BLOCKS + 1 :], widths):
        for j in range(STEP_BLOCKS):
            out_ref[j] = product[j * LANES : (j + 1) * LANES, start : start + size]
        start += size


def chunk_products(perm, left, right, widths):
    count = perm.shape[0]
    tokens = left.shape[0]

    def column_block(place):
        return pl.BlockSpec((tokens, LANES), lambda i, perm: (0, perm[i * STEP_BLOCKS + place]))

    call = pl.pallas_call(
        functools.partial(chunk_kernel, widths),
        grid_spec=pltpu.PrefetchScalarGridSpec(
            num_scalar_prefetch=1,
            grid=(count // STEP_BLOCKS,),
            in_specs=[column_block(j) for j in range(STEP_BLOCKS)] + [whole(right.shape)],
            out_specs=[stepped((STEP_BLOCKS, LANES, size), 0) for size in widths],
        ),
        out_shape=[jax.ShapeDtypeStruct((count, LANES, size), BF16) for size in widths],
        compiler_params=pltpu.CompilerParams(vmem_limit_bytes=VMEM_BYTES),
        cost_estimate=pl.CostEstimate(
            flops=2 * count * LANES * tokens * right.shape[1],
            transcendentals=0,
            bytes_accessed=count * LANES * right.shape[1] * 2,
        ),
        name="chunk_products",
    )
    return call(perm, *([left] * STEP_BLOCKS), right)


def block_orders(lattice, device_count):
    if not lattice:
        numbers = jnp.arange(device_count, dtype=jnp.int32)
        return numbers[: device_count // 2], numbers[device_count // 2 :]
    spot = my_spot()
    dz, dx, dy = (grid.reshape(-1) for grid in np.indices((4, 2, 2)).astype(np.int32))
    chip = (spot["z"] - dz + 4) % 4 * 2 + (spot["x"] + dx) % 2
    orders = []
    for dc in (1, 0):
        core = (spot["core"] + dc) % 2
        orders.append(((chip * 2 + core) * 2 + (spot["y"] + dy) % 2).astype(jnp.int32))
    return orders


def chunk_orders():
    spot = my_spot()
    dz, dx = (grid.reshape(-1) for grid in np.indices((4, 2)).astype(np.int32))
    chip = (spot["z"] - dz + 4) % 4 * 2 + (spot["x"] + dx) % 2
    return [(chip * 2 + (spot["core"] + dc) % 2).astype(jnp.int32) for dc in (1, 0)]


TOKEN_ORDERS = (("x", "y", "z"), ("y", "z", "x"), ("z", "x", "y"))
EARLY_ORDERS = (("z", "x", "y"), ("x", "z", "y"))
LATE_ORDERS = (("y", "x", "z"), ("y", "z", "x"))
GATHER_ORDERS = (("z", "y", "x"), ("x", "z", "y"), ("y", "x", "z"))
CHUNK_ORDERS = (("x", "z"), ("z", "x"))
TURNS = (1, -1, 1)


def scatter_job(partner, own):
    everything = jnp.concatenate([partner, own], axis=0)
    total = lax.psum_scatter(everything, BOTH, scatter_dimension=0, tiled=True)
    return total[0].astype(F32)
    yield


def tokens_home_jobs(lattice, partner, own, received, orders):
    jobs = []
    for n, order in enumerate(orders):
        if not lattice:
            jobs.append(scatter_job(partner[n], own[n]))
            continue
        shape = (4, 2, 2) + own[n].shape[1:]
        mine = own[n].reshape(shape)
        both = Pending(mine, received[n].reshape(shape))
        jobs.append(home_job(None, both, "zxy", order, TURNS[n]))
    return jobs


def product_job(left, right):
    product = dot(left, right, 0, 0).astype(BF16)
    return lax.psum_scatter(product, DP, scatter_dimension=0, tiled=True).astype(F32)
    yield


def weight_grads_chunks(lattice, left, right, widths):
    if not lattice:
        return left, right
    return tuple(chunk_products(order, left, right, widths) for order in chunk_orders())


def weight_grads_jobs(lattice, first, second):
    if not lattice:
        return [product_job(first, second)]
    jobs = []
    for n, order in enumerate(CHUNK_ORDERS):
        shape = (4, 2) + first[n].shape[1:]
        jobs.append(
            home_job(first[n].reshape(shape), second[n].reshape(shape), "zx", order, TURNS[n])
        )
    return jobs


def on_device(
    inputs,
    input_gain,
    post_gain,
    query_gain,
    key_gain,
    query_weight,
    key_projection_matrix,
    value_projection_matrix,
    output_weight,
    router_weight,
    gate_weight,
    up_weight,
    down_weight,
    routes,
    cotangent,
):
    dp_count, tensor_count = lax.axis_size(DP), lax.axis_size("tensor")
    device_count = dp_count * tensor_count
    lattice = is_lattice(dp_count, tensor_count)
    row_count, width = inputs.shape
    experts = router_weight.shape[1]
    experts_here = gate_weight.shape[0]
    capacity = 2 * row_count * routes.shape[1] // experts

    links, slow, outer = Links(), Links(), Links()
    projections = jnp.concatenate(
        [query_weight, key_projection_matrix, value_projection_matrix], axis=0
    )
    query_rows, key_rows = query_weight.shape[0], key_projection_matrix.shape[0]

    expert_ids = jnp.arange(experts, dtype=jnp.int32)
    chosen_mask = jnp.any(routes[:, :, None] == expert_ids[None, None, :], axis=1)
    small = [input_gain, post_gain, query_gain, key_gain]
    sizes = [item.shape[0] for item in small]
    flat = jnp.concatenate(small)
    padded = -(-flat.shape[0] // LANES) * LANES
    flat = jnp.pad(flat, (0, padded - flat.shape[0]))
    router_lines = router_weight.size // LANES
    payload = jnp.concatenate(
        [
            router_weight.reshape(router_lines, LANES),
            flat.reshape(-1, LANES),
            chosen_mask.T.astype(BF16),
        ],
        axis=0,
    )
    gathered_at, other_inputs_at = links.add(gather_small_job(payload), swap_job(inputs))
    projections_full = lax.all_gather(projections.T, DP, axis=0, tiled=True)
    if lattice:
        cuts = (width // 8 * 3, width // 16 * 11)
        grads_at = slow.add(*spread_jobs(cotangent, cuts[:1], "zxy", EARLY_ORDERS))
        links.marks = links.marks + slow.marks

    def join_up(gate, up):
        return jnp.concatenate([gate, up], axis=2)

    def turn_last(values):
        return with_layout_constraint(jnp.swapaxes(values, 1, 2), Layout((0, 1, 2)))

    up_both = links.round(join_up, gate_weight, up_weight)
    output_held = after(output_weight, up_both[0, :8, :LANES])
    output_full = lax.all_gather(output_held, DP, axis=0, tiled=True)
    slow.aside(links)
    up_both_t = links.round(turn_last, up_both)
    slow.aside(links)
    down_t = links.round(turn_last, down_weight)
    slow.aside(links)
    while gathered_at[0] is None:
        links.round()
    gathered, other_inputs = gathered_at[0], other_inputs_at[0]

    router_full = gathered[:, :router_lines].reshape(width, experts)
    flat_all = gathered[:, router_lines : router_lines + padded // LANES].reshape(
        device_count, padded
    )
    starts = np.cumsum([0] + sizes)
    input_scale, post_scale, query_scale, key_scale = (
        flat_all[:, starts[n] : starts[n + 1]].reshape(-1).astype(F32) for n in range(4)
    )
    mask_all = gathered[:, router_lines + padded // LANES :]
    first_expert = lax.axis_index(DP) * experts_here
    mask_here = lax.dynamic_slice_in_dim(mask_all, first_expert, experts_here, axis=1)
    earlier = jnp.asarray(np.triu(np.ones((row_count, row_count), np.float32), 1), BF16)
    rank = jnp.einsum("bet,tu->beu", mask_here, earlier, preferred_element_type=F32)
    position = jnp.where(mask_here > 0.5, rank, -1.0)
    orders = block_orders(lattice, device_count)
    positions = [position[order] for order in orders]
    masks = [mask_all[order] for order in orders]
    router_t = router_full.T

    both_inputs = in_order(inputs, other_inputs).astype(F32)
    residual_in = inputs.astype(F32)
    sequence = norm_rows(both_inputs, input_scale)[0].astype(BF16)
    _, input_hat, input_inv = norm_rows(residual_in, input_scale)
    seq_len = sequence.shape[0]
    local_heads = query_rows // HEAD_SIZE
    local_groups = key_rows // HEAD_SIZE
    per_group = local_heads // local_groups
    cosine_table, sine_table = rope_tables(seq_len, HEAD_SIZE)
    cosine, sine = cosine_table[:, None, :], sine_table[:, None, :]
    score_scale = 1.0 / math.sqrt(HEAD_SIZE)

    def project(projections_full):
        projected = dot(sequence, projections_full)
        query_raw = projected[:, :query_rows].reshape(seq_len, local_heads, HEAD_SIZE)
        key_raw = projected[:, query_rows : query_rows + key_rows].reshape(
            seq_len, local_groups, HEAD_SIZE
        )
        value_low = (
            projected[:, query_rows + key_rows :]
            .astype(BF16)
            .reshape(seq_len, local_groups, HEAD_SIZE)
        )
        query_norm, query_hat, query_inv = norm_rows(query_raw, query_scale)
        query_low = (query_norm * cosine + rotate_half(query_norm) * sine).astype(BF16)
        key_norm, key_hat, key_inv = norm_rows(key_raw, key_scale)
        key_low = (key_norm * cosine + rotate_half(key_norm) * sine).astype(BF16)
        query_groups = query_low.reshape(seq_len, local_groups, per_group, HEAD_SIZE)
        return query_groups, query_hat, query_inv, key_hat, key_inv, key_low, value_low

    def attention(query_groups, key_low, value_low):
        scores = (
            jnp.einsum("qhgd,khd->hgqk", query_groups, key_low, preferred_element_type=F32)
            * score_scale
        )
        row_index = jnp.arange(seq_len, dtype=jnp.int32)
        scores = jnp.where(row_index[None, :] <= row_index[:, None], scores, -1e30)
        attend = jax.nn.softmax(scores, axis=-1)
        attend_low = attend.astype(BF16)
        mixed_low = (
            jnp.einsum("hgqk,khd->qhgd", attend_low, value_low, preferred_element_type=F32)
            .astype(BF16)
            .reshape(seq_len, query_rows)
        )
        return mixed_low, attend, attend_low

    query_groups, query_hat, query_inv, key_hat, key_inv, key_low, value_low = links.round(
        project, projections_full
    )
    mixed_low, attend, attend_low = links.round(attention, query_groups, key_low, value_low)
    slow.aside(links)
    links.finish()
    ready = (positions, masks, router_t, up_both, up_both_t, down_t)
    mixed_low, (positions, masks, router_t, up_both, up_both_t, down_t) = (
        lax.optimization_barrier((mixed_low, ready))
    )
    mixed_out = dot(after(mixed_low, links.marks), output_full, 1, 1)
    (mixed_home,) = links.add(sum_tokens_job(mixed_out))
    links.finish()
    residual_mid = residual_in + mixed_home[0]
    post_norm, post_hat, post_inv = norm_rows(residual_mid, post_scale)
    post_low = post_norm.astype(BF16)
    block_starts = (0, 0)
    if lattice:
        tokens_at = links.add(*spread_jobs(post_low, cuts, "zxy", GATHER_ORDERS))
        slow.aside(links)
        links.finish()
        all_tokens, all_grads = gathered_groups(tokens_at), gathered_groups(grads_at)
    else:
        block_starts = (0, device_count // 2)
        all_tokens, all_grads = (
            ([lax.all_gather(values[None], BOTH, axis=0, tiled=True)],) * 2
            for values in (post_low, cotangent)
        )

    logits = dot(post_low, router_full)
    top = jnp.max(jnp.where(chosen_mask, logits, -3e38), axis=-1, keepdims=True)
    powers = jnp.where(chosen_mask, jnp.exp(jnp.minimum(logits - top, 0.0)), 0.0)
    gates = powers / jnp.sum(powers, axis=-1, keepdims=True)

    wide = width // 8 * 3
    widths = (wide, wide, width - 2 * wide + LANES)
    first_scalar = first_expert.astype(jnp.int32).reshape(1)

    def half_grads(half, carry):
        return expert_grads(
            half, carry, first_scalar, all_tokens[half], all_grads[half],
            block_starts[half], positions[half], masks[half],
            router_t, up_both, up_both_t, down_t, capacity, widths,
        )

    results = half_grads(0, ())
    partner = results[5:]
    received = [hop(group, "core") for group in partner] if lattice else None
    results = half_grads(1, results[:5])
    rows, grad_rows, gated, grad_gate_pre, grad_up_pre = results[:5]
    own = results[5:]

    def slot_product(left, right):
        return jnp.einsum("esd,esf->edf", left, right, preferred_element_type=F32)

    out_widths = (wide, width - wide)

    def outputs(gated):
        return [
            expert_outputs(n, gated, positions[n], down_weight, capacity, out_widths)
            for n in range(2)
        ]

    home = links.add(*tokens_home_jobs(lattice, partner, own, received, TOKEN_ORDERS))
    out_partner, out_own = links.round(outputs, gated)
    out_received = [hop(group, "core") for group in out_partner] if lattice else None
    grad_gate_w = links.round(slot_product, rows, grad_gate_pre)
    grad_down = links.round(slot_product, gated, grad_rows)
    links.finish()
    home = [place[0] for place in home]

    grad_out = cotangent.astype(F32)
    grad_post = jnp.concatenate([home[0], home[1], home[2][:, : width - 2 * wide]], axis=1)
    start = width - 2 * wide
    grad_gates = home[2][:, start : start + experts]
    grad_logits = (
        gates * (grad_gates - jnp.sum(gates * grad_gates, axis=-1, keepdims=True))
    ).astype(BF16)
    grad_post = grad_post + dot(grad_logits, router_full, 1, 1)
    grad_mid_norm, post_terms = norm_back(grad_post, post_scale, post_hat, post_inv)
    grad_mid = grad_out + grad_mid_norm
    grad_mid_low = grad_mid.astype(BF16)
    (other_grads,) = links.add(swap_job(grad_mid_low))
    out_jobs = tokens_home_jobs(lattice, out_partner, out_own, out_received, LATE_ORDERS)
    out_home = outer.add(*out_jobs)
    links.marks = links.marks + outer.marks
    grad_up_w = slot_product(*after((rows, grad_up_pre), links.marks))
    links.marks = [grad_up_w]
    while other_grads[0] is None:
        swapped = links.active.pop(0)
        links.advance(*swapped[:3], after(swapped[3], links.marks))
    grad_attention = in_order(grad_mid_low, other_grads[0])


    def back_scores(grad_attention):
        grad_mixed = dot(grad_attention, output_full).astype(BF16)
        grad_groups = grad_mixed.reshape(seq_len, local_groups, per_group, HEAD_SIZE)
        grad_attend = jnp.einsum(
            "qhgd,khd->hgqk", grad_groups, value_low, preferred_element_type=F32
        )
        row_inner = jnp.sum(attend * grad_attend, axis=-1, keepdims=True)
        grad_scores = (attend * (grad_attend - row_inner)).astype(BF16)
        return grad_groups, grad_scores

    out_split = query_rows // 8 * 3
    chunks = weight_grads_chunks(
        lattice, grad_attention, mixed_low, (out_split, query_rows - out_split)
    )
    grad_output_at = slow.add(*weight_grads_jobs(lattice, *chunks))
    links.marks = links.marks + slow.marks
    grad_groups, grad_scores = links.round(back_scores, grad_attention)
    slow.aside(links)
    grad_router = dot(post_low, grad_logits, 0, 0)
    grad_post_gain = jnp.sum(post_terms, axis=0)
    def back_heads(grad_groups, grad_scores):
        grad_value = jnp.einsum(
            "hgqk,qhgd->khd", attend_low, grad_groups, preferred_element_type=F32
        )
        grad_key_rot = (
            jnp.einsum("hgqk,qhgd->khd", grad_scores, query_groups, preferred_element_type=F32)
            * score_scale
        )
        grad_query_rot = (
            jnp.einsum("hgqk,khd->qhgd", grad_scores, key_low, preferred_element_type=F32)
            * score_scale
        ).reshape(seq_len, local_heads, HEAD_SIZE)
        return grad_value, grad_key_rot, grad_query_rot

    grad_value, grad_key_rot, grad_query_rot = links.round(back_heads, grad_groups, grad_scores)

    def back_norms(grad_query_rot):
        grad_query_norm = grad_query_rot * cosine + rotate_back(grad_query_rot * sine)
        grad_query_raw, query_terms = norm_back(grad_query_norm, query_scale, query_hat, query_inv)
        return grad_query_raw.reshape(seq_len, query_rows).astype(BF16), query_terms

    grad_query_low, query_terms = links.round(back_norms, grad_query_rot)
    grad_query_gain = jnp.sum(query_terms, axis=(0, 1))
    grad_key_norm = grad_key_rot * cosine + rotate_back(grad_key_rot * sine)
    grad_key_raw, key_terms = norm_back(grad_key_norm, key_scale, key_hat, key_inv)
    grad_key_gain = jnp.sum(key_terms, axis=(0, 1))
    grad_projected = jnp.concatenate(
        [
            grad_query_low,
            grad_key_raw.reshape(seq_len, key_rows).astype(BF16),
            grad_value.reshape(seq_len, key_rows).astype(BF16),
        ],
        axis=1,
    )
    total_rows = query_rows + 2 * key_rows
    split = total_rows // LANES * 2 // 5 * LANES
    chunks = weight_grads_chunks(
        lattice, sequence, grad_projected, (split, total_rows - split)
    )
    grad_projections_at = links.add(
        *weight_grads_jobs(lattice, *chunks), rank=-1
    )
    slow.aside(links)
    normed_parts = links.round(
        lambda grad: dot(grad, projections_full, 1, 1), grad_projected
    )
    (grad_normed,) = links.add(sum_tokens_job(normed_parts), rank=-1)
    links.round()
    slow.aside(links)
    outer.aside(links)
    grad_in_norm, input_terms = norm_back(grad_normed[0], input_scale, input_hat, input_inv)
    grad_input_gain = jnp.sum(input_terms, axis=0)
    grad_inputs = (grad_mid + grad_in_norm).astype(BF16)
    late_parts = [grad_router, grad_post_gain, grad_input_gain, grad_query_gain, grad_key_gain]
    flat = jnp.concatenate([part.reshape(device_count, -1) for part in late_parts], axis=1)
    flat = jnp.pad(flat, ((0, 0), (0, -flat.shape[1] % LANES)))
    (late,) = links.add(reduce_small_job(flat.reshape(device_count, -1, LANES)))
    while links.active or slow.active or outer.active:
        links.round()
        slow.aside(links)
        outer.aside(links)
    result = (residual_mid + jnp.concatenate([p[0] for p in out_home], axis=1)).astype(BF16)
    grad_output_w = jnp.concatenate([place[0] for place in grad_output_at], axis=1)
    grad_projections = jnp.concatenate([place[0] for place in grad_projections_at], axis=1).T
    grad_query_w = grad_projections[:query_rows]
    grad_key_w = grad_projections[query_rows : query_rows + key_rows]
    grad_value_w = grad_projections[query_rows + key_rows :]
    bounds = np.cumsum([0, router_weight.size, sizes[1], sizes[0], sizes[2], sizes[3]])
    late = late[0].reshape(-1)
    grad_router, grad_post_gain, grad_input_gain, grad_query_gain, grad_key_gain = (
        late[bounds[n] : bounds[n + 1]] for n in range(5)
    )
    grad_router = grad_router.reshape(router_weight.shape)
    return (
        result,
        grad_inputs,
        grad_input_gain,
        grad_post_gain,
        grad_query_gain,
        grad_key_gain,
        grad_query_w,
        grad_key_w,
        grad_value_w,
        grad_output_w,
        grad_router,
        grad_gate_w,
        grad_up_w,
        grad_down,
    )


def solution(mesh):
    dp_count, tensor_count = mesh.devices.shape
    split = jax.sharding.Mesh(
        mesh.devices.reshape(dp_count // 2, 2, tensor_count), ("chip", "core", "tensor")
    )
    tokens, line = P(BOTH, None), P(BOTH)
    gated = P(DP, None, "tensor")
    weights = (P("tensor", DP),) * 3 + (P(DP, "tensor"), tokens, gated, gated, P(DP, "tensor", None))
    return jax.shard_map(
        on_device,
        mesh=split,
        in_specs=(tokens,) + (line,) * 4 + weights + (tokens, tokens),
        out_specs=(tokens, tokens) + (line,) * 4 + weights,
        check_vma=False,
    )
```

```python
import functools
import math

import jax
import jax.numpy as jnp
import numpy as np
from jax import lax
from jax.experimental import pallas as pl
from jax.experimental.layout import Layout, with_layout_constraint
from jax.experimental.pallas import tpu as pltpu
from jax.sharding import PartitionSpec as P

HEAD_SIZE = 128
LANES = 128
EPSILON = 1e-06
ROPE_BASE = 1000000.0
DP = ("chip", "core")
BOTH = ("chip", "core", "tensor")
BF16 = jnp.bfloat16
F32 = jnp.float32
STEP_BLOCKS = 4
VMEM_BYTES = 60 * 1024 * 1024


def norm_rows(values, weights):
    inverse = lax.rsqrt(jnp.mean(values * values, axis=-1, keepdims=True) + EPSILON)
    normalized_rows = values * inverse
    return (normalized_rows * weights, normalized_rows, inverse)


def norm_back(upstream, weights, normalized_rows, inverse):
    scaled = upstream * weights
    inner_term = jnp.mean(scaled * normalized_rows, axis=-1, keepdims=True)
    return (inverse * (scaled - normalized_rows * inner_term), upstream * normalized_rows)


def rope_tables(length, head_width):
    half_width = head_width // 2
    frequency = jnp.exp(
        jnp.arange(half_width, dtype=F32) * (-2.0 * math.log(ROPE_BASE) / head_width)
    )
    angles = jnp.arange(length, dtype=F32)[:, None] * frequency[None, :]
    angles = jnp.concatenate([angles, angles], axis=-1)
    return (jnp.cos(angles), jnp.sin(angles))


def rotate_half(values):
    half_width = values.shape[-1] // 2
    return jnp.concatenate([-values[..., half_width:], values[..., :half_width]], axis=-1)


def rotate_back(values):
    half_width = values.shape[-1] // 2
    return jnp.concatenate([values[..., half_width:], -values[..., :half_width]], axis=-1)


def dot(left, right, left_dim=1, right_dim=0):
    return lax.dot_general(
        left, right, (((left_dim,), (right_dim,)), ((), ())), preferred_element_type=F32
    )


LATTICE = {"z": 4, "x": 2, "core": 2, "y": 2}


def is_lattice(dp_count, tensor_count):
    return dp_count == 16 and tensor_count == 2


def hop(values, axis, step=1):
    sizes = tuple(LATTICE.values())
    place = list(LATTICE).index(axis)
    pairs = []
    for source in range(math.prod(sizes)):
        spot = list(np.unravel_index(source, sizes))
        spot[place] = (spot[place] + step) % sizes[place]
        pairs.append((source, int(np.ravel_multi_index(spot, sizes))))
    return lax.ppermute(values, BOTH, pairs)


def my_spot():
    chip_core = lax.axis_index(DP)
    return {
        "z": chip_core // 4,
        "x": (chip_core // 2) % 2,
        "core": chip_core % 2,
        "y": lax.axis_index("tensor"),
    }


def add_low(first, second):
    return (first.astype(F32) + second.astype(F32)).astype(BF16)


class Pending:
    def __init__(self, *parts):
        self.parts = parts

    def total(self):
        return sum(part.astype(F32) for part in self.parts)

    def piece(self, place, dim):
        picked = [lax.index_in_dim(part, place, dim, keepdims=False) for part in self.parts]
        return Pending(*picked).total().astype(BF16)


def after(values, others):
    return lax.optimization_barrier((values, others))[0]


class Links:
    def __init__(self):
        self.active = []
        self.marks = []

    def add(self, *jobs, rank=0):
        places = [[None] for _ in jobs]
        for job, place in zip(jobs, places):
            self.advance(rank, job, place, None)
        return places

    def advance(self, rank, job, place, arrived):
        try:
            sends = job.send(arrived)
        except StopIteration as stop:
            place[0] = stop.value
            return
        sent = lax.optimization_barrier(tuple(array for array, _ in sends))
        self.marks += sent
        moved = [move(array) for (_, move), array in zip(sends, sent)]
        self.active.append((rank, job, place, moved))

    def round(self, work=None, *operands):
        moving, self.active = sorted(self.active, key=lambda entry: entry[0]), []
        result = None
        if work is not None:
            result = work(*(after(operands, self.marks) if self.marks else operands))
            self.marks = jax.tree.leaves(result)[:1]
        for rank, job, place, moved in moving:
            if self.marks:
                moved = after(moved, self.marks)
            self.marks = []
            self.advance(rank, job, place, moved)
        return result

    def finish(self):
        while self.active:
            self.round()

    def aside(self, main):
        self.marks = main.marks
        self.round()
        main.marks = self.marks


def mover(axis, step=1):
    return lambda values: hop(values, axis, step)


def home_job(partner, own, axes, order, turn):
    axes = list(axes)
    if partner is None:
        pending = own
    else:
        (received,) = yield [(partner, mover("core"))]
        pending = Pending(own, received)
    for axis in order:
        dim = axes.index(axis)
        axes.remove(axis)
        if axis == "z":
            (received,) = yield [(pending.piece(2, dim), mover("z", turn))]
            near = {-1: pending.piece(1, dim), 1: pending.piece(3, dim)}
            near[turn] = add_low(near[turn], received)
            arrived = yield [(near[step], mover("z", step)) for step in (-1, 1)]
        else:
            arrived = yield [(pending.piece(1, dim), mover(axis))]
        pending = Pending(pending.piece(0, dim), *arrived)
    return pending.total()


def spread_job(own, axes, order, turn):
    pieces = own.reshape((1,) * len(axes) + own.shape)
    for axis in order:
        dim = axes.index(axis)
        if axis == "z":
            near = yield [(pieces, mover("z", 1)), (pieces, mover("z", -1))]
            (far,) = yield [(near[0 if turn == 1 else 1], mover("z", turn))]
            pieces = jnp.concatenate([pieces, near[0], far, near[1]], axis=dim)
        else:
            (other,) = yield [(pieces, mover(axis))]
            pieces = jnp.concatenate([pieces, other], axis=dim)
    flat = pieces.reshape((-1,) + own.shape)
    (partner,) = yield [(flat, mover("core"))]
    return partner, flat


def spread_jobs(own, cuts, axes, orders):
    groups = jnp.split(own, cuts, axis=1)
    return [spread_job(*job) for job in zip(groups, [axes] * len(groups), orders, TURNS)]


def gathered_groups(places):
    return [[place[0][half] for place in places] for half in range(2)]


def flip(bits):
    count = lax.axis_size(BOTH)
    return lambda values: lax.ppermute(
        values, BOTH, [(source, source ^ bits) for source in range(count)]
    )


def gather_small_job(values):
    device_count = lax.axis_size(BOTH)
    number = lax.axis_index(BOTH)
    everything = jnp.zeros((device_count,) + values.shape, values.dtype)
    everything = lax.dynamic_update_index_in_dim(everything, values, number, 0)
    bit = 1
    while bit < device_count:
        fan = min(4, device_count // bit)
        start = number // bit * bit
        sent = lax.dynamic_slice_in_dim(everything, start, bit, 0)
        arrived = yield [(sent, flip(k * bit)) for k in range(1, fan)]
        for k, received in enumerate(arrived, 1):
            everything = lax.dynamic_update_slice_in_dim(
                everything, received, start ^ (k * bit), 0
            )
        bit *= fan
    return everything


def reduce_small_job(values):
    number = lax.axis_index(BOTH)
    count = values.shape[0]
    while count > 1:
        fan = min(4, count)
        bit = count // fan
        parts = values.reshape((fan, bit) + values.shape[1:])
        mine = (number // bit) % fan
        pick = lambda place: lax.dynamic_index_in_dim(parts, place, 0, keepdims=False)
        arrived = yield [(pick(mine ^ k), flip(k * bit)) for k in range(1, fan)]
        values = sum(arrived, pick(mine))
        count = bit
    return values[0]


def swap_tensor(values):
    return lax.ppermute(values, "tensor", [(0, 1), (1, 0)])


def swap_job(values):
    (received,) = yield [(values, swap_tensor)]
    return received


def in_order(mine, other):
    first = lax.axis_index("tensor") == 0
    return jnp.where(
        first, jnp.concatenate([mine, other], axis=0), jnp.concatenate([other, mine], axis=0)
    )


def sum_tokens_job(terms):
    low = terms.astype(BF16).reshape((2, terms.shape[0] // 2) + terms.shape[1:])
    half = lax.axis_index("tensor")
    sent = lax.dynamic_index_in_dim(low, 1 - half, 0, keepdims=False)
    kept = lax.dynamic_index_in_dim(low, half, 0, keepdims=False)
    (received,) = yield [(sent, swap_tensor)]
    return kept.astype(F32) + received.astype(F32)


def choose(position_row, capacity):
    slot = lax.broadcasted_iota(jnp.int32, (capacity, position_row.shape[1]), 0).astype(F32)
    picks = [
        (slot == position_row[e : e + 1, :]).astype(F32) for e in range(position_row.shape[0])
    ]
    return picks


def expert_kernel(capacity, widths, token_groups, grad_groups, carried, first, *refs):
    blocks = STEP_BLOCKS
    groups = token_groups + grad_groups
    token_refs, grad_refs, refs = refs[:token_groups], refs[token_groups:groups], refs[groups:]
    position_ref, mask_ref, router_ref, up_ref, up_t_ref, down_t_ref = refs[:6]
    refs = refs[6 + carried :]
    rows_ref, grad_rows_ref, gated_ref, grad_gate_ref, grad_up_ref = refs[:5]
    out_refs, packed_ref = refs[5:-1], refs[-1]
    experts_here = up_ref.shape[0]
    hidden_units = down_t_ref.shape[2]
    width = sum(ref.shape[2] for ref in token_refs)
    first_expert = first[0]
    gates = [[] for _ in range(experts_here)]
    choices = []
    for j in range(blocks):
        picks = choose(position_ref[j], capacity)
        choice = jnp.concatenate(picks, axis=0).astype(BF16)
        choices.append(choice)
        here = slice(j * capacity, (j + 1) * capacity)
        for group_refs, kept_ref in ((token_refs, rows_ref), (grad_refs, grad_rows_ref)):
            start = 0
            for ref in group_refs:
                size = ref.shape[2]
                picked = dot(choice, ref[j]).astype(BF16)
                for e in range(experts_here):
                    kept_ref[e, here, start : start + size] = picked[
                        e * capacity : (e + 1) * capacity
                    ]
                start += size
        logits, start = 0.0, 0
        for ref in token_refs:
            size = ref.shape[2]
            logits = logits + dot(router_ref[:, start : start + size], ref[j], 1, 1)
            start += size
        chosen = mask_ref[j].astype(F32) > 0.5
        top = jnp.max(jnp.where(chosen, logits, -3e38), axis=0, keepdims=True)
        powers = jnp.where(chosen, jnp.exp(jnp.minimum(logits - top, 0.0)), 0.0)
        gate_all = powers / jnp.sum(powers, axis=0, keepdims=True)
        expert_number = lax.broadcasted_iota(jnp.int32, gate_all.shape, 0)
        for e in range(experts_here):
            gate_row = jnp.sum(
                jnp.where(expert_number == first_expert + e, gate_all, 0.0), axis=0, keepdims=True
            )
            gates[e].append(jnp.sum(picks[e] * gate_row, axis=1, keepdims=True))
    for e in range(experts_here):
        both = dot(rows_ref[e], up_ref[e])
        gate_pre = both[:, :hidden_units]
        up_pre = both[:, hidden_units:]
        raw = dot(grad_rows_ref[e], down_t_ref[e])
        sigmoid = 1.0 / (1.0 + jnp.exp(-gate_pre))
        silu = gate_pre * sigmoid
        hidden = silu * up_pre
        gate = jnp.concatenate(gates[e], axis=0)
        grad_gate = jnp.sum(hidden * raw, axis=1, keepdims=True)
        grad_hidden = gate * raw
        grad_gate_pre = (
            grad_hidden * up_pre * sigmoid * (1.0 + gate_pre * (1.0 - sigmoid))
        ).astype(BF16)
        grad_up_pre = (grad_hidden * silu).astype(BF16)
        gated_ref[e] = (gate * hidden).astype(BF16)
        grad_gate_ref[e] = grad_gate_pre
        grad_up_ref[e] = grad_up_pre
        back = dot(grad_gate_pre, up_t_ref[e, :hidden_units, :]) + dot(
            grad_up_pre, up_t_ref[e, hidden_units:, :]
        )
        lane = lax.broadcasted_iota(jnp.int32, (blocks * capacity, LANES), 1)
        extra = jnp.where(lane == first_expert + e, grad_gate, 0.0).astype(BF16)
        back = back.astype(BF16)
        for j in range(blocks):
            packed_ref[j, e * capacity : (e + 1) * capacity, :width] = back[
                j * capacity : (j + 1) * capacity
            ]
            packed_ref[j, e * capacity : (e + 1) * capacity, width:] = extra[
                j * capacity : (j + 1) * capacity
            ]
    for j in range(blocks):
        home = dot(choices[j], packed_ref[j], 0, 0).astype(BF16)
        start = 0
        for out_ref, size in zip(out_refs, widths):
            out_ref[j] = home[:, start : start + size]
            start += size


def whole(shape):
    return pl.BlockSpec(
        shape, lambda i, *scalars: (0,) * len(shape), pipeline_mode=pl.Buffered(1)
    )


def stepped(shape, dim):
    return pl.BlockSpec(
        shape, lambda i, *scalars: tuple(i if d == dim else 0 for d in range(len(shape)))
    )


def expert_grads(
    half, carry, first, tokens, grads, block_start, position, mask,
    router_t, up_both, up_both_t, down_t, capacity, widths,
):
    count = position.shape[0]
    width = sum(group.shape[2] for group in tokens)
    experts_here, hidden_units = down_t.shape[0], down_t.shape[2]
    slots = STEP_BLOCKS * capacity
    expert_count = router_t.shape[0]
    slot_shape = lambda size: jax.ShapeDtypeStruct((experts_here, 2 * count * capacity, size), BF16)
    steps = count // STEP_BLOCKS
    slot_spec = lambda size: pl.BlockSpec(
        (experts_here, slots, size), lambda i, *scalars: (0, i + half * steps, 0)
    )
    before = 1 + len(tokens) + len(grads) + 6
    flops = 2 * count * capacity * experts_here * (7 * hidden_units * width + 3 * LANES * width)
    call = pl.pallas_call(
        functools.partial(
            expert_kernel, capacity, widths, len(tokens), len(grads), len(carry)
        ),
        grid_spec=pltpu.PrefetchScalarGridSpec(
            num_scalar_prefetch=1,
            grid=(steps,),
            in_specs=[
                pl.BlockSpec(
                    (STEP_BLOCKS, LANES, group.shape[2]),
                    lambda i, *scalars: (i + block_start // STEP_BLOCKS, 0, 0),
                )
                for group in (*tokens, *grads)
            ]
            + [
                stepped((STEP_BLOCKS, experts_here, LANES), 0),
                stepped((STEP_BLOCKS, expert_count, LANES), 0),
                whole(router_t.shape),
                whole(up_both.shape),
                whole(up_both_t.shape),
                whole(down_t.shape),
            ]
            + [pl.BlockSpec(memory_space=pl.ANY)] * len(carry),
            out_specs=[slot_spec(width)] * 2
            + [slot_spec(hidden_units)] * 3
            + [stepped((STEP_BLOCKS, LANES, size), 0) for size in widths],
            scratch_shapes=[
                pltpu.VMEM((STEP_BLOCKS, experts_here * capacity, sum(widths)), BF16)
            ],
        ),
        out_shape=[slot_shape(width)] * 2
        + [slot_shape(hidden_units)] * 3
        + [jax.ShapeDtypeStruct((count, LANES, size), BF16) for size in widths],
        compiler_params=pltpu.CompilerParams(vmem_limit_bytes=VMEM_BYTES),
        cost_estimate=pl.CostEstimate(
            flops=flops, transcendentals=0, bytes_accessed=6 * count * LANES * width * 2
        ),
        input_output_aliases={before + n: n for n in range(len(carry))},
        name="expert_grads",
    )
    return call(
        first, *tokens, *grads,
        position, mask, router_t, up_both, up_both_t, down_t, *carry,
    )


def output_kernel(capacity, widths, gated_ref, position_ref, down_ref, *refs):
    out_refs, packed_ref = refs[:-1], refs[-1]
    for e in range(down_ref.shape[0]):
        rows = dot(gated_ref[e], down_ref[e]).astype(BF16)
        for j in range(STEP_BLOCKS):
            packed_ref[j, e * capacity : (e + 1) * capacity, :] = rows[
                j * capacity : (j + 1) * capacity
            ]
    for j in range(STEP_BLOCKS):
        choice = jnp.concatenate(choose(position_ref[j], capacity), axis=0).astype(BF16)
        home = dot(choice, packed_ref[j], 0, 0).astype(BF16)
        start = 0
        for out_ref, size in zip(out_refs, widths):
            out_ref[j] = home[:, start : start + size]
            start += size


def expert_outputs(half, gated, position, down, capacity, widths):
    count = position.shape[0]
    experts_here, hidden_units, width = down.shape
    slots = STEP_BLOCKS * capacity
    steps = count // STEP_BLOCKS
    call = pl.pallas_call(
        functools.partial(output_kernel, capacity, widths),
        grid=(steps,),
        in_specs=[
            pl.BlockSpec(
                (experts_here, slots, hidden_units), lambda i: (0, i + half * steps, 0)
            ),
            stepped((STEP_BLOCKS, experts_here, LANES), 0),
            whole(down.shape),
        ],
        out_specs=[stepped((STEP_BLOCKS, LANES, size), 0) for size in widths],
        out_shape=[jax.ShapeDtypeStruct((count, LANES, size), BF16) for size in widths],
        scratch_shapes=[pltpu.VMEM((STEP_BLOCKS, experts_here * capacity, width), BF16)],
        compiler_params=pltpu.CompilerParams(vmem_limit_bytes=VMEM_BYTES),
        cost_estimate=pl.CostEstimate(
            flops=2 * count * capacity * experts_here * (hidden_units * width + LANES * width),
            transcendentals=0,
            bytes_accessed=2 * count * LANES * width * 2,
        ),
        name="expert_outputs",
    )
    return call(gated, position, down)


def chunk_kernel(widths, perm, *refs):
    left = jnp.concatenate([ref[...] for ref in refs[:STEP_BLOCKS]], axis=1)
    product = dot(left, refs[STEP_BLOCKS][...], 0, 0).astype(BF16)
    start = 0
    for out_ref, size in zip(refs[STEP_BLOCKS + 1 :], widths):
        for j in range(STEP_BLOCKS):
            out_ref[j] = product[j * LANES : (j + 1) * LANES, start : start + size]
        start += size


def chunk_products(perm, left, right, widths):
    count = perm.shape[0]
    tokens = left.shape[0]

    def column_block(place):
        return pl.BlockSpec((tokens, LANES), lambda i, perm: (0, perm[i * STEP_BLOCKS + place]))

    call = pl.pallas_call(
        functools.partial(chunk_kernel, widths),
        grid_spec=pltpu.PrefetchScalarGridSpec(
            num_scalar_prefetch=1,
            grid=(count // STEP_BLOCKS,),
            in_specs=[column_block(j) for j in range(STEP_BLOCKS)] + [whole(right.shape)],
            out_specs=[stepped((STEP_BLOCKS, LANES, size), 0) for size in widths],
        ),
        out_shape=[jax.ShapeDtypeStruct((count, LANES, size), BF16) for size in widths],
        compiler_params=pltpu.CompilerParams(vmem_limit_bytes=VMEM_BYTES),
        cost_estimate=pl.CostEstimate(
            flops=2 * count * LANES * tokens * right.shape[1],
            transcendentals=0,
            bytes_accessed=count * LANES * right.shape[1] * 2,
        ),
        name="chunk_products",
    )
    return call(perm, *([left] * STEP_BLOCKS), right)


def block_orders(lattice, device_count):
    if not lattice:
        numbers = jnp.arange(device_count, dtype=jnp.int32)
        return numbers[: device_count // 2], numbers[device_count // 2 :]
    spot = my_spot()
    dz, dx, dy = (grid.reshape(-1) for grid in np.indices((4, 2, 2)).astype(np.int32))
    chip = (spot["z"] - dz + 4) % 4 * 2 + (spot["x"] + dx) % 2
    orders = []
    for dc in (1, 0):
        core = (spot["core"] + dc) % 2
        orders.append(((chip * 2 + core) * 2 + (spot["y"] + dy) % 2).astype(jnp.int32))
    return orders


def chunk_orders():
    spot = my_spot()
    dz, dx = (grid.reshape(-1) for grid in np.indices((4, 2)).astype(np.int32))
    chip = (spot["z"] - dz + 4) % 4 * 2 + (spot["x"] + dx) % 2
    return [(chip * 2 + (spot["core"] + dc) % 2).astype(jnp.int32) for dc in (1, 0)]


TOKEN_ORDERS = (("x", "y", "z"), ("y", "z", "x"), ("z", "x", "y"))
EARLY_ORDERS = (("z", "x", "y"), ("x", "z", "y"))
LATE_ORDERS = (("y", "x", "z"), ("y", "z", "x"))
GATHER_ORDERS = (("z", "y", "x"), ("x", "z", "y"), ("y", "x", "z"))
CHUNK_ORDERS = (("x", "z"), ("z", "x"))
TURNS = (1, -1, 1)


def scatter_job(partner, own):
    everything = jnp.concatenate([partner, own], axis=0)
    total = lax.psum_scatter(everything, BOTH, scatter_dimension=0, tiled=True)
    return total[0].astype(F32)
    yield


def tokens_home_jobs(lattice, partner, own, received, orders):
    jobs = []
    for n, order in enumerate(orders):
        if not lattice:
            jobs.append(scatter_job(partner[n], own[n]))
            continue
        shape = (4, 2, 2) + own[n].shape[1:]
        mine = own[n].reshape(shape)
        both = Pending(mine, received[n].reshape(shape))
        turn = 1 if orders is LATE_ORDERS else TURNS[n]
        jobs.append(home_job(None, both, "zxy", order, turn))
    return jobs


def product_job(left, right):
    product = dot(left, right, 0, 0).astype(BF16)
    return lax.psum_scatter(product, DP, scatter_dimension=0, tiled=True).astype(F32)
    yield


def weight_grads_chunks(lattice, left, right, widths):
    if not lattice:
        return left, right
    return tuple(chunk_products(order, left, right, widths) for order in chunk_orders())


def weight_grads_jobs(lattice, first, second):
    if not lattice:
        return [product_job(first, second)]
    jobs = []
    for n, order in enumerate(CHUNK_ORDERS):
        shape = (4, 2) + first[n].shape[1:]
        jobs.append(
            home_job(first[n].reshape(shape), second[n].reshape(shape), "zx", order, TURNS[n])
        )
    return jobs


def on_device(
    inputs,
    input_gain,
    post_gain,
    query_gain,
    key_gain,
    query_weight,
    key_projection_matrix,
    value_projection_matrix,
    output_weight,
    router_weight,
    gate_weight,
    up_weight,
    down_weight,
    routes,
    cotangent,
):
    dp_count, tensor_count = lax.axis_size(DP), lax.axis_size("tensor")
    device_count = dp_count * tensor_count
    lattice = is_lattice(dp_count, tensor_count)
    row_count, width = inputs.shape
    experts = router_weight.shape[1]
    experts_here = gate_weight.shape[0]
    capacity = 2 * row_count * routes.shape[1] // experts

    links, slow, outer = Links(), Links(), Links()
    projections = jnp.concatenate(
        [query_weight, key_projection_matrix, value_projection_matrix], axis=0
    )
    query_rows, key_rows = query_weight.shape[0], key_projection_matrix.shape[0]

    expert_ids = jnp.arange(experts, dtype=jnp.int32)
    chosen_mask = jnp.any(routes[:, :, None] == expert_ids[None, None, :], axis=1)
    small = [input_gain, post_gain, query_gain, key_gain]
    sizes = [item.shape[0] for item in small]
    flat = jnp.concatenate(small)
    padded = -(-flat.shape[0] // LANES) * LANES
    flat = jnp.pad(flat, (0, padded - flat.shape[0]))
    router_lines = router_weight.size // LANES
    payload = jnp.concatenate(
        [
            router_weight.reshape(router_lines, LANES),
            flat.reshape(-1, LANES),
            chosen_mask.T.astype(BF16),
        ],
        axis=0,
    )
    gathered_at, other_inputs_at = links.add(gather_small_job(payload), swap_job(inputs))
    projections_full = lax.all_gather(projections.T, DP, axis=0, tiled=True)
    if lattice:
        cuts = (width // 8 * 3, width // 16 * 11)
        grads_at = slow.add(*spread_jobs(cotangent, cuts[:1], "zxy", EARLY_ORDERS))
        links.marks = links.marks + slow.marks

    def join_up(gate, up):
        return jnp.concatenate([gate, up], axis=2)

    def turn_last(values):
        return with_layout_constraint(jnp.swapaxes(values, 1, 2), Layout((0, 1, 2)))

    up_both = links.round(join_up, gate_weight, up_weight)
    output_held = after(output_weight, up_both[0, :8, :LANES])
    output_full = lax.all_gather(output_held, DP, axis=0, tiled=True)
    slow.aside(links)
    up_both_t = links.round(turn_last, up_both)
    slow.aside(links)
    down_t = links.round(turn_last, down_weight)
    slow.aside(links)
    while gathered_at[0] is None:
        links.round()
    gathered, other_inputs = gathered_at[0], other_inputs_at[0]

    router_full = gathered[:, :router_lines].reshape(width, experts)
    flat_all = gathered[:, router_lines : router_lines + padded // LANES].reshape(
        device_count, padded
    )
    starts = np.cumsum([0] + sizes)
    input_scale, post_scale, query_scale, key_scale = (
        flat_all[:, starts[n] : starts[n + 1]].reshape(-1).astype(F32) for n in range(4)
    )
    mask_all = gathered[:, router_lines + padded // LANES :]
    first_expert = lax.axis_index(DP) * experts_here
    mask_here = lax.dynamic_slice_in_dim(mask_all, first_expert, experts_here, axis=1)
    earlier = jnp.asarray(np.triu(np.ones((row_count, row_count), np.float32), 1), BF16)
    rank = jnp.einsum("bet,tu->beu", mask_here, earlier, preferred_element_type=F32)
    position = jnp.where(mask_here > 0.5, rank, -1.0)
    orders = block_orders(lattice, device_count)
    positions = [position[order] for order in orders]
    masks = [mask_all[order] for order in orders]
    router_t = router_full.T

    both_inputs = in_order(inputs, other_inputs).astype(F32)
    residual_in = inputs.astype(F32)
    sequence = norm_rows(both_inputs, input_scale)[0].astype(BF16)
    _, input_hat, input_inv = norm_rows(residual_in, input_scale)
    seq_len = sequence.shape[0]
    local_heads = query_rows // HEAD_SIZE
    local_groups = key_rows // HEAD_SIZE
    per_group = local_heads // local_groups
    cosine_table, sine_table = rope_tables(seq_len, HEAD_SIZE)
    cosine, sine = cosine_table[:, None, :], sine_table[:, None, :]
    score_scale = 1.0 / math.sqrt(HEAD_SIZE)

    def project(projections_full):
        projected = dot(sequence, projections_full)
        query_raw = projected[:, :query_rows].reshape(seq_len, local_heads, HEAD_SIZE)
        key_raw = projected[:, query_rows : query_rows + key_rows].reshape(
            seq_len, local_groups, HEAD_SIZE
        )
        value_low = (
            projected[:, query_rows + key_rows :]
            .astype(BF16)
            .reshape(seq_len, local_groups, HEAD_SIZE)
        )
        query_norm, query_hat, query_inv = norm_rows(query_raw, query_scale)
        query_low = (query_norm * cosine + rotate_half(query_norm) * sine).astype(BF16)
        key_norm, key_hat, key_inv = norm_rows(key_raw, key_scale)
        key_low = (key_norm * cosine + rotate_half(key_norm) * sine).astype(BF16)
        query_groups = query_low.reshape(seq_len, local_groups, per_group, HEAD_SIZE)
        return query_groups, query_hat, query_inv, key_hat, key_inv, key_low, value_low

    def attention(query_groups, key_low, value_low):
        scores = (
            jnp.einsum("qhgd,khd->hgqk", query_groups, key_low, preferred_element_type=F32)
            * score_scale
        )
        row_index = jnp.arange(seq_len, dtype=jnp.int32)
        scores = jnp.where(row_index[None, :] <= row_index[:, None], scores, -1e30)
        attend = jax.nn.softmax(scores, axis=-1)
        attend_low = attend.astype(BF16)
        mixed_low = (
            jnp.einsum("hgqk,khd->qhgd", attend_low, value_low, preferred_element_type=F32)
            .astype(BF16)
            .reshape(seq_len, query_rows)
        )
        return mixed_low, attend, attend_low

    query_groups, query_hat, query_inv, key_hat, key_inv, key_low, value_low = links.round(
        project, projections_full
    )
    mixed_low, attend, attend_low = links.round(attention, query_groups, key_low, value_low)
    slow.aside(links)
    links.finish()
    ready = (positions, masks, router_t, up_both, up_both_t, down_t)
    mixed_low, (positions, masks, router_t, up_both, up_both_t, down_t) = (
        lax.optimization_barrier((mixed_low, ready))
    )
    mixed_out = dot(after(mixed_low, links.marks), output_full, 1, 1)
    (mixed_home,) = links.add(sum_tokens_job(mixed_out))
    links.finish()
    residual_mid = residual_in + mixed_home[0]
    post_norm, post_hat, post_inv = norm_rows(residual_mid, post_scale)
    post_low = post_norm.astype(BF16)
    block_starts = (0, 0)
    if lattice:
        tokens_at = links.add(*spread_jobs(post_low, cuts, "zxy", GATHER_ORDERS))
        slow.aside(links)
        links.finish()
        all_tokens, all_grads = gathered_groups(tokens_at), gathered_groups(grads_at)
    else:
        block_starts = (0, device_count // 2)
        all_tokens, all_grads = (
            ([lax.all_gather(values[None], BOTH, axis=0, tiled=True)],) * 2
            for values in (post_low, cotangent)
        )

    logits = dot(post_low, router_full)
    top = jnp.max(jnp.where(chosen_mask, logits, -3e38), axis=-1, keepdims=True)
    powers = jnp.where(chosen_mask, jnp.exp(jnp.minimum(logits - top, 0.0)), 0.0)
    gates = powers / jnp.sum(powers, axis=-1, keepdims=True)

    wide = width // 8 * 3
    widths = (wide, wide, width - 2 * wide + LANES)
    first_scalar = first_expert.astype(jnp.int32).reshape(1)

    def half_grads(half, carry):
        return expert_grads(
            half, carry, first_scalar, all_tokens[half], all_grads[half],
            block_starts[half], positions[half], masks[half],
            router_t, up_both, up_both_t, down_t, capacity, widths,
        )

    results = half_grads(0, ())
    partner = results[5:]
    received = [hop(group, "core") for group in partner] if lattice else None
    results = half_grads(1, results[:5])
    rows, grad_rows, gated, grad_gate_pre, grad_up_pre = results[:5]
    own = results[5:]

    def slot_product(left, right):
        return jnp.einsum("esd,esf->edf", left, right, preferred_element_type=F32)

    out_widths = (wide, width - wide)

    def outputs(gated):
        return [
            expert_outputs(n, gated, positions[n], down_weight, capacity, out_widths)
            for n in range(2)
        ]

    home = links.add(*tokens_home_jobs(lattice, partner, own, received, TOKEN_ORDERS))
    out_partner, out_own = links.round(outputs, gated)
    out_received = [hop(group, "core") for group in out_partner] if lattice else None
    grad_gate_w = links.round(slot_product, rows, grad_gate_pre)
    grad_down = links.round(slot_product, gated, grad_rows)
    links.finish()
    home = [place[0] for place in home]

    grad_out = cotangent.astype(F32)
    grad_post = jnp.concatenate([home[0], home[1], home[2][:, : width - 2 * wide]], axis=1)
    start = width - 2 * wide
    grad_gates = home[2][:, start : start + experts]
    grad_logits = (
        gates * (grad_gates - jnp.sum(gates * grad_gates, axis=-1, keepdims=True))
    ).astype(BF16)
    grad_post = grad_post + dot(grad_logits, router_full, 1, 1)
    grad_mid_norm, post_terms = norm_back(grad_post, post_scale, post_hat, post_inv)
    grad_mid = grad_out + grad_mid_norm
    grad_mid_low = grad_mid.astype(BF16)
    (other_grads,) = links.add(swap_job(grad_mid_low))
    out_jobs = tokens_home_jobs(lattice, out_partner, out_own, out_received, LATE_ORDERS)
    out_home = outer.add(*out_jobs)
    links.marks = links.marks + outer.marks
    grad_up_w = slot_product(*after((rows, grad_up_pre), links.marks))
    links.marks = [grad_up_w]
    while other_grads[0] is None:
        swapped = links.active.pop(0)
        links.advance(*swapped[:3], after(swapped[3], links.marks))
    grad_attention = in_order(grad_mid_low, other_grads[0])


    def back_scores(grad_attention):
        grad_mixed = dot(grad_attention, output_full).astype(BF16)
        grad_groups = grad_mixed.reshape(seq_len, local_groups, per_group, HEAD_SIZE)
        grad_attend = jnp.einsum(
            "qhgd,khd->hgqk", grad_groups, value_low, preferred_element_type=F32
        )
        row_inner = jnp.sum(attend * grad_attend, axis=-1, keepdims=True)
        grad_scores = (attend * (grad_attend - row_inner)).astype(BF16)
        return grad_groups, grad_scores

    out_split = query_rows // 8 * 3
    chunks = weight_grads_chunks(
        lattice, grad_attention, mixed_low, (out_split, query_rows - out_split)
    )
    grad_output_at = slow.add(*weight_grads_jobs(lattice, *chunks))
    links.marks = links.marks + slow.marks
    grad_groups, grad_scores = links.round(back_scores, grad_attention)
    slow.aside(links)
    grad_router = dot(post_low, grad_logits, 0, 0)
    grad_post_gain = jnp.sum(post_terms, axis=0)
    def back_heads(grad_groups, grad_scores):
        grad_value = jnp.einsum(
            "hgqk,qhgd->khd", attend_low, grad_groups, preferred_element_type=F32
        )
        grad_key_rot = (
            jnp.einsum("hgqk,qhgd->khd", grad_scores, query_groups, preferred_element_type=F32)
            * score_scale
        )
        grad_query_rot = (
            jnp.einsum("hgqk,khd->qhgd", grad_scores, key_low, preferred_element_type=F32)
            * score_scale
        ).reshape(seq_len, local_heads, HEAD_SIZE)
        return grad_value, grad_key_rot, grad_query_rot

    grad_value, grad_key_rot, grad_query_rot = links.round(back_heads, grad_groups, grad_scores)

    def back_norms(grad_query_rot):
        grad_query_norm = grad_query_rot * cosine + rotate_back(grad_query_rot * sine)
        grad_query_raw, query_terms = norm_back(grad_query_norm, query_scale, query_hat, query_inv)
        return grad_query_raw.reshape(seq_len, query_rows).astype(BF16), query_terms

    grad_query_low, query_terms = links.round(back_norms, grad_query_rot)
    grad_query_gain = jnp.sum(query_terms, axis=(0, 1))
    grad_key_norm = grad_key_rot * cosine + rotate_back(grad_key_rot * sine)
    grad_key_raw, key_terms = norm_back(grad_key_norm, key_scale, key_hat, key_inv)
    grad_key_gain = jnp.sum(key_terms, axis=(0, 1))
    grad_projected = jnp.concatenate(
        [
            grad_query_low,
            grad_key_raw.reshape(seq_len, key_rows).astype(BF16),
            grad_value.reshape(seq_len, key_rows).astype(BF16),
        ],
        axis=1,
    )
    total_rows = query_rows + 2 * key_rows
    split = total_rows // LANES * 2 // 5 * LANES
    chunks = weight_grads_chunks(
        lattice, sequence, grad_projected, (split, total_rows - split)
    )
    grad_projections_at = links.add(
        *weight_grads_jobs(lattice, *chunks), rank=-1
    )
    slow.aside(links)
    normed_parts = links.round(
        lambda grad: dot(grad, projections_full, 1, 1), grad_projected
    )
    (grad_normed,) = links.add(sum_tokens_job(normed_parts), rank=-1)
    links.round()
    slow.aside(links)
    outer.aside(links)
    grad_in_norm, input_terms = norm_back(grad_normed[0], input_scale, input_hat, input_inv)
    grad_input_gain = jnp.sum(input_terms, axis=0)
    grad_inputs = (grad_mid + grad_in_norm).astype(BF16)
    late_parts = [grad_router, grad_post_gain, grad_input_gain, grad_query_gain, grad_key_gain]
    flat = jnp.concatenate([part.reshape(device_count, -1) for part in late_parts], axis=1)
    flat = jnp.pad(flat, ((0, 0), (0, -flat.shape[1] % LANES)))
    (late,) = links.add(reduce_small_job(flat.reshape(device_count, -1, LANES)))
    while links.active or slow.active or outer.active:
        links.round()
        slow.aside(links)
        outer.aside(links)
    result = (residual_mid + jnp.concatenate([p[0] for p in out_home], axis=1)).astype(BF16)
    grad_output_w = jnp.concatenate([place[0] for place in grad_output_at], axis=1)
    grad_projections = jnp.concatenate([place[0] for place in grad_projections_at], axis=1).T
    grad_query_w = grad_projections[:query_rows]
    grad_key_w = grad_projections[query_rows : query_rows + key_rows]
    grad_value_w = grad_projections[query_rows + key_rows :]
    bounds = np.cumsum([0, router_weight.size, sizes[1], sizes[0], sizes[2], sizes[3]])
    late = late[0].reshape(-1)
    grad_router, grad_post_gain, grad_input_gain, grad_query_gain, grad_key_gain = (
        late[bounds[n] : bounds[n + 1]] for n in range(5)
    )
    grad_router = grad_router.reshape(router_weight.shape)
    return (
        result,
        grad_inputs,
        grad_input_gain,
        grad_post_gain,
        grad_query_gain,
        grad_key_gain,
        grad_query_w,
        grad_key_w,
        grad_value_w,
        grad_output_w,
        grad_router,
        grad_gate_w,
        grad_up_w,
        grad_down,
    )


def solution(mesh):
    dp_count, tensor_count = mesh.devices.shape
    split = jax.sharding.Mesh(
        mesh.devices.reshape(dp_count // 2, 2, tensor_count), ("chip", "core", "tensor")
    )
    tokens, line = P(BOTH, None), P(BOTH)
    gated = P(DP, None, "tensor")
    weights = (P("tensor", DP),) * 3 + (P(DP, "tensor"), tokens, gated, gated, P(DP, "tensor", None))
    return jax.shard_map(
        on_device,
        mesh=split,
        in_specs=(tokens,) + (line,) * 4 + weights + (tokens, tokens),
        out_specs=(tokens, tokens) + (line,) * 4 + weights,
        check_vma=False,
    )
```
